128 devices in a mesh: stage: 1, data: 64 (over z, y, x), tp: 2 (over core).
Axes of the slice: x: 4, y: 4, z: 4, core: 2. Of those that a mesh axis runs over, the one named last changes fastest.
Arguments:
- weight: float32 [1536, 12288], P(('stage', 'data'), 'tp')
- momentum: float32 [1536, 12288], P(('stage', 'data'), 'tp')
- gradient: bfloat16 [1536, 12288], P(('stage', 'data'), 'tp')
Outputs:
- output 1: float32 [1536, 12288], P(('stage', 'data'), 'tp')
- output 2: float32 [1536, 12288], P(('stage', 'data'), 'tp')
All inputs are finite; a program needn't handle non-finite values.
Results may differ from the reference program's by a relative error of at most 0.00743.
Values are sent between devices in bfloat16 or wider.
A program may use at most 1 GiB of HBM per device.

```python
import math
import jax
import jax.numpy as jnp
from jax import lax

MAT_ROWS = 1536
MAT_COLS = 12288
NS_STEPS = 5
LOW_RANK = 8
MOMENTUM = 0.95
LEARN_RATE = 0.5
WEIGHT_DECAY = 0.1
COEF_A = 3.4445
COEF_B = -4.7750
COEF_C = 2.0315
EPSILON = 1e-7


def draw_structured(base_key):
    key_noise, key_left, key_right = jax.random.split(base_key, 3)
    noise_mat = jax.random.normal(key_noise, (MAT_ROWS, MAT_COLS), jnp.float32)
    left_fac = jax.random.normal(key_left, (MAT_ROWS, LOW_RANK), jnp.float32)
    right_fac = jax.random.normal(key_right, (LOW_RANK, MAT_COLS), jnp.float32)
    col_pos = jnp.arange(MAT_COLS, dtype=jnp.float32) / MAT_COLS
    row_pos = jnp.arange(MAT_ROWS, dtype=jnp.float32) / MAT_ROWS
    rank_pos = jnp.arange(LOW_RANK, dtype=jnp.float32) / LOW_RANK
    window = 1.0 + jnp.cos(2.0 * math.pi * (col_pos[None, :] - rank_pos[:, None]))
    low_part = jnp.dot(left_fac, right_fac * window) * (LOW_RANK ** -0.5)
    col_scale = 0.25 + 1.5 * col_pos
    row_scale = 0.5 + row_pos
    return (noise_mat + low_part) * col_scale[None, :] * row_scale[:, None]


def setup_inputs(seed: int = 0, part: int = 0) -> dict:
    base_key = jax.random.fold_in(jax.random.key(seed), part)
    key_weight, key_mom, key_grad = jax.random.split(base_key, 3)
    weight = 0.1 * jax.random.normal(key_weight, (MAT_ROWS, MAT_COLS), jnp.float32)
    momentum = 0.8 * draw_structured(key_mom)
    gradient = draw_structured(key_grad).astype(jnp.bfloat16)
    return {"weight": weight, "momentum": momentum, "gradient": gradient}


def reference(weight, momentum, gradient):
    grad_f32 = gradient.astype(jnp.float32)
    new_mom = MOMENTUM * momentum + grad_f32
    nest_term = grad_f32 + MOMENTUM * new_mom
    frob_norm = jnp.sqrt(jnp.sum(nest_term * nest_term))
    x_init = (nest_term / (frob_norm + EPSILON)).astype(jnp.bfloat16)

    def ns_iter(x_cur, unused):
        gram_mat = jnp.dot(x_cur, x_cur.T, preferred_element_type=jnp.float32).astype(jnp.bfloat16)
        poly_mat = (COEF_B * gram_mat.astype(jnp.float32) + COEF_C * jnp.dot(gram_mat, gram_mat, preferred_element_type=jnp.float32)).astype(jnp.bfloat16)
        x_next = (COEF_A * x_cur.astype(jnp.float32) + jnp.dot(poly_mat, x_cur, preferred_element_type=jnp.float32)).astype(jnp.bfloat16)
        return x_next, None

    x_final, unused_out = lax.scan(ns_iter, x_init, None, length=NS_STEPS)
    rms_scale = 0.2 * math.sqrt(max(MAT_ROWS, MAT_COLS))
    new_weight = weight - LEARN_RATE * (rms_scale * x_final.astype(jnp.float32) + WEIGHT_DECAY * weight)
    return (new_weight, new_mom)
```

```python
import math
import jax
import jax.numpy as jnp
from jax import lax
from jax.sharding import PartitionSpec as P

NS_STEPS = 5
MOMENTUM = 0.95
LEARN_RATE = 0.5
WEIGHT_DECAY = 0.1
COEF_A = 3.4445
COEF_B = -4.7750
COEF_C = 2.0315
EPSILON = 1e-7


def solution(mesh):
    data_size = mesh.shape["data"]
    tp_size = mesh.shape["tp"]
    part_spec = P(("stage", "data"), "tp")

    def dot(p, q):
        return jnp.dot(p, q, preferred_element_type=jnp.float32)

    def dot_bf16(p, q):
        return dot(p.astype(jnp.bfloat16), q)

    def dot_wide(p, q):
        high = lax.reduce_precision(p, 8, 7)
        low = (p - high).astype(jnp.bfloat16)
        return dot(high.astype(jnp.bfloat16), q) + dot(low, q)

    def local_step(weight, momentum, gradient):
        rows_local, cols_local = gradient.shape
        rows = rows_local * data_size
        half = rows // tp_size
        cols = cols_local // data_size
        grad_f32 = gradient.astype(jnp.float32)
        new_mom = MOMENTUM * momentum + grad_f32
        nest_term = grad_f32 + MOMENTUM * new_mom
        frob_norm = jnp.sqrt(lax.psum(jnp.sum(nest_term * nest_term), ("data", "tp")))
        x_local = (nest_term / (frob_norm + EPSILON)).astype(jnp.bfloat16)
        x_cols = lax.all_to_all(x_local.reshape(rows_local, data_size, cols), "data", 1, 0, tiled=True)
        x_t = x_cols.reshape(rows, cols).T
        x_pair = lax.all_gather(x_t, "tp", axis=0, tiled=True)
        mine = lax.dynamic_slice_in_dim(x_pair, lax.axis_index("tp") * half, half, 1)
        gram = lax.psum(jnp.einsum("ki,kj->ij", mine, x_pair, preferred_element_type=jnp.float32), "data")
        for step in range(NS_STEPS):
            gram_b = gram.astype(jnp.bfloat16)
            gram_full = lax.all_gather(gram_b, "tp", axis=0, tiled=True)
            poly = (COEF_B * gram_b.astype(jnp.float32) + COEF_C * dot(gram_b, gram_full)).astype(jnp.bfloat16)
            poly_full = lax.all_gather(poly, "tp", axis=0, tiled=True)
            if step < NS_STEPS - 1:
                wide = dot_wide if step == NS_STEPS - 2 else dot_bf16
                mid = COEF_A * gram + wide(gram, poly_full)
                gram = COEF_A * mid + wide(mid, poly_full)
            x_t = (COEF_A * x_t.astype(jnp.float32) + dot(x_t, poly_full)).astype(jnp.bfloat16)
        x_fin = lax.all_to_all(x_t.T.reshape(data_size, rows_local, cols), "data", 0, 2, tiled=True)
        x_fin = x_fin.reshape(rows_local, cols_local)
        rms_scale = 0.2 * math.sqrt(max(rows, cols_local * tp_size))
        new_weight = weight - LEARN_RATE * (rms_scale * x_fin.astype(jnp.float32) + WEIGHT_DECAY * weight)
        return new_weight, new_mom

    return jax.shard_map(local_step, mesh=mesh, in_specs=(part_spec, part_spec, part_spec), out_specs=(part_spec, part_spec), check_vma=False)
```

```python
import functools
import math
import jax
import jax.numpy as jnp
from jax import lax
from jax.experimental import pallas as pl
from jax.experimental.pallas import tpu as pltpu
from jax.sharding import PartitionSpec as P

NS_STEPS = 5
MOMENTUM = 0.95
LEARN_RATE = 0.5
WEIGHT_DECAY = 0.1
COEF_A = 3.4445
COEF_B = -4.7750
COEF_C = 2.0315
EPSILON = 1e-7

MESH = pl.DeviceIdType.MESH
F32 = jnp.float32
BF16 = jnp.bfloat16
BLOCKS = ((0, 0), (1, 0), (1, 1), (2, 0), (2, 1), (2, 2), (0, 3), (0, 4), (0, 5), (1, 4), (1, 5), (2, 5))
SWAPPED = (7, 8, 10)
STRIDES = (1, 4, 16)


def dot(p, q):
    return jnp.dot(p, q, preferred_element_type=F32)


def kernel(nb, y_ref, rx, sq, xg, part, rb1, s1, rb2, s2, rb3, gath, swap, gram, mid, af, bff, al, tb, xt, xp, ys, yr,
           a2a_s, a2a_r, sq_s, sq_r, xg_s, xg_r, rs_s, rs_r, ag_s, ag_r, sw_s, sw_r, pa_s, pa_r, pb_s, pb_r, out_s, out_r):
    me = lax.axis_index("data")
    t = lax.axis_index("tp")
    sib = {"tp": 1 - t}
    coord = (me % 4, (me // 4) % 4, me // 16)
    n_data, rows_src, lanes = nb.shape
    used = 96
    half = 768

    def rcopy(src, dst, ssem, rsem, dev):
        return pltpu.make_async_remote_copy(src_ref=src, dst_ref=dst, send_sem=ssem, recv_sem=rsem, device_id=dev, device_id_type=MESH)

    slot = (me + 32 * t) % 64

    def a2a_copy(o):
        d = (me + o) % 64
        return rcopy(nb.at[d], rx.at[slot], a2a_s.at[o], a2a_r.at[slot], {"data": d})

    @pl.loop(1, 64)
    def _(o):
        a2a_copy(o).start()

    rx[slot] = nb[me]

    @pl.loop(1, 64)
    def _(o):
        src = ((me + 64 - o) % 64 + 32 * t) % 64
        rcopy(nb.at[0], rx.at[src], a2a_s.at[o], a2a_r.at[src], {"data": (me + o) % 64}).wait()

    sq[0] = jnp.sum(rx[:, 0:8, :], axis=0)
    c = rcopy(sq.at[0], sq.at[1], sq_s, sq_r, sib)
    c.start()
    c.wait()
    total = (sq[0] + sq[1])[0:1, lanes - 1:lanes]
    norm = jnp.sqrt(total) + EPSILON
    lane_ok = lax.broadcasted_iota(jnp.int32, (384, lanes), 1) < used

    @pl.loop(0, 4)
    def _(i):
        v = rx[pl.ds(i * 16, 16)].reshape(384, lanes)
        x = jnp.where(lane_ok, v / norm, 0.0).astype(BF16)
        xg[pl.ds(pl.multiple_of(i * 384, 384), 384), 0:128] = x
        xt[:, pl.ds(pl.multiple_of(i * 384, 384), 384)] = x.astype(F32).T.astype(BF16)

    def xg_copy(h):
        return rcopy(xg.at[pl.ds(h * half, half), pl.ds(0, 128)], xg.at[pl.ds((1 - h) * half, half), pl.ds(128, 128)], xg_s.at[h], xg_r.at[h], sib)

    for h in range(2):
        xg_copy(h).start()
    for h in range(2):
        xg_copy(h).wait()

    def peer(dim, o):
        m = coord[dim]
        return {"data": me + ((m + o) % 4 - m) * STRIDES[dim]}

    def dims(col):
        return col, (col + 1) % 3, (col + 2) % 3

    def rs_copy(col, ph, o):
        d = dims(col)[ph]
        j = (coord[d] + o) % 4
        src = (part, s1, s2)[ph].at[col, j]
        dst = (rb1, rb2, rb3)[ph].at[col, o - 1]
        k = (ph * 3 + col) * 3 + o - 1
        return rcopy(src, dst, rs_s.at[k], rs_r.at[k], peer(d, o))

    def ag_ref(col, ph):
        m1, m2, m3 = (coord[d] for d in dims(col))
        return (gath.at[col, m1, m2, m3], gath.at[col, m1, m2], gath.at[col, m1])[ph]

    def ag_copy(col, ph, o):
        d = dims(col)[2 - ph]
        k = (ph * 3 + col) * 3 + o - 1
        return rcopy(ag_ref(col, ph), ag_ref(col, ph), ag_s.at[k], ag_r.at[k], peer(d, o))

    for col in range(3):
        for b in range(4):
            i, j = BLOCKS[col * 4 + b]
            res = lax.dot_general(xg[i * 256:(i + 1) * 256, :], xg[j * 256:(j + 1) * 256, :], (((1,), (1,)), ((), ())), preferred_element_type=F32)
            for h in range(2):
                part[col, b, h * 8:(h + 1) * 8] = res[:, h * 128:(h + 1) * 128].reshape(8, 32, 128)
        for o in range(1, 4):
            rs_copy(col, 0, o).start()
    for ph in range(3):
        for col in range(3):
            for o in range(1, 4):
                rs_copy(col, ph, o).wait()
            m1, m2, m3 = (coord[d] for d in dims(col))
            if ph == 0:
                s1[col] = (part[col, m1] + rb1[col, 0] + rb1[col, 1] + rb1[col, 2]).reshape(4, 4, 32, 128)
            elif ph == 1:
                s2[col] = s1[col, m2] + rb2[col, 0] + rb2[col, 1] + rb2[col, 2]
            else:
                gath[col, m1, m2, m3] = s2[col, m3] + rb3[col, 0] + rb3[col, 1] + rb3[col, 2]
            for o in range(1, 4):
                if ph < 2:
                    rs_copy(col, ph + 1, o).start()
                else:
                    ag_copy(col, 0, o).start()
    for ph in range(3):
        for col in range(3):
            for o in range(1, 4):
                ag_copy(col, ph, o).wait()
            if ph < 2:
                for o in range(1, 4):
                    ag_copy(col, ph + 1, o).start()

    def swap_copy(n):
        q = SWAPPED[n]
        return rcopy(gath.at[q // 4, q % 4], swap.at[n], sw_s.at[n], sw_r.at[n], sib)

    for n in range(3):
        swap_copy(n).start()

    def put(i, j, h, v):
        gram[i * 256:(i + 1) * 256, j * 256 + h * 128:j * 256 + (h + 1) * 128] = v

    def put_t(i, j, h, v):
        gram[i * 256 + h * 128:i * 256 + (h + 1) * 128, j * 256:(j + 1) * 256] = v.T

    for q, (i, j) in enumerate(BLOCKS):
        for h in range(2):
            v = gath[q // 4, q % 4, 2 * h:2 * h + 2].reshape(256, 128)
            put(i, j, h, v)
            if j < i:
                put_t(j, i, h, v)
    for n in range(3):
        swap_copy(n).wait()
        i, j = BLOCKS[SWAPPED[n]]
        for h in range(2):
            put_t(j - 3, i + 3, h, swap[n, 2 * h:2 * h + 2].reshape(256, 128))

    def piece(buf, ssem, rsem, p):
        q = (p + 3) % 6
        return rcopy(buf.at[pl.ds(0, half), pl.ds(pl.multiple_of(p * 256, 256), 256)],
                     buf.at[pl.ds(half, half), pl.ds(pl.multiple_of(q * 256, 256), 256)], ssem.at[p], rsem.at[p], sib)

    def send_two(buf, ssem, rsem, n):
        piece(buf, ssem, rsem, 2 * n).start()
        piece(buf, ssem, rsem, 2 * n + 1).start()

    def wait_recv(buf, ssem, rsem):
        for p in range(6):
            piece(buf, ssem, rsem, p).wait_recv()

    def wait_send(buf, ssem, rsem):
        for p in range(6):
            piece(buf, ssem, rsem, p).wait_send()

    def columns(n):
        return pl.ds(pl.multiple_of(n * 512, 512), 512)

    own = slice(0, half)
    oth = slice(half, 2 * half)

    @pl.loop(0, 3)
    def _(n):
        cs = columns(n)
        af[own, cs] = gram[:, cs].astype(BF16)
        send_two(af, pa_s, pa_r, n)

    def poly_step():
        @pl.loop(0, 3)
        def _(n):
            cs = columns(n)
            mid[:, cs] = dot(af[own, own], af[own, cs])

        wait_recv(af, pa_s, pa_r)

        @pl.loop(0, 3)
        def _(n):
            cs = columns(n)
            acc = mid[:, cs] + dot(af[own, oth], af[oth, cs])
            bff[own, cs] = (COEF_B * af[own, cs].astype(F32) + COEF_C * acc).astype(BF16)
            send_two(bff, pb_s, pb_r, n)

    def x_first(cs):
        xp[:, cs] = COEF_A * xt[:, cs].astype(F32) + dot(xt[:, own], bff[own, cs])

    def x_second(cs):
        xp[:, cs] = xp[:, cs] + dot(xt[:, oth], bff[oth, cs])

    def gram_step(wide):
        if wide:
            @pl.loop(0, 3)
            def _(n):
                cs = columns(n)
                al[:, cs] = (gram[:, cs] - af[own, cs].astype(F32)).astype(BF16)

        @pl.loop(0, 3)
        def _(n):
            cs = columns(n)
            v = COEF_A * gram[:, cs] + dot(af[own, own], bff[own, cs])
            if wide:
                v = v + dot(al[:, own], bff[own, cs])
            mid[:, cs] = v
            x_first(cs)

        wait_recv(bff, pb_s, pb_r)

        @pl.loop(0, 3)
        def _(n):
            cs = columns(n)
            v = mid[:, cs] + dot(af[own, oth], bff[oth, cs])
            if wide:
                v = v + dot(al[:, oth], bff[oth, cs])
            mid[:, cs] = v
            tb[:, cs] = v.astype(BF16)
            x_second(cs)

        xt[...] = xp[...].astype(BF16)
        if wide:
            @pl.loop(0, 3)
            def _(n):
                cs = columns(n)
                al[:, cs] = (mid[:, cs] - tb[:, cs].astype(F32)).astype(BF16)
        wait_send(af, pa_s, pa_r)

        @pl.loop(0, 3)
        def _(n):
            cs = columns(n)
            v = COEF_A * mid[:, cs] + dot(tb[...], bff[:, cs])
            if wide:
                v = v + dot(al[...], bff[:, cs])
            gram[:, cs] = v
            af[own, cs] = v.astype(BF16)
            send_two(af, pa_s, pa_r, n)

        wait_send(bff, pb_s, pb_r)

    @pl.loop(0, NS_STEPS - 2)
    def _(k):
        poly_step()
        gram_step(False)

    poly_step()
    gram_step(True)
    poly_step()

    @pl.loop(0, 3)
    def _(n):
        x_first(columns(n))

    wait_recv(bff, pb_s, pb_r)

    @pl.loop(0, 3)
    def _(n):
        x_second(columns(n))

    wait_send(af, pa_s, pa_r)
    wait_send(bff, pb_s, pb_r)

    ys[...] = jnp.zeros_like(ys)

    @pl.loop(0, 4)
    def _(i):
        v = xp[:, pl.ds(pl.multiple_of(i * 384, 384), 384)].astype(BF16).astype(F32).T
        ys[pl.ds(i * 16, 16), 0:24, :] = v.reshape(16, 24, 128).astype(BF16)

    def out_copy(o):
        d = (me + o) % 64
        return rcopy(ys.at[(d + 32 * t) % 64], yr.at[me], out_s.at[o], out_r.at[me], {"data": d})

    @pl.loop(1, 64)
    def _(o):
        out_copy(o).start()

    yr[me] = ys[slot]

    @pl.loop(1, 64)
    def _(o):
        src = (me + 64 - o) % 64
        rcopy(ys.at[0], yr.at[src], out_s.at[o], out_r.at[src], {"data": (me + o) % 64}).wait()

    y_ref[...] = yr[...]


def solution(mesh):
    data_size = mesh.shape["data"]
    tp_size = mesh.shape["tp"]
    part_spec = P(("stage", "data"), "tp")

    def local_step(weight, momentum, gradient):
        rows_local, cols_local = gradient.shape
        rows = rows_local * data_size
        cols = cols_local // data_size
        grad_f32 = gradient.astype(F32)
        new_mom = MOMENTUM * momentum + grad_f32
        nest_term = grad_f32 + MOMENTUM * new_mom
        sumsq = jnp.sum(nest_term * nest_term)
        blocks = nest_term.reshape(rows_local, data_size, cols).transpose(1, 0, 2)
        blocks = jnp.concatenate([blocks, jnp.broadcast_to(sumsq, (data_size, rows_local, 128 - cols))], axis=2)
        sem = pltpu.SemaphoreType.DMA
        shapes = [
            pltpu.VMEM((64, 24, 128), F32), pltpu.VMEM((2, 8, 128), F32), pltpu.VMEM((1536, 256), BF16),
            pltpu.VMEM((3, 4, 16, 32, 128), F32), pltpu.VMEM((3, 3, 16, 32, 128), F32), pltpu.VMEM((3, 4, 4, 32, 128), F32),
            pltpu.VMEM((3, 3, 4, 32, 128), F32), pltpu.VMEM((3, 4, 32, 128), F32), pltpu.VMEM((3, 3, 32, 128), F32),
            pltpu.VMEM((3, 4, 4, 4, 32, 128), F32), pltpu.VMEM((3, 4, 4, 32, 128), F32),
            pltpu.VMEM((768, 1536), F32), pltpu.VMEM((768, 1536), F32), pltpu.VMEM((1536, 1536), BF16), pltpu.VMEM((1536, 1536), BF16),
            pltpu.VMEM((768, 1536), BF16), pltpu.VMEM((768, 1536), BF16), pltpu.VMEM((128, 1536), BF16), pltpu.VMEM((128, 1536), F32),
            pltpu.VMEM((64, 32, 128), BF16), pltpu.VMEM((64, 32, 128), BF16),
            sem((64,)), sem((64,)), sem, sem, sem((2,)), sem((2,)), sem((27,)), sem((27,)), sem((27,)), sem((27,)),
            sem((3,)), sem((3,)), sem((6,)), sem((6,)), sem((6,)), sem((6,)), sem((64,)), sem((64,)),
        ]
        x_blocks = pl.pallas_call(
            kernel,
            out_shape=jax.ShapeDtypeStruct((64, 32, 128), BF16),
            in_specs=[pl.BlockSpec(memory_space=pltpu.VMEM)],
            out_specs=pl.BlockSpec(memory_space=pltpu.VMEM),
            scratch_shapes=shapes,
            compiler_params=pltpu.CompilerParams(has_side_effects=True, vmem_limit_bytes=60 * 1024 * 1024),
            name="muon_steps",
        )(blocks)
        x_fin = x_blocks[:, :rows_local, :cols].transpose(1, 0, 2).reshape(rows_local, cols_local)
        rms_scale = 0.2 * math.sqrt(max(rows, cols_local * tp_size))
        new_weight = weight - LEARN_RATE * (rms_scale * x_fin.astype(F32) + WEIGHT_DECAY * weight)
        return new_weight, new_mom

    return jax.shard_map(local_step, mesh=mesh, in_specs=(part_spec, part_spec, part_spec), out_specs=(part_spec, part_spec), check_vma=False)
```

```python
import functools
import math
import jax
import jax.numpy as jnp
from jax import lax
from jax.experimental import pallas as pl
from jax.experimental.pallas import tpu as pltpu
from jax.sharding import PartitionSpec as P

NS_STEPS = 5
MOMENTUM = 0.95
LEARN_RATE = 0.5
WEIGHT_DECAY = 0.1
COEF_A = 3.4445
COEF_B = -4.7750
COEF_C = 2.0315
EPSILON = 1e-7

MESH = pl.DeviceIdType.MESH
F32 = jnp.float32
BF16 = jnp.bfloat16
BLOCKS = ((0, 0), (1, 0), (1, 1), (2, 0), (2, 1), (2, 2), (0, 3), (0, 4), (0, 5), (1, 4), (1, 5), (2, 5))
SWAPPED = (7, 8, 10)
STRIDES = (1, 4, 16)


def dot(p, q):
    return jnp.dot(p, q, preferred_element_type=F32)


def kernel(scale, w_hbm, m_hbm, g_hbm, w_out, m_out, wv, mv, gv, nb, rx, sq, xg, part, rb1, s1, rb2, s2, rb3, gath, swap, gram, mid, af, bff, al, tb, ys, yr,
           in_s, a2a_s, a2a_r, sq_s, sq_r, xg_s, xg_r, rs_s, rs_r, ag_s, ag_r, sw_s, sw_r, pa_s, pa_r, pb_s, pb_r, out_s, out_r):
    me = lax.axis_index("data")
    t = lax.axis_index("tp")
    sib = {"tp": 1 - t}
    coord = (me % 4, (me // 4) % 4, me // 16)
    rows_src, lanes = nb.shape[1:]
    used = 96
    half = 768
    own = slice(0, half)
    xrow = slice(half, half + 128)
    both = slice(0, half + 128)
    oth = slice(half, 2 * half)
    oth_rows = slice(half + 128, 2 * half + 128)

    def rcopy(src, dst, ssem, rsem, dev):
        return pltpu.make_async_remote_copy(src_ref=src, dst_ref=dst, send_sem=ssem, recv_sem=rsem, device_id=dev, device_id_type=MESH)

    barrier = pltpu.get_barrier_semaphore()

    @pl.loop(1, 64)
    def _(o):
        pl.semaphore_signal(barrier, inc=1, device_id={"data": (me + o) % 64}, device_id_type=MESH)

    pl.semaphore_signal(barrier, inc=1, device_id=sib, device_id_type=MESH)

    load_m = pltpu.make_async_copy(m_hbm, mv, in_s.at[0])
    load_g = pltpu.make_async_copy(g_hbm, gv, in_s.at[1])
    load_w = pltpu.make_async_copy(w_hbm, wv, in_s.at[2])
    load_m.start()
    load_g.start()
    load_w.start()
    load_m.wait()
    load_g.wait()
    lane = lax.broadcasted_iota(jnp.int32, (rows_src, lanes), 1)

    def group(g, ssq):
        tiles = []
        for r in range(3):
            cs = pl.ds(pl.multiple_of((g * 3 + r) * 128, 128), 128)
            grad = gv[:, cs].astype(F32)
            new_mom = MOMENTUM * mv[:, cs] + grad
            mv[:, cs] = new_mom
            nest = grad + MOMENTUM * new_mom
            nb[g * 4 + r] = nest
            ssq = ssq + nest * nest
            tiles.append(pltpu.roll(nest, 32 * (r + 1), 1))
        nb[g * 4 + 3] = jnp.where(lane < 32, tiles[0], jnp.where(lane < 64, tiles[1], tiles[2]))
        return ssq

    ssq = lax.fori_loop(0, 16, group, jnp.zeros((rows_src, lanes), F32))
    store_m = pltpu.make_async_copy(mv, m_out, in_s.at[3])
    store_m.start()
    ssq = jnp.sum(jnp.sum(ssq, axis=0, keepdims=True), axis=1, keepdims=True)
    lane8 = lax.broadcasted_iota(jnp.int32, (8, lanes), 1)

    @pl.loop(0, 64)
    def _(d):
        nb[d, 0:8] = jnp.where(lane8 < used, nb[d, 0:8], ssq)

    pl.semaphore_wait(barrier, 64)

    slot = (me + 32 * t) % 64

    def a2a_copy(o):
        d = (me + o) % 64
        return rcopy(nb.at[d], rx.at[slot], a2a_s.at[o], a2a_r.at[slot], {"data": d})

    @pl.loop(1, 64)
    def _(o):
        a2a_copy(o).start()

    rx[slot] = nb[me]

    @pl.loop(1, 64)
    def _(o):
        src = ((me + 64 - o) % 64 + 32 * t) % 64
        rcopy(nb.at[0], rx.at[src], a2a_s.at[o], a2a_r.at[src], {"data": (me + o) % 64}).wait()

    sq[0] = jnp.sum(rx[:, 0:8, :], axis=0)
    c = rcopy(sq.at[0], sq.at[1], sq_s, sq_r, sib)
    c.start()
    c.wait()
    total = (sq[0] + sq[1])[0:1, lanes - 1:lanes]
    norm = jnp.sqrt(total) + EPSILON
    lane_ok = lax.broadcasted_iota(jnp.int32, (384, lanes), 1) < used

    @pl.loop(0, 4)
    def _(i):
        v = rx[pl.ds(i * 16, 16)].reshape(384, lanes)
        x = jnp.where(lane_ok, v / norm, 0.0).astype(BF16)
        xg[pl.ds(pl.multiple_of(i * 384, 384), 384), 0:128] = x
        af[xrow, pl.ds(pl.multiple_of(i * 384, 384), 384)] = x.astype(F32).T.astype(BF16)

    def xg_copy(h):
        return rcopy(xg.at[pl.ds(h * half, half), pl.ds(0, 128)], xg.at[pl.ds((1 - h) * half, half), pl.ds(128, 128)], xg_s.at[h], xg_r.at[h], sib)

    for h in range(2):
        xg_copy(h).start()
    for h in range(2):
        xg_copy(h).wait()

    def peer(dim, o):
        m = coord[dim]
        return {"data": me + ((m + o) % 4 - m) * STRIDES[dim]}

    def dims(col):
        return col, (col + 1) % 3, (col + 2) % 3

    def rs_copy(col, ph, o):
        d = dims(col)[ph]
        j = (coord[d] + o) % 4
        src = (part, s1, s2)[ph].at[col, j]
        dst = (rb1, rb2, rb3)[ph].at[col, o - 1]
        k = (ph * 3 + col) * 3 + o - 1
        return rcopy(src, dst, rs_s.at[k], rs_r.at[k], peer(d, o))

    def ag_ref(col, ph):
        m1, m2, m3 = (coord[d] for d in dims(col))
        return (gath.at[col, m1, m2, m3], gath.at[col, m1, m2], gath.at[col, m1])[ph]

    def ag_copy(col, ph, o):
        d = dims(col)[2 - ph]
        k = (ph * 3 + col) * 3 + o - 1
        return rcopy(ag_ref(col, ph), ag_ref(col, ph), ag_s.at[k], ag_r.at[k], peer(d, o))

    for col in range(3):
        for b in range(4):
            i, j = BLOCKS[col * 4 + b]
            res = lax.dot_general(xg[i * 256:(i + 1) * 256, :], xg[j * 256:(j + 1) * 256, :], (((1,), (1,)), ((), ())), preferred_element_type=F32)
            for h in range(2):
                part[col, b, h * 8:(h + 1) * 8] = res[:, h * 128:(h + 1) * 128].reshape(8, 32, 128)
        for o in range(1, 4):
            rs_copy(col, 0, o).start()
    for ph in range(3):
        for col in range(3):
            for o in range(1, 4):
                rs_copy(col, ph, o).wait()
            m1, m2, m3 = (coord[d] for d in dims(col))
            if ph == 0:
                s1[col] = (part[col, m1] + rb1[col, 0] + rb1[col, 1] + rb1[col, 2]).reshape(4, 4, 32, 128)
            elif ph == 1:
                s2[col] = s1[col, m2] + rb2[col, 0] + rb2[col, 1] + rb2[col, 2]
            else:
                gath[col, m1, m2, m3] = s2[col, m3] + rb3[col, 0] + rb3[col, 1] + rb3[col, 2]
            for o in range(1, 4):
                if ph < 2:
                    rs_copy(col, ph + 1, o).start()
                else:
                    ag_copy(col, 0, o).start()
    for ph in range(3):
        for col in range(3):
            for o in range(1, 4):
                ag_copy(col, ph, o).wait()
            if ph < 2:
                for o in range(1, 4):
                    ag_copy(col, ph + 1, o).start()

    def swap_copy(n):
        q = SWAPPED[n]
        return rcopy(gath.at[q // 4, q % 4], swap.at[n], sw_s.at[n], sw_r.at[n], sib)

    for n in range(3):
        swap_copy(n).start()

    def put(i, j, h, v):
        gram[i * 256:(i + 1) * 256, j * 256 + h * 128:j * 256 + (h + 1) * 128] = v

    def put_t(i, j, h, v):
        gram[i * 256 + h * 128:i * 256 + (h + 1) * 128, j * 256:(j + 1) * 256] = v.T

    for q, (i, j) in enumerate(BLOCKS):
        for h in range(2):
            v = gath[q // 4, q % 4, 2 * h:2 * h + 2].reshape(256, 128)
            put(i, j, h, v)
            if j < i:
                put_t(j, i, h, v)
    for n in range(3):
        swap_copy(n).wait()
        i, j = BLOCKS[SWAPPED[n]]
        for h in range(2):
            put_t(j - 3, i + 3, h, swap[n, 2 * h:2 * h + 2].reshape(256, 128))

    def piece(buf, ssem, rsem, p):
        q = (p + 3) % 6
        return rcopy(buf.at[pl.ds(0, half), pl.ds(pl.multiple_of(p * 256, 256), 256)],
                     buf.at[pl.ds(half + 128, half), pl.ds(pl.multiple_of(q * 256, 256), 256)], ssem.at[p], rsem.at[p], sib)

    def send_two(buf, ssem, rsem, n):
        piece(buf, ssem, rsem, 2 * n).start()
        piece(buf, ssem, rsem, 2 * n + 1).start()

    def wait_recv(buf, ssem, rsem):
        for p in range(6):
            piece(buf, ssem, rsem, p).wait_recv()

    def wait_send(buf, ssem, rsem):
        for p in range(6):
            piece(buf, ssem, rsem, p).wait_send()

    def columns(n):
        return pl.ds(pl.multiple_of(n * 512, 512), 512)

    @pl.loop(0, 3)
    def _(n):
        cs = columns(n)
        af[own, cs] = gram[:, cs].astype(BF16)
        send_two(af, pa_s, pa_r, n)

    def poly_step():
        mid[own, :] = dot(af[own, own], af[own, :])
        wait_recv(af, pa_s, pa_r)

        @pl.loop(0, 3)
        def _(n):
            cs = columns(n)
            acc = mid[own, cs] + dot(af[own, oth], af[oth_rows, cs])
            bff[own, cs] = (COEF_B * af[own, cs].astype(F32) + COEF_C * acc).astype(BF16)
            send_two(bff, pb_s, pb_r, n)

    def low_part(src, high):
        @pl.loop(0, 3)
        def _(n):
            cs = columns(n)
            al[:, cs] = (src[own, cs] - high[own, cs].astype(F32)).astype(BF16)

    @pl.loop(0, NS_STEPS - 1)
    def _(k):
        wide = k == NS_STEPS - 2
        poly_step()
        v = dot(af[both, own], bff[own, :])
        mid[own, :] = COEF_A * gram[...] + v[own]
        mid[xrow, :] = COEF_A * af[xrow, :].astype(F32) + v[xrow]

        @pl.when(wide)
        def _():
            low_part(gram, af)

            @pl.loop(0, 3)
            def _(n):
                cs = columns(n)
                mid[own, cs] = mid[own, cs] + dot(al[:, own], bff[own, cs])

        wait_recv(bff, pb_s, pb_r)
        v = mid[...] + dot(af[both, oth], bff[oth_rows, :])
        mid[...] = v
        tb[...] = v[own].astype(BF16)

        @pl.when(wide)
        def _():
            @pl.loop(0, 3)
            def _(n):
                cs = columns(n)
                v = mid[own, cs] + dot(al[:, oth], bff[oth_rows, cs])
                mid[own, cs] = v
                tb[:, cs] = v.astype(BF16)

            low_part(mid, tb)

        af[xrow, :] = mid[xrow, :].astype(BF16)
        wait_send(af, pa_s, pa_r)

        @pl.loop(0, 3)
        def _(n):
            cs = columns(n)
            v = COEF_A * mid[own, cs] + dot(tb[:, own], bff[own, cs]) + dot(tb[:, oth], bff[oth_rows, cs])
            gram[:, cs] = v

            @pl.when(wide)
            def _():
                gram[:, cs] = gram[:, cs] + dot(al[:, own], bff[own, cs]) + dot(al[:, oth], bff[oth_rows, cs])

            af[own, cs] = gram[:, cs].astype(BF16)
            send_two(af, pa_s, pa_r, n)

        wait_send(bff, pb_s, pb_r)

    poly_step()
    v = dot(af[xrow, own], bff[own, :])
    mid[xrow, :] = COEF_A * af[xrow, :].astype(F32) + v
    wait_recv(bff, pb_s, pb_r)
    mid[xrow, :] = mid[xrow, :] + dot(af[xrow, oth], bff[oth_rows, :])
    wait_send(af, pa_s, pa_r)
    wait_send(bff, pb_s, pb_r)

    @pl.loop(0, 4)
    def _(i):
        v = mid[xrow, pl.ds(pl.multiple_of(i * 384, 384), 384)].astype(BF16).astype(F32).T
        ys[pl.ds(i * 16, 16)] = v.reshape(16, 24, 128).astype(BF16)

    def out_copy(o):
        d = (me + o) % 64
        return rcopy(ys.at[(d + 32 * t) % 64], yr.at[me], out_s.at[o], out_r.at[me], {"data": d})

    @pl.loop(1, 64)
    def _(o):
        out_copy(o).start()

    yr[me] = ys[slot]

    @pl.loop(1, 64)
    def _(o):
        src = (me + 64 - o) % 64
        rcopy(ys.at[0], yr.at[src], out_s.at[o], out_r.at[src], {"data": (me + o) % 64}).wait()

    load_w.wait()

    @pl.loop(0, 16)
    def _(g):
        last = yr[g * 4 + 3].astype(F32)
        for r in range(3):
            x = jnp.where(lane < used, yr[g * 4 + r].astype(F32), pltpu.roll(last, 96 - 32 * r, 1))
            cs = pl.ds(pl.multiple_of((g * 3 + r) * 128, 128), 128)
            wv[:, cs] = wv[:, cs] - LEARN_RATE * (scale * x + WEIGHT_DECAY * wv[:, cs])

    store_w = pltpu.make_async_copy(wv, w_out, in_s.at[4])
    store_w.start()
    store_w.wait()
    store_m.wait()


def solution(mesh):
    data_size = mesh.shape["data"]
    tp_size = mesh.shape["tp"]
    part_spec = P(("stage", "data"), "tp")

    def local_step(weight, momentum, gradient):
        rows_local, cols_local = gradient.shape
        rows = rows_local * data_size
        sem = pltpu.SemaphoreType.DMA
        shapes = [
            pltpu.VMEM((24, 6144), F32), pltpu.VMEM((24, 6144), F32), pltpu.VMEM((24, 6144), BF16),
            pltpu.VMEM((64, 24, 128), F32), pltpu.VMEM((64, 24, 128), F32), pltpu.VMEM((2, 8, 128), F32), pltpu.VMEM((1536, 256), BF16),
            pltpu.VMEM((3, 4, 16, 32, 128), F32), pltpu.VMEM((3, 3, 16, 32, 128), F32), pltpu.VMEM((3, 4, 4, 32, 128), F32),
            pltpu.VMEM((3, 3, 4, 32, 128), F32), pltpu.VMEM((3, 4, 32, 128), F32), pltpu.VMEM((3, 3, 32, 128), F32),
            pltpu.VMEM((3, 4, 4, 4, 32, 128), F32), pltpu.VMEM((3, 4, 4, 32, 128), F32),
            pltpu.VMEM((768, 1536), F32), pltpu.VMEM((896, 1536), F32), pltpu.VMEM((1664, 1536), BF16), pltpu.VMEM((1664, 1536), BF16),
            pltpu.VMEM((768, 1536), BF16), pltpu.VMEM((768, 1536), BF16),
            pltpu.VMEM((64, 24, 128), BF16), pltpu.VMEM((64, 24, 128), BF16),
            sem((5,)), sem((64,)), sem((64,)), sem, sem, sem((2,)), sem((2,)), sem((27,)), sem((27,)), sem((27,)), sem((27,)),
            sem((3,)), sem((3,)), sem((6,)), sem((6,)), sem((6,)), sem((6,)), sem((64,)), sem((64,)),
        ]
        rms_scale = 0.2 * math.sqrt(max(rows, cols_local * tp_size))
        anywhere = pl.BlockSpec(memory_space=pl.ANY)
        full = jax.ShapeDtypeStruct((rows_local, cols_local), F32)
        return pl.pallas_call(
            functools.partial(kernel, rms_scale),
            out_shape=(full, full),
            in_specs=[anywhere] * 3,
            out_specs=(anywhere, anywhere),
            scratch_shapes=shapes,
            compiler_params=pltpu.CompilerParams(collective_id=0, has_side_effects=True, vmem_limit_bytes=60 * 1024 * 1024),
            name="muon_steps",
        )(weight, momentum, gradient)

    return jax.shard_map(local_step, mesh=mesh, in_specs=(part_spec, part_spec, part_spec), out_specs=(part_spec, part_spec), check_vma=False)
```

```python
import functools
import math
import jax
import jax.numpy as jnp
from jax import lax
from jax.experimental import pallas as pl
from jax.experimental.pallas import tpu as pltpu
from jax.sharding import PartitionSpec as P

NS_STEPS = 5
MOMENTUM = 0.95
LEARN_RATE = 0.5
WEIGHT_DECAY = 0.1
COEF_A = 3.4445
COEF_B = -4.7750
COEF_C = 2.0315
EPSILON = 1e-7

MESH = pl.DeviceIdType.MESH
F32 = jnp.float32
BF16 = jnp.bfloat16
BLOCKS = ((0, 0), (1, 0), (1, 1), (2, 0), (2, 1), (2, 2), (0, 3), (0, 4), (0, 5), (1, 4), (1, 5), (2, 5))
SWAPPED = (7, 8, 10)
STRIDES = (1, 4, 16)


def dot(p, q):
    return jnp.dot(p, q, preferred_element_type=F32)


def kernel(m_hbm, g_hbm, x_out, mv, gv, nb, rx, sq, xg, part, rb1, s1, rb2, s2, rb3, gath, swap, gram, mid, af, bff, dv, tb, ys, yr,
           in_s, dv_s, dv_r, a2a_s, a2a_r, sq_s, sq_r, xg_s, xg_r, rs_s, rs_r, ag_s, ag_r, sw_s, sw_r, pa_s, pa_r, pb_s, pb_r, out_s, out_r):
    me = lax.axis_index("data")
    t = lax.axis_index("tp")
    sib = {"tp": 1 - t}
    coord = (me % 4, (me // 4) % 4, me // 16)
    rows_src, lanes = nb.shape[1:]
    used = 96
    half = 768
    own = slice(0, half)
    xrow = slice(half, half + used)
    both = slice(0, half + used)
    oth = slice(half, 2 * half)
    oth_rows = slice(half + used, 2 * half + used)

    def rcopy(src, dst, ssem, rsem, dev):
        return pltpu.make_async_remote_copy(src_ref=src, dst_ref=dst, send_sem=ssem, recv_sem=rsem, device_id=dev, device_id_type=MESH)

    barrier = pltpu.get_barrier_semaphore()

    @pl.loop(1, 64)
    def _(o):
        pl.semaphore_signal(barrier, inc=1, device_id={"data": (me + o) % 64}, device_id_type=MESH)

    pl.semaphore_signal(barrier, inc=1, device_id=sib, device_id_type=MESH)

    load_m = pltpu.make_async_copy(m_hbm, mv, in_s.at[0])
    load_g = pltpu.make_async_copy(g_hbm, gv, in_s.at[1])
    load_m.start()
    load_g.start()
    load_m.wait()
    load_g.wait()
    lane = lax.broadcasted_iota(jnp.int32, (rows_src, lanes), 1)

    def group(g, ssq):
        tiles = []
        for r in range(3):
            cs = pl.ds(pl.multiple_of((g * 3 + r) * 128, 128), 128)
            grad = gv[:, cs].astype(F32)
            new_mom = MOMENTUM * mv[:, cs] + grad
            nest = grad + MOMENTUM * new_mom
            nb[g * 4 + r] = nest
            ssq = ssq + nest * nest
            tiles.append(pltpu.roll(nest, 32 * (r + 1), 1))
        nb[g * 4 + 3] = jnp.where(lane < 32, tiles[0], jnp.where(lane < 64, tiles[1], tiles[2]))
        return ssq

    ssq = lax.fori_loop(0, 16, group, jnp.zeros((rows_src, lanes), F32))
    ssq = jnp.sum(jnp.sum(ssq, axis=0, keepdims=True), axis=1, keepdims=True)
    lane8 = lax.broadcasted_iota(jnp.int32, (8, lanes), 1)

    @pl.loop(0, 64)
    def _(d):
        nb[d, 0:8] = jnp.where(lane8 < used, nb[d, 0:8], ssq)

    pl.semaphore_wait(barrier, 64)

    slot = (me + 32 * t) % 64

    def a2a_copy(o):
        d = (me + o) % 64
        return rcopy(nb.at[d], rx.at[slot], a2a_s.at[o], a2a_r.at[slot], {"data": d})

    @pl.loop(1, 64)
    def _(o):
        a2a_copy(o).start()

    rx[slot] = nb[me]

    @pl.loop(1, 64)
    def _(o):
        src = ((me + 64 - o) % 64 + 32 * t) % 64
        rcopy(nb.at[0], rx.at[src], a2a_s.at[o], a2a_r.at[src], {"data": (me + o) % 64}).wait()

    sq[0] = jnp.sum(rx[:, 0:8, :], axis=0)
    c = rcopy(sq.at[0], sq.at[1], sq_s, sq_r, sib)
    c.start()
    c.wait()
    total = (sq[0] + sq[1])[0:1, lanes - 1:lanes]
    norm = jnp.sqrt(total) + EPSILON
    lane_ok = lax.broadcasted_iota(jnp.int32, (384, lanes), 1) < used

    @pl.loop(0, 4)
    def _(i):
        v = rx[pl.ds(i * 16, 16)].reshape(384, lanes)
        x = jnp.where(lane_ok, v / norm, 0.0).astype(BF16)
        xg[pl.ds(pl.multiple_of(i * 384, 384), 384), 0:128] = x
        af[xrow, pl.ds(pl.multiple_of(i * 384, 384), 384)] = x.astype(F32).T[0:used].astype(BF16)

    def xg_copy(h):
        return rcopy(xg.at[pl.ds(h * half, half), pl.ds(0, 128)], xg.at[pl.ds((1 - h) * half, half), pl.ds(128, 128)], xg_s.at[h], xg_r.at[h], sib)

    for h in range(2):
        xg_copy(h).start()
    for h in range(2):
        xg_copy(h).wait()

    def peer(dim, o):
        m = coord[dim]
        return {"data": me + ((m + o) % 4 - m) * STRIDES[dim]}

    def dims(col):
        return col, (col + 1) % 3, (col + 2) % 3

    def rs_copy(col, ph, o):
        d = dims(col)[ph]
        j = (coord[d] + o) % 4
        src = (part, s1, s2)[ph].at[col, j]
        dst = (rb1, rb2, rb3)[ph].at[col, o - 1]
        k = (ph * 3 + col) * 3 + o - 1
        return rcopy(src, dst, rs_s.at[k], rs_r.at[k], peer(d, o))

    def ag_ref(col, ph):
        m1, m2, m3 = (coord[d] for d in dims(col))
        return (gath.at[col, m1, m2, m3], gath.at[col, m1, m2], gath.at[col, m1])[ph]

    def ag_copy(col, ph, o):
        d = dims(col)[2 - ph]
        k = (ph * 3 + col) * 3 + o - 1
        return rcopy(ag_ref(col, ph), ag_ref(col, ph), ag_s.at[k], ag_r.at[k], peer(d, o))

    for col in range(3):
        for b in range(4):
            i, j = BLOCKS[col * 4 + b]
            res = lax.dot_general(xg[i * 256:(i + 1) * 256, :], xg[j * 256:(j + 1) * 256, :], (((1,), (1,)), ((), ())), preferred_element_type=F32)
            for h in range(2):
                part[col, b, h * 8:(h + 1) * 8] = res[:, h * 128:(h + 1) * 128].reshape(8, 32, 128)
        for o in range(1, 4):
            rs_copy(col, 0, o).start()
    for ph in range(3):
        for col in range(3):
            for o in range(1, 4):
                rs_copy(col, ph, o).wait()
            m1, m2, m3 = (coord[d] for d in dims(col))
            if ph == 0:
                s1[col] = (part[col, m1] + rb1[col, 0] + rb1[col, 1] + rb1[col, 2]).reshape(4, 4, 32, 128)
            elif ph == 1:
                s2[col] = s1[col, m2] + rb2[col, 0] + rb2[col, 1] + rb2[col, 2]
            else:
                gath[col, m1, m2, m3] = s2[col, m3] + rb3[col, 0] + rb3[col, 1] + rb3[col, 2]
            for o in range(1, 4):
                if ph < 2:
                    rs_copy(col, ph + 1, o).start()
                else:
                    ag_copy(col, 0, o).start()
    for ph in range(3):
        for col in range(3):
            for o in range(1, 4):
                ag_copy(col, ph, o).wait()
            if ph < 2:
                for o in range(1, 4):
                    ag_copy(col, ph + 1, o).start()

    def swap_copy(n):
        q = SWAPPED[n]
        return rcopy(gath.at[q // 4, q % 4], swap.at[n], sw_s.at[n], sw_r.at[n], sib)

    for n in range(3):
        swap_copy(n).start()

    def put(i, j, h, v):
        gram[i * 256:(i + 1) * 256, j * 256 + h * 128:j * 256 + (h + 1) * 128] = v

    def put_t(i, j, h, v):
        gram[i * 256 + h * 128:i * 256 + (h + 1) * 128, j * 256:(j + 1) * 256] = v.T

    for q, (i, j) in enumerate(BLOCKS):
        for h in range(2):
            v = gath[q // 4, q % 4, 2 * h:2 * h + 2].reshape(256, 128)
            put(i, j, h, v)
            if j < i:
                put_t(j, i, h, v)
    for n in range(3):
        swap_copy(n).wait()
        i, j = BLOCKS[SWAPPED[n]]
        for h in range(2):
            put_t(j - 3, i + 3, h, swap[n, 2 * h:2 * h + 2].reshape(256, 128))

    def piece(buf, ssem, rsem, p):
        q = (p + 3) % 6
        base = buf.shape[0] - half
        return rcopy(buf.at[pl.ds(0, half), pl.ds(pl.multiple_of(p * 256, 256), 256)],
                     buf.at[pl.ds(base, half), pl.ds(pl.multiple_of(q * 256, 256), 256)], ssem.at[p], rsem.at[p], sib)

    def send_two(buf, ssem, rsem, n):
        piece(buf, ssem, rsem, 2 * n).start()
        piece(buf, ssem, rsem, 2 * n + 1).start()

    def wait_recv(buf, ssem, rsem):
        for p in range(6):
            piece(buf, ssem, rsem, p).wait_recv()

    def wait_send(buf, ssem, rsem):
        for p in range(6):
            piece(buf, ssem, rsem, p).wait_send()

    def diag_copy():
        return rcopy(dv.at[:, pl.ds(0, half)], dv.at[:, pl.ds(half, half)], dv_s, dv_r, sib)

    def columns(n):
        return pl.ds(pl.multiple_of(n * 512, 512), 512)

    @pl.loop(0, 3)
    def _(n):
        cs = columns(n)
        af[own, cs] = gram[:, cs].astype(BF16)
        send_two(af, pa_s, pa_r, n)

    diag = lax.broadcasted_iota(jnp.int32, (128, 128), 0) == lax.broadcasted_iota(jnp.int32, (128, 128), 1)

    def poly_step():
        mid[own, :] = dot(af[own, own], af[own, :])
        wait_recv(af, pa_s, pa_r)

        @pl.loop(0, 3)
        def _(n):
            cs = columns(n)
            acc = mid[own, cs] + dot(af[own, oth], af[oth_rows, cs])
            bff[own, cs] = (COEF_B * af[own, cs].astype(F32) + COEF_C * acc).astype(BF16)

            @pl.when(n < 2)
            def _():
                @pl.loop(4 * n, 4 * n + 4 - 2 * n)
                def _(i):
                    ts = pl.ds(pl.multiple_of(i * 128, 128), 128)
                    tile = bff[ts, ts].astype(F32)
                    on = jnp.sum(jnp.where(diag, tile, 0.0), axis=0, keepdims=True)
                    dv[:, ts] = jnp.broadcast_to(COEF_A + on, (8, 128))
                    bff[ts, ts] = jnp.where(diag, 0.0, tile).astype(BF16)

            send_two(bff, pb_s, pb_r, n)

        diag_copy().start()

    @pl.loop(0, NS_STEPS - 1)
    def _(k):
        poly_step()
        mid[both, :] = dot(af[both, own], bff[own, :])
        wait_recv(bff, pb_s, pb_r)
        diag_copy().wait_recv()
        v = mid[both, :] + dot(af[both, oth], bff[oth, :])
        q_diag = dv[0:1, :]
        top = v[own] + gram[...] * q_diag
        mid[own, :] = top
        tb[...] = top.astype(BF16)
        x_new = (v[xrow] + af[xrow, :].astype(F32) * q_diag).astype(BF16)
        wait_send(af, pa_s, pa_r)
        af[xrow, :] = x_new

        @pl.loop(0, 3)
        def _(n):
            cs = columns(n)
            v = mid[own, cs] * dv[0:1, cs] + dot(tb[...], bff[:, cs])
            gram[:, cs] = v
            af[own, cs] = v.astype(BF16)
            send_two(af, pa_s, pa_r, n)

        wait_send(bff, pb_s, pb_r)
        diag_copy().wait_send()

    poly_step()
    mid[xrow, :] = dot(af[xrow, own], bff[own, :])
    wait_recv(bff, pb_s, pb_r)
    diag_copy().wait_recv()
    mid[xrow, :] = mid[xrow, :] + af[xrow, :].astype(F32) * dv[0:1, :] + dot(af[xrow, oth], bff[oth, :])
    wait_send(af, pa_s, pa_r)
    wait_send(bff, pb_s, pb_r)
    diag_copy().wait_send()

    @pl.loop(0, 4)
    def _(i):
        v = mid[xrow, pl.ds(pl.multiple_of(i * 384, 384), 384)].astype(BF16).astype(F32)
        v = jnp.concatenate([v, jnp.zeros((lanes - used, 384), F32)], axis=0).T
        ys[pl.ds(i * 16, 16)] = v.reshape(16, 24, 128).astype(BF16)

    def out_copy(o):
        d = (me + o) % 64
        return rcopy(ys.at[(d + 32 * t) % 64], yr.at[me], out_s.at[o], out_r.at[me], {"data": d})

    @pl.loop(1, 64)
    def _(o):
        out_copy(o).start()

    yr[me] = ys[slot]

    @pl.loop(1, 64)
    def _(o):
        src = (me + 64 - o) % 64
        rcopy(ys.at[0], yr.at[src], out_s.at[o], out_r.at[src], {"data": (me + o) % 64}).wait()

    @pl.loop(0, 16)
    def _(g):
        last = yr[g * 4 + 3].astype(F32)
        for r in range(3):
            x = jnp.where(lane < used, yr[g * 4 + r].astype(F32), pltpu.roll(last, 96 - 32 * r, 1))
            x_out[:, pl.ds(pl.multiple_of((g * 3 + r) * 128, 128), 128)] = x.astype(BF16)


def solution(mesh):
    data_size = mesh.shape["data"]
    tp_size = mesh.shape["tp"]
    part_spec = P(("stage", "data"), "tp")

    def local_step(weight, momentum, gradient):
        rows_local, cols_local = gradient.shape
        rows = rows_local * data_size
        sem = pltpu.SemaphoreType.DMA
        shapes = [
            pltpu.VMEM((24, 6144), F32), pltpu.VMEM((24, 6144), BF16),
            pltpu.VMEM((64, 24, 128), F32), pltpu.VMEM((64, 24, 128), F32), pltpu.VMEM((2, 8, 128), F32), pltpu.VMEM((1536, 256), BF16),
            pltpu.VMEM((3, 4, 16, 32, 128), F32), pltpu.VMEM((3, 3, 16, 32, 128), F32), pltpu.VMEM((3, 4, 4, 32, 128), F32),
            pltpu.VMEM((3, 3, 4, 32, 128), F32), pltpu.VMEM((3, 4, 32, 128), F32), pltpu.VMEM((3, 3, 32, 128), F32),
            pltpu.VMEM((3, 4, 4, 4, 32, 128), F32), pltpu.VMEM((3, 4, 4, 32, 128), F32),
            pltpu.VMEM((768, 1536), F32), pltpu.VMEM((864, 1536), F32), pltpu.VMEM((1632, 1536), BF16), pltpu.VMEM((1536, 1536), BF16),
            pltpu.VMEM((8, 1536), F32), pltpu.VMEM((768, 1536), BF16),
            pltpu.VMEM((64, 24, 128), BF16), pltpu.VMEM((64, 24, 128), BF16),
            sem((2,)), sem, sem, sem((64,)), sem((64,)), sem, sem, sem((2,)), sem((2,)), sem((27,)), sem((27,)), sem((27,)), sem((27,)),
            sem((3,)), sem((3,)), sem((6,)), sem((6,)), sem((6,)), sem((6,)), sem((64,)), sem((64,)),
        ]
        anywhere = pl.BlockSpec(memory_space=pl.ANY)
        x_fin = pl.pallas_call(
            kernel,
            out_shape=jax.ShapeDtypeStruct((rows_local, cols_local), BF16),
            in_specs=[anywhere] * 2,
            out_specs=pl.BlockSpec(memory_space=pltpu.VMEM),
            scratch_shapes=shapes,
            compiler_params=pltpu.CompilerParams(collective_id=0, has_side_effects=True, vmem_limit_bytes=60 * 1024 * 1024),
            name="muon_steps",
        )(momentum, gradient)
        new_mom = MOMENTUM * momentum + gradient.astype(F32)
        rms_scale = 0.2 * math.sqrt(max(rows, cols_local * tp_size))
        new_weight = weight - LEARN_RATE * (rms_scale * x_fin.astype(F32) + WEIGHT_DECAY * weight)
        return new_weight, new_mom

    return jax.shard_map(local_step, mesh=mesh, in_specs=(part_spec, part_spec, part_spec), out_specs=(part_spec, part_spec), check_vma=False)
```

```python
import functools
import math
import jax
import jax.numpy as jnp
from jax import lax
from jax.experimental import pallas as pl
from jax.experimental.pallas import tpu as pltpu
from jax.sharding import PartitionSpec as P

NS_STEPS = 5
MOMENTUM = 0.95
LEARN_RATE = 0.5
WEIGHT_DECAY = 0.1
COEF_A = 3.4445
COEF_B = -4.7750
COEF_C = 2.0315
EPSILON = 1e-7

MESH = pl.DeviceIdType.MESH
F32 = jnp.float32
BF16 = jnp.bfloat16
BLOCKS = ((0, 0), (1, 0), (1, 1), (2, 0), (2, 1), (2, 2), (0, 3), (0, 4), (0, 5), (1, 4), (1, 5), (2, 5))
SWAPPED = (7, 8, 10)
STRIDES = (1, 4, 16)


def dot(p, q):
    return jnp.dot(p, q, preferred_element_type=F32)


def kernel(m_hbm, g_hbm, x_out, mv, gv, nb, rx, sq, xg, part, rb1, s1, rb2, s2, rb3, gath, swap, gram, mid, af, bff, dv, tb, ys, yr,
           in_s, dv_s, dv_r, a2a_s, a2a_r, sq_s, sq_r, xg_s, xg_r, rs_s, rs_r, ag_s, ag_r, sw_s, sw_r, pa_s, pa_r, pb_s, pb_r, out_s, out_r):
    me = lax.axis_index("data")
    t = lax.axis_index("tp")
    sib = {"tp": 1 - t}
    coord = (me % 4, (me // 4) % 4, me // 16)
    rows_src, lanes = nb.shape[1:]
    used = 96
    half = 768
    own = slice(0, half)
    xrow = slice(half, half + used)
    both = slice(0, half + used)
    oth = slice(half, 2 * half)
    oth_rows = slice(half + used, 2 * half + used)

    def rcopy(src, dst, ssem, rsem, dev):
        return pltpu.make_async_remote_copy(src_ref=src, dst_ref=dst, send_sem=ssem, recv_sem=rsem, device_id=dev, device_id_type=MESH)

    barrier = pltpu.get_barrier_semaphore()

    @pl.loop(1, 64)
    def _(o):
        pl.semaphore_signal(barrier, inc=1, device_id={"data": (me + o) % 64}, device_id_type=MESH)

    pl.semaphore_signal(barrier, inc=1, device_id=sib, device_id_type=MESH)

    load_m = pltpu.make_async_copy(m_hbm, mv, in_s.at[0])
    load_g = pltpu.make_async_copy(g_hbm, gv, in_s.at[1])
    load_m.start()
    load_g.start()
    load_m.wait()
    load_g.wait()
    lane = lax.broadcasted_iota(jnp.int32, (rows_src, lanes), 1)

    def group(g, ssq):
        tiles = []
        for r in range(3):
            cs = pl.ds(pl.multiple_of((g * 3 + r) * 128, 128), 128)
            grad = gv[:, cs].astype(F32)
            new_mom = MOMENTUM * mv[:, cs] + grad
            nest = grad + MOMENTUM * new_mom
            nb[g * 4 + r] = nest
            ssq = ssq + nest * nest
            tiles.append(pltpu.roll(nest, 32 * (r + 1), 1))
        nb[g * 4 + 3] = jnp.where(lane < 32, tiles[0], jnp.where(lane < 64, tiles[1], tiles[2]))
        return ssq

    ssq = lax.fori_loop(0, 16, group, jnp.zeros((rows_src, lanes), F32))
    ssq = jnp.sum(jnp.sum(ssq, axis=0, keepdims=True), axis=1, keepdims=True)
    lane8 = lax.broadcasted_iota(jnp.int32, (8, lanes), 1)

    @pl.loop(0, 64)
    def _(d):
        nb[d, 0:8] = jnp.where(lane8 < used, nb[d, 0:8], ssq)

    pl.semaphore_wait(barrier, 64)

    slot = (me + 32 * t) % 64

    def a2a_copy(o):
        d = (me + o) % 64
        return rcopy(nb.at[d], rx.at[slot], a2a_s, a2a_r, {"data": d})

    @pl.loop(1, 64)
    def _(o):
        a2a_copy(o).start()

    rx[slot] = nb[me]

    rcopy(nb.at[pl.ds(0, 63)], rx.at[pl.ds(0, 63)], a2a_s, a2a_r, sib).wait()

    sq[0] = jnp.sum(rx[:, 0:8, :], axis=0)
    c = rcopy(sq.at[0], sq.at[1], sq_s, sq_r, sib)
    c.start()
    c.wait()
    total = (sq[0] + sq[1])[0:1, lanes - 1:lanes]
    norm = jnp.sqrt(total) + EPSILON
    lane_ok = lax.broadcasted_iota(jnp.int32, (384, lanes), 1) < used

    @pl.loop(0, 4)
    def _(i):
        v = rx[pl.ds(i * 16, 16)].reshape(384, lanes)
        x = jnp.where(lane_ok, v / norm, 0.0).astype(BF16)
        xg[pl.ds(pl.multiple_of(i * 384, 384), 384), 0:128] = x
        af[xrow, pl.ds(pl.multiple_of(i * 384, 384), 384)] = x.astype(F32).T[0:used].astype(BF16)

    def xg_copy(h):
        return rcopy(xg.at[pl.ds(h * half, half), pl.ds(0, 128)], xg.at[pl.ds((1 - h) * half, half), pl.ds(128, 128)], xg_s, xg_r, sib)

    for h in range(2):
        xg_copy(h).start()
    rcopy(xg.at[:, pl.ds(0, 128)], xg.at[:, pl.ds(128, 128)], xg_s, xg_r, sib).wait()

    def peer(dim, o):
        m = coord[dim]
        return {"data": me + ((m + o) % 4 - m) * STRIDES[dim]}

    def dims(col):
        return col, (col + 1) % 3, (col + 2) % 3

    def rs_copy(col, ph, o):
        d = dims(col)[ph]
        j = (coord[d] + o) % 4
        src = (part, s1, s2)[ph].at[col, j]
        dst = (rb1, rb2, rb3)[ph].at[col, o - 1]
        k = ph * 3 + col
        return rcopy(src, dst, rs_s.at[k], rs_r.at[k], peer(d, o))

    def rs_wait(col, ph):
        k = ph * 3 + col
        three = (rb1, rb2, rb3)[ph].at[col]
        rcopy(three, three, rs_s.at[k], rs_r.at[k], sib).wait()

    def ag_ref(col, ph):
        m1, m2, m3 = (coord[d] for d in dims(col))
        return (gath.at[col, m1, m2, m3], gath.at[col, m1, m2], gath.at[col, m1])[ph]

    def ag_copy(col, ph, o):
        d = dims(col)[2 - ph]
        k = ph * 3 + col
        return rcopy(ag_ref(col, ph), ag_ref(col, ph), ag_s.at[k], ag_r.at[k], peer(d, o))

    def ag_wait(col, ph):
        k = ph * 3 + col
        first = pl.ds(0, 3)
        three = (gath.at[col, 0, 0, first], gath.at[col, 0, first], gath.at[col, first])[ph]
        rcopy(three, three, ag_s.at[k], ag_r.at[k], sib).wait()

    for col in range(3):
        for b in range(4):
            i, j = BLOCKS[col * 4 + b]
            res = lax.dot_general(xg[i * 256:(i + 1) * 256, :], xg[j * 256:(j + 1) * 256, :], (((1,), (1,)), ((), ())), preferred_element_type=F32)
            for h in range(2):
                part[col, b, h * 8:(h + 1) * 8] = res[:, h * 128:(h + 1) * 128].reshape(8, 32, 128)
        for o in range(1, 4):
            rs_copy(col, 0, o).start()
    for ph in range(3):
        for col in range(3):
            rs_wait(col, ph)
            m1, m2, m3 = (coord[d] for d in dims(col))
            if ph == 0:
                s1[col] = (part[col, m1] + rb1[col, 0] + rb1[col, 1] + rb1[col, 2]).reshape(4, 4, 32, 128)
            elif ph == 1:
                s2[col] = s1[col, m2] + rb2[col, 0] + rb2[col, 1] + rb2[col, 2]
            else:
                gath[col, m1, m2, m3] = s2[col, m3] + rb3[col, 0] + rb3[col, 1] + rb3[col, 2]
            for o in range(1, 4):
                if ph < 2:
                    rs_copy(col, ph + 1, o).start()
                else:
                    ag_copy(col, 0, o).start()
    for ph in range(3):
        for col in range(3):
            ag_wait(col, ph)
            if ph < 2:
                for o in range(1, 4):
                    ag_copy(col, ph + 1, o).start()

    def swap_copy(n):
        q = SWAPPED[n]
        return rcopy(gath.at[q // 4, q % 4], swap.at[n], sw_s, sw_r, sib)

    for n in range(3):
        swap_copy(n).start()

    def put(i, j, h, v):
        gram[i * 256:(i + 1) * 256, j * 256 + h * 128:j * 256 + (h + 1) * 128] = v

    def put_t(i, j, h, v):
        gram[i * 256 + h * 128:i * 256 + (h + 1) * 128, j * 256:(j + 1) * 256] = v.T

    for q, (i, j) in enumerate(BLOCKS):
        for h in range(2):
            v = gath[q // 4, q % 4, 2 * h:2 * h + 2].reshape(256, 128)
            put(i, j, h, v)
            if j < i:
                put_t(j, i, h, v)
    rcopy(swap, swap, sw_s, sw_r, sib).wait()
    for n in range(3):
        i, j = BLOCKS[SWAPPED[n]]
        for h in range(2):
            put_t(j - 3, i + 3, h, swap[n, 2 * h:2 * h + 2].reshape(256, 128))

    def piece(buf, ssem, rsem, p):
        q = (p + 3) % 6
        base = buf.shape[0] - half
        return rcopy(buf.at[pl.ds(0, half), pl.ds(pl.multiple_of(p * 256, 256), 256)],
                     buf.at[pl.ds(base, half), pl.ds(pl.multiple_of(q * 256, 256), 256)], ssem, rsem, sib)

    def send_two(buf, ssem, rsem, n):
        piece(buf, ssem, rsem, 2 * n).start()
        piece(buf, ssem, rsem, 2 * n + 1).start()

    def wait_recv(buf, ssem, rsem):
        rcopy(buf.at[pl.ds(0, half)], buf.at[pl.ds(0, half)], ssem, rsem, sib).wait_recv()

    def wait_send(buf, ssem, rsem):
        rcopy(buf.at[pl.ds(0, half)], buf.at[pl.ds(0, half)], ssem, rsem, sib).wait_send()

    def diag_copy():
        return rcopy(dv.at[:, pl.ds(0, half)], dv.at[:, pl.ds(half, half)], dv_s, dv_r, sib)

    def columns(n):
        return pl.ds(pl.multiple_of(n * 512, 512), 512)

    @pl.loop(0, 3)
    def _(n):
        cs = columns(n)
        af[own, cs] = gram[:, cs].astype(BF16)
        send_two(af, pa_s, pa_r, n)

    diag = lax.broadcasted_iota(jnp.int32, (128, 128), 0) == lax.broadcasted_iota(jnp.int32, (128, 128), 1)

    def poly_step():
        mid[own, :] = dot(af[own, own], af[own, :])
        wait_recv(af, pa_s, pa_r)

        @pl.loop(0, 3)
        def _(n):
            cs = columns(n)
            acc = mid[own, cs] + dot(af[own, oth], af[oth_rows, cs])
            bff[own, cs] = (COEF_B * af[own, cs].astype(F32) + COEF_C * acc).astype(BF16)

            @pl.when(n < 2)
            def _():
                @pl.loop(4 * n, 4 * n + 4 - 2 * n)
                def _(i):
                    ts = pl.ds(pl.multiple_of(i * 128, 128), 128)
                    tile = bff[ts, ts].astype(F32)
                    on = jnp.sum(jnp.where(diag, tile, 0.0), axis=0, keepdims=True)
                    dv[:, ts] = jnp.broadcast_to(COEF_A + on, (8, 128))
                    bff[ts, ts] = jnp.where(diag, 0.0, tile).astype(BF16)

            send_two(bff, pb_s, pb_r, n)

        diag_copy().start()

    @pl.loop(0, NS_STEPS - 1)
    def _(k):
        poly_step()
        mid[both, :] = dot(af[both, own], bff[own, :])
        wait_recv(bff, pb_s, pb_r)
        diag_copy().wait_recv()
        v = mid[both, :] + dot(af[both, oth], bff[oth, :])
        q_diag = dv[0:1, :]
        top = v[own] + gram[...] * q_diag
        mid[own, :] = top
        tb[...] = top.astype(BF16)
        x_new = (v[xrow] + af[xrow, :].astype(F32) * q_diag).astype(BF16)
        wait_send(af, pa_s, pa_r)
        af[xrow, :] = x_new

        @pl.loop(0, 3)
        def _(n):
            cs = columns(n)
            v = mid[own, cs] * dv[0:1, cs] + dot(tb[...], bff[:, cs])
            gram[:, cs] = v
            af[own, cs] = v.astype(BF16)
            send_two(af, pa_s, pa_r, n)

        wait_send(bff, pb_s, pb_r)
        diag_copy().wait_send()

    poly_step()
    mid[xrow, :] = dot(af[xrow, own], bff[own, :])
    wait_recv(bff, pb_s, pb_r)
    diag_copy().wait_recv()
    mid[xrow, :] = mid[xrow, :] + af[xrow, :].astype(F32) * dv[0:1, :] + dot(af[xrow, oth], bff[oth, :])
    wait_send(af, pa_s, pa_r)
    wait_send(bff, pb_s, pb_r)
    diag_copy().wait_send()

    @pl.loop(0, 4)
    def _(i):
        v = mid[xrow, pl.ds(pl.multiple_of(i * 384, 384), 384)].astype(BF16).astype(F32)
        v = jnp.concatenate([v, jnp.zeros((lanes - used, 384), F32)], axis=0).T
        ys[pl.ds(i * 16, 16)] = v.reshape(16, 24, 128).astype(BF16)

    def out_copy(o):
        d = (me + o) % 64
        return rcopy(ys.at[(d + 32 * t) % 64], yr.at[me], out_s, out_r, {"data": d})

    @pl.loop(1, 64)
    def _(o):
        out_copy(o).start()

    yr[me] = ys[slot]

    rcopy(ys.at[pl.ds(0, 63)], yr.at[pl.ds(0, 63)], out_s, out_r, sib).wait()

    @pl.loop(0, 16)
    def _(g):
        last = yr[g * 4 + 3].astype(F32)
        for r in range(3):
            x = jnp.where(lane < used, yr[g * 4 + r].astype(F32), pltpu.roll(last, 96 - 32 * r, 1))
            x_out[:, pl.ds(pl.multiple_of((g * 3 + r) * 128, 128), 128)] = x.astype(BF16)


def solution(mesh):
    data_size = mesh.shape["data"]
    tp_size = mesh.shape["tp"]
    part_spec = P(("stage", "data"), "tp")

    def local_step(weight, momentum, gradient):
        rows_local, cols_local = gradient.shape
        rows = rows_local * data_size
        sem = pltpu.SemaphoreType.DMA
        shapes = [
            pltpu.VMEM((24, 6144), F32), pltpu.VMEM((24, 6144), BF16),
            pltpu.VMEM((64, 24, 128), F32), pltpu.VMEM((64, 24, 128), F32), pltpu.VMEM((2, 8, 128), F32), pltpu.VMEM((1536, 256), BF16),
            pltpu.VMEM((3, 4, 16, 32, 128), F32), pltpu.VMEM((3, 3, 16, 32, 128), F32), pltpu.VMEM((3, 4, 4, 32, 128), F32),
            pltpu.VMEM((3, 3, 4, 32, 128), F32), pltpu.VMEM((3, 4, 32, 128), F32), pltpu.VMEM((3, 3, 32, 128), F32),
            pltpu.VMEM((3, 4, 4, 4, 32, 128), F32), pltpu.VMEM((3, 4, 4, 32, 128), F32),
            pltpu.VMEM((768, 1536), F32), pltpu.VMEM((864, 1536), F32), pltpu.VMEM((1632, 1536), BF16), pltpu.VMEM((1536, 1536), BF16),
            pltpu.VMEM((8, 1536), F32), pltpu.VMEM((768, 1536), BF16),
            pltpu.VMEM((64, 24, 128), BF16), pltpu.VMEM((64, 24, 128), BF16),
            sem((2,)), sem, sem, sem, sem, sem, sem, sem, sem, sem((9,)), sem((9,)), sem((9,)), sem((9,)),
            sem, sem, sem, sem, sem, sem, sem, sem,
        ]
        anywhere = pl.BlockSpec(memory_space=pl.ANY)
        x_fin = pl.pallas_call(
            kernel,
            out_shape=jax.ShapeDtypeStruct((rows_local, cols_local), BF16),
            in_specs=[anywhere] * 2,
            out_specs=pl.BlockSpec(memory_space=pltpu.VMEM),
            scratch_shapes=shapes,
            compiler_params=pltpu.CompilerParams(collective_id=0, has_side_effects=True, vmem_limit_bytes=60 * 1024 * 1024),
            name="muon_steps",
        )(momentum, gradient)
        new_mom = MOMENTUM * momentum + gradient.astype(F32)
        rms_scale = 0.2 * math.sqrt(max(rows, cols_local * tp_size))
        new_weight = weight - LEARN_RATE * (rms_scale * x_fin.astype(F32) + WEIGHT_DECAY * weight)
        return new_weight, new_mom

    return jax.shard_map(local_step, mesh=mesh, in_specs=(part_spec, part_spec, part_spec), out_specs=(part_spec, part_spec), check_vma=False)
```

```python
import functools
import math
import jax
import jax.numpy as jnp
from jax import lax
from jax.experimental import pallas as pl
from jax.experimental.pallas import tpu as pltpu
from jax.sharding import PartitionSpec as P

NS_STEPS = 5
MOMENTUM = 0.95
LEARN_RATE = 0.5
WEIGHT_DECAY = 0.1
COEF_A = 3.4445
COEF_B = -4.7750
COEF_C = 2.0315
EPSILON = 1e-7

MESH = pl.DeviceIdType.MESH
F32 = jnp.float32
BF16 = jnp.bfloat16
BLOCKS = ((0, 0), (1, 0), (1, 1), (2, 0), (2, 1), (2, 2), (0, 3), (0, 4), (0, 5), (1, 4), (1, 5), (2, 5))
SWAPPED = (7, 8, 10)
STRIDES = (1, 4, 16)


def dot(p, q):
    return jnp.dot(p, q, preferred_element_type=F32)


def kernel(m_hbm, g_hbm, x_out, mv, gv, nb, rx, sq, xg, part, rb1, s1, rb2, s2, rb3, gath, swap, gram, mid, af, bff, dv, tb, ys, yr,
           in_s, dv_s, dv_r, a2a_s, a2a_r, sq_s, sq_r, xg_s, xg_r, near_s, near_r, fwd_s, fwd_r, rs_s, rs_r, ag_s, ag_r, sw_s, sw_r, pa_s, pa_r, pb_s, pb_r, out_s, out_r):
    me = lax.axis_index("data")
    t = lax.axis_index("tp")
    sib = {"tp": 1 - t}
    coord = (me % 4, (me // 4) % 4, me // 16)
    rows_src, lanes = nb.shape[1:]
    used = 96
    half = 768
    own = slice(0, half)
    xrow = slice(half, half + used)
    both = slice(0, half + used)
    oth = slice(half, 2 * half)
    oth_rows = slice(half + used, 2 * half + used)

    def rcopy(src, dst, ssem, rsem, dev):
        return pltpu.make_async_remote_copy(src_ref=src, dst_ref=dst, send_sem=ssem, recv_sem=rsem, device_id=dev, device_id_type=MESH)

    barrier = pltpu.get_barrier_semaphore()

    @pl.loop(1, 64)
    def _(o):
        pl.semaphore_signal(barrier, inc=1, device_id={"data": (me + o) % 64}, device_id_type=MESH)

    pl.semaphore_signal(barrier, inc=1, device_id=sib, device_id_type=MESH)

    load_m = pltpu.make_async_copy(m_hbm, mv, in_s.at[0])
    load_g = pltpu.make_async_copy(g_hbm, gv, in_s.at[1])
    load_m.start()
    load_g.start()
    load_m.wait()
    load_g.wait()
    lane = lax.broadcasted_iota(jnp.int32, (rows_src, lanes), 1)

    def group(g, ssq):
        tiles = []
        for r in range(3):
            cs = pl.ds(pl.multiple_of((g * 3 + r) * 128, 128), 128)
            grad = gv[:, cs].astype(F32)
            new_mom = MOMENTUM * mv[:, cs] + grad
            nest = grad + MOMENTUM * new_mom
            nb[g * 4 + r] = nest
            ssq = ssq + nest * nest
            tiles.append(pltpu.roll(nest, 32 * (r + 1), 1))
        nb[g * 4 + 3] = jnp.where(lane < 32, tiles[0], jnp.where(lane < 64, tiles[1], tiles[2]))
        return ssq

    ssq = lax.fori_loop(0, 16, group, jnp.zeros((rows_src, lanes), F32))
    ssq = jnp.sum(jnp.sum(ssq, axis=0, keepdims=True), axis=1, keepdims=True)
    lane8 = lax.broadcasted_iota(jnp.int32, (8, lanes), 1)

    @pl.loop(0, 64)
    def _(d):
        nb[d, 0:8] = jnp.where(lane8 < used, nb[d, 0:8], ssq)

    pl.semaphore_wait(barrier, 64)

    slot = (me + 32 * t) % 64

    def a2a_copy(o):
        d = (me + o) % 64
        return rcopy(nb.at[d], rx.at[slot], a2a_s, a2a_r, {"data": d})

    @pl.loop(1, 64)
    def _(o):
        a2a_copy(o).start()

    rx[slot] = nb[me]

    rcopy(nb.at[pl.ds(0, 63)], rx.at[pl.ds(0, 63)], a2a_s, a2a_r, sib).wait()

    sq[0] = jnp.sum(rx[:, 0:8, :], axis=0)
    c = rcopy(sq.at[0], sq.at[1], sq_s, sq_r, sib)
    c.start()
    c.wait()
    total = (sq[0] + sq[1])[0:1, lanes - 1:lanes]
    norm = jnp.sqrt(total) + EPSILON
    lane_ok = lax.broadcasted_iota(jnp.int32, (384, lanes), 1) < used

    @pl.loop(0, 4)
    def _(i):
        v = rx[pl.ds(i * 16, 16)].reshape(384, lanes)
        x = jnp.where(lane_ok, v / norm, 0.0).astype(BF16)
        xg[pl.ds(pl.multiple_of(i * 384, 384), 384), 0:128] = x
        af[xrow, pl.ds(pl.multiple_of(i * 384, 384), 384)] = x.astype(F32).T[0:used].astype(BF16)

    def xg_copy(h):
        return rcopy(xg.at[pl.ds(h * half, half), pl.ds(0, 128)], xg.at[pl.ds((1 - h) * half, half), pl.ds(128, 128)], xg_s, xg_r, sib)

    for h in range(2):
        xg_copy(h).start()
    rcopy(xg.at[:, pl.ds(0, 128)], xg.at[:, pl.ds(128, 128)], xg_s, xg_r, sib).wait()

    def peer(dim, o):
        m = coord[dim]
        return {"data": me + ((m + o) % 4 - m) * STRIDES[dim]}

    def dims(col):
        return col, (col + 1) % 3, (col + 2) % 3

    def rs_copy(col, ph, o):
        d = dims(col)[ph]
        j = (coord[d] + o) % 4
        src = (part, s1, s2)[ph].at[col, j]
        dst = (rb1, rb2, rb3)[ph].at[col, o - 1]
        k = ph * 3 + col
        return rcopy(src, dst, rs_s.at[k], rs_r.at[k], peer(d, o))

    first, second = pl.ds(0, 8), pl.ds(8, 8)

    def near(col, src, dst, k, o):
        return rcopy(src, dst, near_s.at[col], near_r.at[col * 3 + k], peer(dims(col)[0], o))

    def near_start(col):
        m = coord[dims(col)[0]]
        up, down, far = (m + 1) % 4, (m + 3) % 4, (m + 2) % 4
        near(col, part.at[col, far, first], rb1.at[col, 2, first], 0, 1).start()
        near(col, part.at[col, far, second], rb1.at[col, 2, second], 1, 3).start()
        near(col, part.at[col, up, second], rb1.at[col, 0, second], 2, 1).start()
        near(col, part.at[col, down, first], rb1.at[col, 1, first], 2, 3).start()

    def near_merge(col):
        m = coord[dims(col)[0]]
        up, down = (m + 1) % 4, (m + 3) % 4
        near(col, part.at[col, up, first], rb1.at[col, 2, first], 0, 1).wait_recv()
        part[col, up, first] = part[col, up, first] + rb1[col, 2, first]
        near(col, part.at[col, up, first], rb1.at[col, 0, first], 2, 1).start()
        near(col, part.at[col, down, second], rb1.at[col, 2, second], 1, 3).wait_recv()
        part[col, down, second] = part[col, down, second] + rb1[col, 2, second]
        near(col, part.at[col, down, second], rb1.at[col, 1, second], 2, 3).start()

    def near_wait(col):
        two = rb1.at[col, pl.ds(0, 2)]
        near(col, two, two, 2, 1).wait_recv()
        near(col, rb1.at[col], rb1.at[col], 2, 1).wait_send()

    low, high = pl.ds(0, 2), pl.ds(2, 2)

    def fwd(col, block, rows, k, o):
        ref = gath.at[col, block, rows]
        return rcopy(ref, ref, fwd_s.at[col], fwd_r.at[col * 3 + k], peer(dims(col)[0], o))

    def fwd_start(col):
        m = coord[dims(col)[0]]
        fwd(col, m, low, 0, 1).start()
        fwd(col, m, high, 1, 3).start()
        fwd(col, m, high, 2, 1).start()
        fwd(col, m, low, 2, 3).start()

    def fwd_pass(col):
        m = coord[dims(col)[0]]
        up, down = (m + 1) % 4, (m + 3) % 4
        fwd(col, down, low, 0, 1).wait_recv()
        fwd(col, down, low, 2, 1).start()
        fwd(col, up, high, 1, 3).wait_recv()
        fwd(col, up, high, 2, 3).start()

    def fwd_wait(col):
        two = gath.at[col, pl.ds(0, 2)]
        three = gath.at[col, pl.ds(0, 3)]
        rcopy(two, two, fwd_s.at[col], fwd_r.at[col * 3 + 2], sib).wait_recv()
        rcopy(three, three, fwd_s.at[col], fwd_r.at[col * 3 + 2], sib).wait_send()

    def rs_wait(col, ph):
        k = ph * 3 + col
        three = (rb1, rb2, rb3)[ph].at[col]
        rcopy(three, three, rs_s.at[k], rs_r.at[k], sib).wait()

    def ag_ref(col, ph):
        m1, m2, m3 = (coord[d] for d in dims(col))
        return (gath.at[col, m1, m2, m3], gath.at[col, m1, m2], gath.at[col, m1])[ph]

    def ag_copy(col, ph, o):
        d = dims(col)[2 - ph]
        k = ph * 3 + col
        return rcopy(ag_ref(col, ph), ag_ref(col, ph), ag_s.at[k], ag_r.at[k], peer(d, o))

    def ag_wait(col, ph):
        k = ph * 3 + col
        first = pl.ds(0, 3)
        three = (gath.at[col, 0, 0, first], gath.at[col, 0, first], gath.at[col, first])[ph]
        rcopy(three, three, ag_s.at[k], ag_r.at[k], sib).wait()

    for col in range(3):
        for b in range(4):
            i, j = BLOCKS[col * 4 + b]
            res = lax.dot_general(xg[i * 256:(i + 1) * 256, :], xg[j * 256:(j + 1) * 256, :], (((1,), (1,)), ((), ())), preferred_element_type=F32)
            for h in range(2):
                part[col, b, h * 8:(h + 1) * 8] = res[:, h * 128:(h + 1) * 128].reshape(8, 32, 128)
        near_start(col)
    for col in range(3):
        near_merge(col)
    for ph in range(3):
        for col in range(3):
            if ph == 0:
                near_wait(col)
            else:
                rs_wait(col, ph)
            m1, m2, m3 = (coord[d] for d in dims(col))
            if ph == 0:
                s1[col] = (part[col, m1] + rb1[col, 0] + rb1[col, 1]).reshape(4, 4, 32, 128)
            elif ph == 1:
                s2[col] = s1[col, m2] + rb2[col, 0] + rb2[col, 1] + rb2[col, 2]
            else:
                gath[col, m1, m2, m3] = s2[col, m3] + rb3[col, 0] + rb3[col, 1] + rb3[col, 2]
            for o in range(1, 4):
                if ph < 2:
                    rs_copy(col, ph + 1, o).start()
                else:
                    ag_copy(col, 0, o).start()
    for ph in range(2):
        for col in range(3):
            ag_wait(col, ph)
            if ph == 0:
                for o in range(1, 4):
                    ag_copy(col, 1, o).start()
            else:
                fwd_start(col)
    for col in range(3):
        fwd_pass(col)
    for col in range(3):
        fwd_wait(col)

    def swap_copy(n):
        q = SWAPPED[n]
        return rcopy(gath.at[q // 4, q % 4], swap.at[n], sw_s, sw_r, sib)

    for n in range(3):
        swap_copy(n).start()

    def put(i, j, h, v):
        gram[i * 256:(i + 1) * 256, j * 256 + h * 128:j * 256 + (h + 1) * 128] = v

    def put_t(i, j, h, v):
        gram[i * 256 + h * 128:i * 256 + (h + 1) * 128, j * 256:(j + 1) * 256] = v.T

    for q, (i, j) in enumerate(BLOCKS):
        for h in range(2):
            v = gath[q // 4, q % 4, 2 * h:2 * h + 2].reshape(256, 128)
            put(i, j, h, v)
            if j < i:
                put_t(j, i, h, v)
    rcopy(swap, swap, sw_s, sw_r, sib).wait()
    for n in range(3):
        i, j = BLOCKS[SWAPPED[n]]
        for h in range(2):
            put_t(j - 3, i + 3, h, swap[n, 2 * h:2 * h + 2].reshape(256, 128))

    def piece(buf, ssem, rsem, p):
        q = (p + 3) % 6
        base = buf.shape[0] - half
        return rcopy(buf.at[pl.ds(0, half), pl.ds(pl.multiple_of(p * 256, 256), 256)],
                     buf.at[pl.ds(base, half), pl.ds(pl.multiple_of(q * 256, 256), 256)], ssem, rsem, sib)

    def send_two(buf, ssem, rsem, n):
        piece(buf, ssem, rsem, 2 * n).start()
        piece(buf, ssem, rsem, 2 * n + 1).start()

    def wait_recv(buf, ssem, rsem):
        rcopy(buf.at[pl.ds(0, half)], buf.at[pl.ds(0, half)], ssem, rsem, sib).wait_recv()

    def wait_send(buf, ssem, rsem):
        rcopy(buf.at[pl.ds(0, half)], buf.at[pl.ds(0, half)], ssem, rsem, sib).wait_send()

    def diag_copy():
        return rcopy(dv.at[:, pl.ds(0, half)], dv.at[:, pl.ds(half, half)], dv_s, dv_r, sib)

    def columns(n):
        return pl.ds(pl.multiple_of(n * 512, 512), 512)

    @pl.loop(0, 3)
    def _(n):
        cs = columns(n)
        af[own, cs] = gram[:, cs].astype(BF16)
        send_two(af, pa_s, pa_r, n)

    diag = lax.broadcasted_iota(jnp.int32, (128, 128), 0) == lax.broadcasted_iota(jnp.int32, (128, 128), 1)

    def poly_step():
        mid[own, :] = dot(af[own, own], af[own, :])
        wait_recv(af, pa_s, pa_r)

        @pl.loop(0, 3)
        def _(n):
            cs = columns(n)
            acc = mid[own, cs] + dot(af[own, oth], af[oth_rows, cs])
            bff[own, cs] = (COEF_B * af[own, cs].astype(F32) + COEF_C * acc).astype(BF16)

            @pl.when(n < 2)
            def _():
                @pl.loop(4 * n, 4 * n + 4 - 2 * n)
                def _(i):
                    ts = pl.ds(pl.multiple_of(i * 128, 128), 128)
                    tile = bff[ts, ts].astype(F32)
                    on = jnp.sum(jnp.where(diag, tile, 0.0), axis=0, keepdims=True)
                    dv[:, ts] = jnp.broadcast_to(COEF_A + on, (8, 128))
                    bff[ts, ts] = jnp.where(diag, 0.0, tile).astype(BF16)

            send_two(bff, pb_s, pb_r, n)

        diag_copy().start()

    @pl.loop(0, NS_STEPS - 1)
    def _(k):
        poly_step()
        mid[both, :] = dot(af[both, own], bff[own, :])
        wait_recv(bff, pb_s, pb_r)
        diag_copy().wait_recv()
        v = mid[both, :] + dot(af[both, oth], bff[oth, :])
        q_diag = dv[0:1, :]
        top = v[own] + gram[...] * q_diag
        mid[own, :] = top
        tb[...] = top.astype(BF16)
        x_new = (v[xrow] + af[xrow, :].astype(F32) * q_diag).astype(BF16)
        wait_send(af, pa_s, pa_r)
        af[xrow, :] = x_new

        @pl.loop(0, 3)
        def _(n):
            cs = columns(n)
            v = mid[own, cs] * dv[0:1, cs] + dot(tb[...], bff[:, cs])
            gram[:, cs] = v
            af[own, cs] = v.astype(BF16)
            send_two(af, pa_s, pa_r, n)

        wait_send(bff, pb_s, pb_r)
        diag_copy().wait_send()

    poly_step()
    mid[xrow, :] = dot(af[xrow, own], bff[own, :])
    wait_recv(bff, pb_s, pb_r)
    diag_copy().wait_recv()
    mid[xrow, :] = mid[xrow, :] + af[xrow, :].astype(F32) * dv[0:1, :] + dot(af[xrow, oth], bff[oth, :])
    wait_send(af, pa_s, pa_r)
    wait_send(bff, pb_s, pb_r)
    diag_copy().wait_send()

    @pl.loop(0, 4)
    def _(i):
        v = mid[xrow, pl.ds(pl.multiple_of(i * 384, 384), 384)].astype(BF16).astype(F32)
        v = jnp.concatenate([v, jnp.zeros((lanes - used, 384), F32)], axis=0).T
        ys[pl.ds(i * 16, 16)] = v.reshape(16, 24, 128).astype(BF16)

    def out_copy(o):
        d = (me + o) % 64
        return rcopy(ys.at[(d + 32 * t) % 64], yr.at[me], out_s, out_r, {"data": d})

    @pl.loop(1, 64)
    def _(o):
        out_copy(o).start()

    yr[me] = ys[slot]

    rcopy(ys.at[pl.ds(0, 63)], yr.at[pl.ds(0, 63)], out_s, out_r, sib).wait()

    @pl.loop(0, 16)
    def _(g):
        last = yr[g * 4 + 3].astype(F32)
        for r in range(3):
            x = jnp.where(lane < used, yr[g * 4 + r].astype(F32), pltpu.roll(last, 96 - 32 * r, 1))
            x_out[:, pl.ds(pl.multiple_of((g * 3 + r) * 128, 128), 128)] = x.astype(BF16)


def solution(mesh):
    data_size = mesh.shape["data"]
    tp_size = mesh.shape["tp"]
    part_spec = P(("stage", "data"), "tp")

    def local_step(weight, momentum, gradient):
        rows_local, cols_local = gradient.shape
        rows = rows_local * data_size
        sem = pltpu.SemaphoreType.DMA
        shapes = [
            pltpu.VMEM((24, 6144), F32), pltpu.VMEM((24, 6144), BF16),
            pltpu.VMEM((64, 24, 128), F32), pltpu.VMEM((64, 24, 128), F32), pltpu.VMEM((2, 8, 128), F32), pltpu.VMEM((1536, 256), BF16),
            pltpu.VMEM((3, 4, 16, 32, 128), F32), pltpu.VMEM((3, 3, 16, 32, 128), F32), pltpu.VMEM((3, 4, 4, 32, 128), F32),
            pltpu.VMEM((3, 3, 4, 32, 128), F32), pltpu.VMEM((3, 4, 32, 128), F32), pltpu.VMEM((3, 3, 32, 128), F32),
            pltpu.VMEM((3, 4, 4, 4, 32, 128), F32), pltpu.VMEM((3, 4, 4, 32, 128), F32),
            pltpu.VMEM((768, 1536), F32), pltpu.VMEM((864, 1536), F32), pltpu.VMEM((1632, 1536), BF16), pltpu.VMEM((1536, 1536), BF16),
            pltpu.VMEM((8, 1536), F32), pltpu.VMEM((768, 1536), BF16),
            pltpu.VMEM((64, 24, 128), BF16), pltpu.VMEM((64, 24, 128), BF16),
            sem((2,)), sem, sem, sem, sem, sem, sem, sem, sem, sem((3,)), sem((9,)), sem((3,)), sem((9,)), sem((9,)), sem((9,)), sem((9,)), sem((9,)),
            sem, sem, sem, sem, sem, sem, sem, sem,
        ]
        anywhere = pl.BlockSpec(memory_space=pl.ANY)
        x_fin = pl.pallas_call(
            kernel,
            out_shape=jax.ShapeDtypeStruct((rows_local, cols_local), BF16),
            in_specs=[anywhere] * 2,
            out_specs=pl.BlockSpec(memory_space=pltpu.VMEM),
            scratch_shapes=shapes,
            compiler_params=pltpu.CompilerParams(collective_id=0, has_side_effects=True, vmem_limit_bytes=60 * 1024 * 1024),
            name="muon_steps",
        )(momentum, gradient)
        new_mom = MOMENTUM * momentum + gradient.astype(F32)
        rms_scale = 0.2 * math.sqrt(max(rows, cols_local * tp_size))
        new_weight = weight - LEARN_RATE * (rms_scale * x_fin.astype(F32) + WEIGHT_DECAY * weight)
        return new_weight, new_mom

    return jax.shard_map(local_step, mesh=mesh, in_specs=(part_spec, part_spec, part_spec), out_specs=(part_spec, part_spec), check_vma=False)
```

```python
import functools
import math
import jax
import jax.numpy as jnp
from jax import lax
from jax.experimental import pallas as pl
from jax.experimental.pallas import tpu as pltpu
from jax.sharding import PartitionSpec as P

NS_STEPS = 5
MOMENTUM = 0.95
LEARN_RATE = 0.5
WEIGHT_DECAY = 0.1
COEF_A = 3.4445
COEF_B = -4.7750
COEF_C = 2.0315
EPSILON = 1e-7

MESH = pl.DeviceIdType.MESH
F32 = jnp.float32
BF16 = jnp.bfloat16
BLOCKS = ((0, 0), (1, 0), (1, 1), (2, 0), (2, 1), (2, 2), (0, 3), (0, 4), (0, 5), (1, 4), (1, 5), (2, 5))
SWAPPED = (7, 8, 10)
STRIDES = (1, 4, 16)


def dot(p, q):
    return jnp.dot(p, q, preferred_element_type=F32)


def kernel(m_hbm, g_hbm, x_out, mv, gv, nb, rx, sq, xg, part, rb1, s1, rb2, s2, rb3, gath, swap, gram, mid, af, bff, dv, tb, ys, yr,
           in_s, dv_s, dv_r, a2a_s, a2a_r, sq_s, sq_r, xg_s, xg_r, near_s, near_r, fwd_s, fwd_r, rs_s, rs_r, ag_s, ag_r, sw_s, sw_r, pa_s, pa_r, pb_s, pb_r, out_s, out_r):
    me = lax.axis_index("data")
    t = lax.axis_index("tp")
    sib = {"tp": 1 - t}
    coord = (me % 4, (me // 4) % 4, me // 16)
    rows_src, lanes = nb.shape[1:]
    used = 96
    half = 768
    own = slice(0, half)
    xrow = slice(half, half + used)
    both = slice(0, half + used)
    oth = slice(half, 2 * half)
    oth_rows = slice(half + used, 2 * half + used)

    def rcopy(src, dst, ssem, rsem, dev):
        return pltpu.make_async_remote_copy(src_ref=src, dst_ref=dst, send_sem=ssem, recv_sem=rsem, device_id=dev, device_id_type=MESH)

    barrier = pltpu.get_barrier_semaphore()

    @pl.loop(1, 64)
    def _(o):
        pl.semaphore_signal(barrier, inc=1, device_id={"data": (me + o) % 64}, device_id_type=MESH)

    pl.semaphore_signal(barrier, inc=1, device_id=sib, device_id_type=MESH)

    load_m = pltpu.make_async_copy(m_hbm, mv, in_s.at[0])
    load_g = pltpu.make_async_copy(g_hbm, gv, in_s.at[1])
    load_m.start()
    load_g.start()
    load_m.wait()
    load_g.wait()
    lane = lax.broadcasted_iota(jnp.int32, (rows_src, lanes), 1)

    def group(g, ssq):
        tiles = []
        for r in range(3):
            cs = pl.ds(pl.multiple_of((g * 3 + r) * 128, 128), 128)
            grad = gv[:, cs].astype(F32)
            new_mom = MOMENTUM * mv[:, cs] + grad
            nest = grad + MOMENTUM * new_mom
            nb[g * 4 + r] = nest
            ssq = ssq + nest * nest
            tiles.append(pltpu.roll(nest, 32 * (r + 1), 1))
        nb[g * 4 + 3] = jnp.where(lane < 32, tiles[0], jnp.where(lane < 64, tiles[1], tiles[2]))
        return ssq

    ssq = lax.fori_loop(0, 16, group, jnp.zeros((rows_src, lanes), F32))
    ssq = jnp.sum(jnp.sum(ssq, axis=0, keepdims=True), axis=1, keepdims=True)
    lane8 = lax.broadcasted_iota(jnp.int32, (8, lanes), 1)

    @pl.loop(0, 64)
    def _(d):
        nb[d, 0:8] = jnp.where(lane8 < used, nb[d, 0:8], ssq)

    pl.semaphore_wait(barrier, 64)

    slot = (me + 32 * t) % 64

    def a2a_copy(o):
        d = (me + o) % 64
        return rcopy(nb.at[d], rx.at[slot], a2a_s, a2a_r, {"data": d})

    @pl.loop(1, 64)
    def _(o):
        a2a_copy(o).start()

    rx[slot] = nb[me]

    rcopy(nb.at[pl.ds(0, 63)], rx.at[pl.ds(0, 63)], a2a_s, a2a_r, sib).wait()

    sq[0] = jnp.sum(rx[:, 0:8, :], axis=0)
    c = rcopy(sq.at[0], sq.at[1], sq_s, sq_r, sib)
    c.start()
    c.wait()
    total = (sq[0] + sq[1])[0:1, lanes - 1:lanes]
    norm = jnp.sqrt(total) + EPSILON
    lane_ok = lax.broadcasted_iota(jnp.int32, (384, lanes), 1) < used

    @pl.loop(0, 4)
    def _(i):
        v = rx[pl.ds(i * 16, 16)].reshape(384, lanes)
        x = jnp.where(lane_ok, v / norm, 0.0).astype(BF16)
        xg[pl.ds(pl.multiple_of(i * 384, 384), 384), 0:128] = x
        af[xrow, pl.ds(pl.multiple_of(i * 384, 384), 384)] = x.astype(F32).T[0:used].astype(BF16)

    def xg_copy(h):
        return rcopy(xg.at[pl.ds(h * half, half), pl.ds(0, 128)], xg.at[pl.ds((1 - h) * half, half), pl.ds(128, 128)], xg_s, xg_r, sib)

    for h in range(2):
        xg_copy(h).start()
    rcopy(xg.at[:, pl.ds(0, 128)], xg.at[:, pl.ds(128, 128)], xg_s, xg_r, sib).wait()

    def peer(dim, o):
        m = coord[dim]
        return {"data": me + ((m + o) % 4 - m) * STRIDES[dim]}

    def dims(col):
        return col, (col + 1) % 3, (col + 2) % 3

    def rs_copy(col, ph, o):
        d = dims(col)[ph]
        j = (coord[d] + o) % 4
        src = (part, s1, s2)[ph].at[col, j]
        dst = (rb1, rb2, rb3)[ph].at[col, o - 1]
        k = ph * 3 + col
        return rcopy(src, dst, rs_s.at[k], rs_r.at[k], peer(d, o))

    first, second = pl.ds(0, 8), pl.ds(8, 8)

    def near(col, src, dst, k, o):
        return rcopy(src, dst, near_s.at[col], near_r.at[col * 3 + k], peer(dims(col)[0], o))

    def near_start(col):
        m = coord[dims(col)[0]]
        up, down, far = (m + 1) % 4, (m + 3) % 4, (m + 2) % 4
        near(col, part.at[col, far, first], rb1.at[col, 2, first], 0, 1).start()
        near(col, part.at[col, far, second], rb1.at[col, 2, second], 1, 3).start()
        near(col, part.at[col, up, second], rb1.at[col, 0, second], 2, 1).start()
        near(col, part.at[col, down, first], rb1.at[col, 1, first], 2, 3).start()

    def near_merge(col):
        m = coord[dims(col)[0]]
        up, down = (m + 1) % 4, (m + 3) % 4
        near(col, part.at[col, up, first], rb1.at[col, 2, first], 0, 1).wait_recv()
        part[col, up, first] = part[col, up, first] + rb1[col, 2, first]
        near(col, part.at[col, up, first], rb1.at[col, 0, first], 2, 1).start()
        near(col, part.at[col, down, second], rb1.at[col, 2, second], 1, 3).wait_recv()
        part[col, down, second] = part[col, down, second] + rb1[col, 2, second]
        near(col, part.at[col, down, second], rb1.at[col, 1, second], 2, 3).start()

    def near_wait(col):
        two = rb1.at[col, pl.ds(0, 2)]
        near(col, two, two, 2, 1).wait_recv()
        near(col, rb1.at[col], rb1.at[col], 2, 1).wait_send()

    low, high = pl.ds(0, 2), pl.ds(2, 2)

    def fwd(col, block, rows, k, o):
        ref = gath.at[col, block, rows]
        return rcopy(ref, ref, fwd_s.at[col], fwd_r.at[col * 4 + k], peer(dims(col)[0], o))

    def fwd_start(col):
        m = coord[dims(col)[0]]
        fwd(col, m, low, 0, 1).start()
        fwd(col, m, high, 1, 3).start()
        fwd(col, m, high, 2, 1).start()
        fwd(col, m, low, 2, 3).start()

    def fwd_pass(col):
        m = coord[dims(col)[0]]
        up, down = (m + 1) % 4, (m + 3) % 4
        fwd(col, down, low, 0, 1).wait_recv()
        fwd(col, down, low, 3, 1).start()
        fwd(col, up, high, 1, 3).wait_recv()
        fwd(col, up, high, 3, 3).start()

    def fwd_wait(col, k):
        one = gath.at[col, 0]
        rcopy(one, one, fwd_s.at[col], fwd_r.at[col * 4 + k], sib).wait_recv()

    def fwd_sent(col):
        three = gath.at[col, pl.ds(0, 3)]
        rcopy(three, three, fwd_s.at[col], fwd_r.at[col * 4 + 2], sib).wait_send()

    def rs_wait(col, ph):
        k = ph * 3 + col
        three = (rb1, rb2, rb3)[ph].at[col]
        rcopy(three, three, rs_s.at[k], rs_r.at[k], sib).wait()

    def ag_ref(col, ph):
        m1, m2, m3 = (coord[d] for d in dims(col))
        return (gath.at[col, m1, m2, m3], gath.at[col, m1, m2], gath.at[col, m1])[ph]

    def ag_copy(col, ph, o):
        d = dims(col)[2 - ph]
        k = ph * 3 + col
        return rcopy(ag_ref(col, ph), ag_ref(col, ph), ag_s.at[k], ag_r.at[k], peer(d, o))

    def ag_wait(col, ph):
        k = ph * 3 + col
        first = pl.ds(0, 3)
        three = (gath.at[col, 0, 0, first], gath.at[col, 0, first], gath.at[col, first])[ph]
        rcopy(three, three, ag_s.at[k], ag_r.at[k], sib).wait()

    for col in range(3):
        for b in range(4):
            i, j = BLOCKS[col * 4 + b]
            res = lax.dot_general(xg[i * 256:(i + 1) * 256, :], xg[j * 256:(j + 1) * 256, :], (((1,), (1,)), ((), ())), preferred_element_type=F32)
            for h in range(2):
                part[col, b, h * 8:(h + 1) * 8] = res[:, h * 128:(h + 1) * 128].reshape(8, 32, 128)
        near_start(col)
    for col in range(3):
        near_merge(col)
    for ph in range(3):
        for col in range(3):
            if ph == 0:
                near_wait(col)
            else:
                rs_wait(col, ph)
            m1, m2, m3 = (coord[d] for d in dims(col))
            if ph == 0:
                s1[col] = (part[col, m1] + rb1[col, 0] + rb1[col, 1]).reshape(4, 4, 32, 128)
            elif ph == 1:
                s2[col] = s1[col, m2] + rb2[col, 0] + rb2[col, 1] + rb2[col, 2]
            else:
                gath[col, m1, m2, m3] = s2[col, m3] + rb3[col, 0] + rb3[col, 1] + rb3[col, 2]
            for o in range(1, 4):
                if ph < 2:
                    rs_copy(col, ph + 1, o).start()
                else:
                    ag_copy(col, 0, o).start()
    for ph in range(2):
        for col in range(3):
            ag_wait(col, ph)
            if ph == 0:
                for o in range(1, 4):
                    ag_copy(col, 1, o).start()
            else:
                fwd_start(col)
    base = half + used

    def lookup(values, at):
        out = values[3]
        for n in range(3):
            out = jnp.where(at == n, values[n], out)
        return out

    def to_sibling(r, c, rows, cols_n, r2, c2):
        rcopy(af.at[pl.ds(r, rows), pl.ds(c, cols_n)], af.at[pl.ds(r2, rows), pl.ds(c2, cols_n)], pa_s, pa_r, sib).start()

    def al256(v):
        return pl.multiple_of(v, 256)

    def al128(v):
        return pl.multiple_of(v, 128)

    def place(col, b, h):
        quad = BLOCKS[col * 4:col * 4 + 4]
        i = lookup([p[0] for p in quad], b)
        j = lookup([p[1] for p in quad], b)
        v = gath[col, b, 2 * h:2 * h + 2].reshape(256, 128)
        r, c = al256(i * 256), al128(j * 256 + h * 128)
        gram[pl.ds(r, 256), pl.ds(c, 128)] = v
        af[pl.ds(r, 256), pl.ds(c, 128)] = v.astype(BF16)
        to_sibling(r, c, 256, 128, base + r, al128((j + 3) % 6 * 256 + h * 128))
        mirrored = [n for n in range(4) if quad[n][1] < quad[n][0]]
        swapped = [n for n in range(4) if col * 4 + n in SWAPPED]
        if mirrored:
            hit = b == mirrored[0]
            for n in mirrored[1:]:
                hit = hit | (b == n)

            @pl.when(hit)
            def _():
                vt = v.T
                r2, c2 = al128(j * 256 + h * 128), al256(i * 256)
                gram[pl.ds(r2, 128), pl.ds(c2, 256)] = vt
                af[pl.ds(r2, 128), pl.ds(c2, 256)] = vt.astype(BF16)
                to_sibling(r2, c2, 128, 256, base + r2, al256((i + 3) * 256))

        for n in swapped:
            i0, j0 = quad[n]
            k = SWAPPED.index(col * 4 + n)

            @pl.when(b == n)
            def _():
                vt = v.T
                r2 = (j0 - 3) * 256 + h * 128
                swap[k, h] = vt
                rcopy(swap.at[k, h], gram.at[pl.ds(r2, 128), pl.ds((i0 + 3) * 256, 256)], sw_s, sw_r, sib).start()
                af[base + r2:base + r2 + 128, i0 * 256:(i0 + 1) * 256] = vt.astype(BF16)

    ring = [coord[dims(col)[0]] for col in range(3)]
    for col in range(3):
        for h in range(2):
            place(col, ring[col], h)
    for col in range(3):
        fwd_pass(col)
    for col in range(3):
        place(col, (ring[col] + 3) % 4, 0)
        place(col, (ring[col] + 1) % 4, 1)
    for col in range(3):
        fwd_wait(col, 2)
        place(col, (ring[col] + 3) % 4, 1)
        place(col, (ring[col] + 1) % 4, 0)
    for col in range(3):
        fwd_wait(col, 3)
        for h in range(2):
            place(col, (ring[col] + 2) % 4, h)
    for col in range(3):
        fwd_sent(col)
    rcopy(swap, swap, sw_s, sw_r, sib).wait()
    for n in range(3):
        i, j = BLOCKS[SWAPPED[n]]
        rs, cs = slice((j - 3) * 256, (j - 2) * 256), slice((i + 3) * 256, (i + 4) * 256)
        af[rs, cs] = gram[rs, cs].astype(BF16)

    def piece(buf, ssem, rsem, p):
        q = (p + 3) % 6
        base = buf.shape[0] - half
        return rcopy(buf.at[pl.ds(0, half), pl.ds(pl.multiple_of(p * 256, 256), 256)],
                     buf.at[pl.ds(base, half), pl.ds(pl.multiple_of(q * 256, 256), 256)], ssem, rsem, sib)

    def send_two(buf, ssem, rsem, n):
        piece(buf, ssem, rsem, 2 * n).start()
        piece(buf, ssem, rsem, 2 * n + 1).start()

    def wait_recv(buf, ssem, rsem, rows=768):
        rcopy(buf.at[pl.ds(0, rows)], buf.at[pl.ds(0, rows)], ssem, rsem, sib).wait_recv()

    def wait_send(buf, ssem, rsem, rows=768):
        rcopy(buf.at[pl.ds(0, rows)], buf.at[pl.ds(0, rows)], ssem, rsem, sib).wait_send()

    def diag_copy():
        return rcopy(dv.at[:, pl.ds(0, half)], dv.at[:, pl.ds(half, half)], dv_s, dv_r, sib)

    def columns(n):
        return pl.ds(pl.multiple_of(n * 512, 512), 512)

    diag = lax.broadcasted_iota(jnp.int32, (128, 128), 0) == lax.broadcasted_iota(jnp.int32, (128, 128), 1)

    def poly_step(rows):
        mid[own, :] = dot(af[own, own], af[own, :])
        wait_recv(af, pa_s, pa_r, rows)

        @pl.loop(0, 3)
        def _(n):
            cs = columns(n)
            acc = mid[own, cs] + dot(af[own, oth], af[oth_rows, cs])
            bff[own, cs] = (COEF_B * af[own, cs].astype(F32) + COEF_C * acc).astype(BF16)

            @pl.when(n < 2)
            def _():
                @pl.loop(4 * n, 4 * n + 4 - 2 * n)
                def _(i):
                    ts = pl.ds(pl.multiple_of(i * 128, 128), 128)
                    tile = bff[ts, ts].astype(F32)
                    on = jnp.sum(jnp.where(diag, tile, 0.0), axis=0, keepdims=True)
                    dv[:, ts] = jnp.broadcast_to(COEF_A + on, (8, 128))
                    bff[ts, ts] = jnp.where(diag, 0.0, tile).astype(BF16)

            send_two(bff, pb_s, pb_r, n)

        diag_copy().start()
        wait_send(af, pa_s, pa_r, rows)

    poly_step(640)

    @pl.loop(0, NS_STEPS - 1)
    def _(k):
        mid[both, :] = dot(af[both, own], bff[own, :])
        wait_recv(bff, pb_s, pb_r)
        diag_copy().wait_recv()
        v = mid[both, :] + dot(af[both, oth], bff[oth, :])
        q_diag = dv[0:1, :]
        top = v[own] + gram[...] * q_diag
        mid[own, :] = top
        tb[...] = top.astype(BF16)
        x_new = (v[xrow] + af[xrow, :].astype(F32) * q_diag).astype(BF16)
        af[xrow, :] = x_new

        @pl.loop(0, 3)
        def _(n):
            cs = columns(n)
            v = mid[own, cs] * dv[0:1, cs] + dot(tb[...], bff[:, cs])
            gram[:, cs] = v
            af[own, cs] = v.astype(BF16)
            send_two(af, pa_s, pa_r, n)

        wait_send(bff, pb_s, pb_r)
        diag_copy().wait_send()
        poly_step(768)

    mid[xrow, :] = dot(af[xrow, own], bff[own, :])
    wait_recv(bff, pb_s, pb_r)
    diag_copy().wait_recv()
    mid[xrow, :] = mid[xrow, :] + af[xrow, :].astype(F32) * dv[0:1, :] + dot(af[xrow, oth], bff[oth, :])
    wait_send(bff, pb_s, pb_r)
    diag_copy().wait_send()

    @pl.loop(0, 4)
    def _(i):
        v = mid[xrow, pl.ds(pl.multiple_of(i * 384, 384), 384)].astype(BF16).astype(F32)
        v = jnp.concatenate([v, jnp.zeros((lanes - used, 384), F32)], axis=0).T
        ys[pl.ds(i * 16, 16)] = v.reshape(16, 24, 128).astype(BF16)

    def out_copy(o):
        d = (me + o) % 64
        return rcopy(ys.at[(d + 32 * t) % 64], yr.at[me], out_s, out_r, {"data": d})

    @pl.loop(1, 64)
    def _(o):
        out_copy(o).start()

    yr[me] = ys[slot]

    rcopy(ys.at[pl.ds(0, 63)], yr.at[pl.ds(0, 63)], out_s, out_r, sib).wait()

    @pl.loop(0, 16)
    def _(g):
        last = yr[g * 4 + 3].astype(F32)
        for r in range(3):
            x = jnp.where(lane < used, yr[g * 4 + r].astype(F32), pltpu.roll(last, 96 - 32 * r, 1))
            x_out[:, pl.ds(pl.multiple_of((g * 3 + r) * 128, 128), 128)] = x.astype(BF16)


def solution(mesh):
    data_size = mesh.shape["data"]
    tp_size = mesh.shape["tp"]
    part_spec = P(("stage", "data"), "tp")

    def local_step(weight, momentum, gradient):
        rows_local, cols_local = gradient.shape
        rows = rows_local * data_size
        sem = pltpu.SemaphoreType.DMA
        shapes = [
            pltpu.VMEM((24, 6144), F32), pltpu.VMEM((24, 6144), BF16),
            pltpu.VMEM((64, 24, 128), F32), pltpu.VMEM((64, 24, 128), F32), pltpu.VMEM((2, 8, 128), F32), pltpu.VMEM((1536, 256), BF16),
            pltpu.VMEM((3, 4, 16, 32, 128), F32), pltpu.VMEM((3, 3, 16, 32, 128), F32), pltpu.VMEM((3, 4, 4, 32, 128), F32),
            pltpu.VMEM((3, 3, 4, 32, 128), F32), pltpu.VMEM((3, 4, 32, 128), F32), pltpu.VMEM((3, 3, 32, 128), F32),
            pltpu.VMEM((3, 4, 4, 4, 32, 128), F32), pltpu.VMEM((3, 2, 128, 256), F32),
            pltpu.VMEM((768, 1536), F32), pltpu.VMEM((864, 1536), F32), pltpu.VMEM((1632, 1536), BF16), pltpu.VMEM((1536, 1536), BF16),
            pltpu.VMEM((8, 1536), F32), pltpu.VMEM((768, 1536), BF16),
            pltpu.VMEM((64, 24, 128), BF16), pltpu.VMEM((64, 24, 128), BF16),
            sem((2,)), sem, sem, sem, sem, sem, sem, sem, sem, sem((3,)), sem((9,)), sem((3,)), sem((12,)), sem((9,)), sem((9,)), sem((9,)), sem((9,)),
            sem, sem, sem, sem, sem, sem, sem, sem,
        ]
        anywhere = pl.BlockSpec(memory_space=pl.ANY)
        x_fin = pl.pallas_call(
            kernel,
            out_shape=jax.ShapeDtypeStruct((rows_local, cols_local), BF16),
            in_specs=[anywhere] * 2,
            out_specs=pl.BlockSpec(memory_space=pltpu.VMEM),
            scratch_shapes=shapes,
            compiler_params=pltpu.CompilerParams(collective_id=0, has_side_effects=True, vmem_limit_bytes=60 * 1024 * 1024),
            name="muon_steps",
        )(momentum, gradient)
        new_mom = MOMENTUM * momentum + gradient.astype(F32)
        rms_scale = 0.2 * math.sqrt(max(rows, cols_local * tp_size))
        new_weight = weight - LEARN_RATE * (rms_scale * x_fin.astype(F32) + WEIGHT_DECAY * weight)
        return new_weight, new_mom

    return jax.shard_map(local_step, mesh=mesh, in_specs=(part_spec, part_spec, part_spec), out_specs=(part_spec, part_spec), check_vma=False)
```

```python
import functools
import math
import jax
import jax.numpy as jnp
from jax import lax
from jax.experimental import pallas as pl
from jax.experimental.pallas import tpu as pltpu
from jax.sharding import PartitionSpec as P

NS_STEPS = 5
MOMENTUM = 0.95
LEARN_RATE = 0.5
WEIGHT_DECAY = 0.1
COEF_A = 3.4445
COEF_B = -4.7750
COEF_C = 2.0315
EPSILON = 1e-7

MESH = pl.DeviceIdType.MESH
F32 = jnp.float32
BF16 = jnp.bfloat16
BLOCKS = ((0, 0), (1, 0), (1, 1), (2, 0), (2, 1), (2, 2), (0, 3), (0, 4), (0, 5), (1, 4), (1, 5), (2, 5))
SWAPPED = (7, 8, 10)
STRIDES = (1, 4, 16)
VMEM_MIB = 54
HOPS = (0, 1, 2, 1)
OFFSETS = [(i, j, k) for i in range(4) for j in range(4) for k in range(4) if i + j + k]
FAR_FIRST = sorted(OFFSETS, key=lambda o: -sum(HOPS[n] for n in o))


def dot(p, q):
    return jnp.dot(p, q, preferred_element_type=F32)


def kernel(m_hbm, g_hbm, x_out, mv, gv, nb, rx, sq, xg, part, rb1, s1, rb2, s2, rb3, gath, swap, gram, mid, af, bff, dv, tb, ys, yr,
           in_s, dv_s, dv_r, a2a_s, a2a_r, sq_s, sq_r, xg_s, xg_r, near_s, near_r, fwd_s, fwd_r, rs_s, rs_r, ag_s, ag_r, sw_s, sw_r, pa_s, pa_r, pb_s, pb_r, out_s, out_r):
    me = lax.axis_index("data")
    t = lax.axis_index("tp")
    sib = {"tp": 1 - t}
    coord = (me % 4, (me // 4) % 4, me // 16)
    rows_src, lanes = nb.shape[1:]
    used = 96
    half = 768
    own = slice(0, half)
    xrow = slice(half, half + used)
    both = slice(0, half + used)
    oth = slice(half, 2 * half)
    oth_rows = slice(half + used, 2 * half + used)

    def rcopy(src, dst, ssem, rsem, dev):
        return pltpu.make_async_remote_copy(src_ref=src, dst_ref=dst, send_sem=ssem, recv_sem=rsem, device_id=dev, device_id_type=MESH)

    barrier = pltpu.get_barrier_semaphore()

    shifted = [[((coord[n] + o) % 4) * STRIDES[n] for o in range(4)] for n in range(3)]

    def target(o):
        return shifted[0][o[0]] + shifted[1][o[1]] + shifted[2][o[2]]

    for o in FAR_FIRST:
        pl.semaphore_signal(barrier, inc=1, device_id={"data": target(o)}, device_id_type=MESH)

    pl.semaphore_signal(barrier, inc=1, device_id=sib, device_id_type=MESH)

    load_m = pltpu.make_async_copy(m_hbm, mv, in_s.at[0])
    load_g = pltpu.make_async_copy(g_hbm, gv, in_s.at[1])
    load_m.start()
    load_g.start()
    load_m.wait()
    load_g.wait()
    lane = lax.broadcasted_iota(jnp.int32, (rows_src, lanes), 1)

    def group(g, ssq):
        tiles = []
        for r in range(3):
            cs = pl.ds(pl.multiple_of((g * 3 + r) * 128, 128), 128)
            grad = gv[:, cs].astype(F32)
            new_mom = MOMENTUM * mv[:, cs] + grad
            nest = grad + MOMENTUM * new_mom
            nb[g * 4 + r] = nest
            ssq = ssq + nest * nest
            tiles.append(pltpu.roll(nest, 32 * (r + 1), 1))
        nb[g * 4 + 3] = jnp.where(lane < 32, tiles[0], jnp.where(lane < 64, tiles[1], tiles[2]))
        return ssq

    ssq = lax.fori_loop(0, 16, group, jnp.zeros((rows_src, lanes), F32))
    ssq = jnp.sum(jnp.sum(ssq, axis=0, keepdims=True), axis=1, keepdims=True)
    lane8 = lax.broadcasted_iota(jnp.int32, (8, lanes), 1)

    @pl.loop(0, 64)
    def _(d):
        nb[d, 0:8] = jnp.where(lane8 < used, nb[d, 0:8], ssq)

    pl.semaphore_wait(barrier, 64)

    slot = (me + 32 * t) % 64

    for o in FAR_FIRST:
        d = target(o)
        rcopy(nb.at[d], rx.at[slot], a2a_s, a2a_r, {"data": d}).start()

    rx[slot] = nb[me]

    rcopy(nb.at[pl.ds(0, 63)], rx.at[pl.ds(0, 63)], a2a_s, a2a_r, sib).wait()

    sq[0] = jnp.sum(rx[:, 0:8, :], axis=0)
    c = rcopy(sq.at[0], sq.at[1], sq_s, sq_r, sib)
    c.start()
    c.wait()
    total = (sq[0] + sq[1])[0:1, lanes - 1:lanes]
    norm = jnp.sqrt(total) + EPSILON
    lane_ok = lax.broadcasted_iota(jnp.int32, (384, lanes), 1) < used

    def xg_copy(h):
        return rcopy(xg.at[pl.ds(h * half, half), pl.ds(0, 128)], xg.at[pl.ds((1 - h) * half, half), pl.ds(128, 128)], xg_s, xg_r, sib)

    for i in range(4):
        v = rx[pl.ds(i * 16, 16)].reshape(384, lanes)
        x = jnp.where(lane_ok, v / norm, 0.0).astype(BF16)
        xg[pl.ds(pl.multiple_of(i * 384, 384), 384), 0:128] = x
        af[xrow, pl.ds(pl.multiple_of(i * 384, 384), 384)] = x.astype(F32).T[0:used].astype(BF16)
        if i % 2 == 1:
            xg_copy(i // 2).start()
    rcopy(xg.at[:, pl.ds(0, 128)], xg.at[:, pl.ds(128, 128)], xg_s, xg_r, sib).wait()

    def peer(dim, o):
        m = coord[dim]
        return {"data": me + ((m + o) % 4 - m) * STRIDES[dim]}

    def dims(col):
        return col, (col + 1) % 3, (col + 2) % 3

    def rs_copy(col, ph, o):
        d = dims(col)[ph]
        j = (coord[d] + o) % 4
        src = (part, s1, s2)[ph].at[col, j]
        dst = (rb1, rb2, rb3)[ph].at[col, o - 1]
        k = ph * 3 + col
        return rcopy(src, dst, rs_s.at[k], rs_r.at[k], peer(d, o))

    first, second = pl.ds(0, 8), pl.ds(8, 8)

    def near(col, src, dst, k, o):
        return rcopy(src, dst, near_s.at[col], near_r.at[col * 3 + k], peer(dims(col)[0], o))

    def near_start(col):
        m = coord[dims(col)[0]]
        up, down, far = (m + 1) % 4, (m + 3) % 4, (m + 2) % 4
        near(col, part.at[col, far, first], rb1.at[col, 2, first], 0, 1).start()
        near(col, part.at[col, far, second], rb1.at[col, 2, second], 1, 3).start()
        near(col, part.at[col, up, second], rb1.at[col, 0, second], 2, 1).start()
        near(col, part.at[col, down, first], rb1.at[col, 1, first], 2, 3).start()

    def near_merge(col):
        m = coord[dims(col)[0]]
        up, down = (m + 1) % 4, (m + 3) % 4
        near(col, part.at[col, up, first], rb1.at[col, 2, first], 0, 1).wait_recv()
        part[col, up, first] = part[col, up, first] + rb1[col, 2, first]
        near(col, part.at[col, up, first], rb1.at[col, 0, first], 2, 1).start()
        near(col, part.at[col, down, second], rb1.at[col, 2, second], 1, 3).wait_recv()
        part[col, down, second] = part[col, down, second] + rb1[col, 2, second]
        near(col, part.at[col, down, second], rb1.at[col, 1, second], 2, 3).start()

    def near_wait(col):
        two = rb1.at[col, pl.ds(0, 2)]
        near(col, two, two, 2, 1).wait_recv()
        near(col, rb1.at[col], rb1.at[col], 2, 1).wait_send()

    low, high = pl.ds(0, 2), pl.ds(2, 2)

    def fwd(col, block, rows, k, o):
        ref = gath.at[col, block, rows]
        return rcopy(ref, ref, fwd_s.at[col], fwd_r.at[col * 4 + k], peer(dims(col)[0], o))

    def fwd_start(col):
        m = coord[dims(col)[0]]
        fwd(col, m, low, 0, 1).start()
        fwd(col, m, high, 1, 3).start()
        fwd(col, m, high, 2, 1).start()
        fwd(col, m, low, 2, 3).start()

    def fwd_pass(col):
        m = coord[dims(col)[0]]
        up, down = (m + 1) % 4, (m + 3) % 4
        fwd(col, down, low, 0, 1).wait_recv()
        fwd(col, down, low, 3, 1).start()
        fwd(col, up, high, 1, 3).wait_recv()
        fwd(col, up, high, 3, 3).start()

    def fwd_wait(col, k):
        one = gath.at[col, 0]
        rcopy(one, one, fwd_s.at[col], fwd_r.at[col * 4 + k], sib).wait_recv()

    def fwd_sent(col):
        three = gath.at[col, pl.ds(0, 3)]
        rcopy(three, three, fwd_s.at[col], fwd_r.at[col * 4 + 2], sib).wait_send()

    def rs_wait(col, ph):
        k = ph * 3 + col
        three = (rb1, rb2, rb3)[ph].at[col]
        rcopy(three, three, rs_s.at[k], rs_r.at[k], sib).wait()

    def ag_ref(col, ph):
        m1, m2, m3 = (coord[d] for d in dims(col))
        return (gath.at[col, m1, m2, m3], gath.at[col, m1, m2], gath.at[col, m1])[ph]

    def ag_copy(col, ph, o):
        d = dims(col)[2 - ph]
        k = ph * 3 + col
        return rcopy(ag_ref(col, ph), ag_ref(col, ph), ag_s.at[k], ag_r.at[k], peer(d, o))

    def ag_wait(col, ph):
        k = ph * 3 + col
        first = pl.ds(0, 3)
        three = (gath.at[col, 0, 0, first], gath.at[col, 0, first], gath.at[col, first])[ph]
        rcopy(three, three, ag_s.at[k], ag_r.at[k], sib).wait()

    for col in range(3):
        for b in range(4):
            i, j = BLOCKS[col * 4 + b]
            res = lax.dot_general(xg[i * 256:(i + 1) * 256, :], xg[j * 256:(j + 1) * 256, :], (((1,), (1,)), ((), ())), preferred_element_type=F32)
            for h in range(2):
                part[col, b, h * 8:(h + 1) * 8] = res[:, h * 128:(h + 1) * 128].reshape(8, 32, 128)
        near_start(col)
    for col in range(3):
        near_merge(col)
    for ph in range(3):
        for col in range(3):
            if ph == 0:
                near_wait(col)
            else:
                rs_wait(col, ph)
            m1, m2, m3 = (coord[d] for d in dims(col))
            if ph == 0:
                s1[col] = (part[col, m1] + rb1[col, 0] + rb1[col, 1]).reshape(4, 4, 32, 128)
            elif ph == 1:
                s2[col] = s1[col, m2] + rb2[col, 0] + rb2[col, 1] + rb2[col, 2]
            else:
                gath[col, m1, m2, m3] = s2[col, m3] + rb3[col, 0] + rb3[col, 1] + rb3[col, 2]
            for o in range(1, 4):
                if ph < 2:
                    rs_copy(col, ph + 1, o).start()
                else:
                    ag_copy(col, 0, o).start()
    for ph in range(2):
        for col in range(3):
            ag_wait(col, ph)
            if ph == 0:
                for o in range(1, 4):
                    ag_copy(col, 1, o).start()
            else:
                fwd_start(col)
    base = half + used

    def lookup(values, at):
        out = values[3]
        for n in range(3):
            out = jnp.where(at == n, values[n], out)
        return out

    def to_sibling(r, c, rows, cols_n, r2, c2):
        rcopy(af.at[pl.ds(r, rows), pl.ds(c, cols_n)], af.at[pl.ds(r2, rows), pl.ds(c2, cols_n)], pa_s, pa_r, sib).start()

    def al256(v):
        return pl.multiple_of(v, 256)

    def al128(v):
        return pl.multiple_of(v, 128)

    def place(col, b, h):
        quad = BLOCKS[col * 4:col * 4 + 4]
        i = lookup([p[0] for p in quad], b)
        j = lookup([p[1] for p in quad], b)
        v = gath[col, b, 2 * h:2 * h + 2].reshape(256, 128)
        r, c = al256(i * 256), al128(j * 256 + h * 128)
        gram[pl.ds(r, 256), pl.ds(c, 128)] = v
        af[pl.ds(r, 256), pl.ds(c, 128)] = v.astype(BF16)
        to_sibling(r, c, 256, 128, base + r, al128((j + 3) % 6 * 256 + h * 128))
        mirrored = [n for n in range(4) if quad[n][1] < quad[n][0]]
        swapped = [n for n in range(4) if col * 4 + n in SWAPPED]
        if mirrored:
            hit = b == mirrored[0]
            for n in mirrored[1:]:
                hit = hit | (b == n)

            @pl.when(hit)
            def _():
                vt = v.T
                r2, c2 = al128(j * 256 + h * 128), al256(i * 256)
                gram[pl.ds(r2, 128), pl.ds(c2, 256)] = vt
                af[pl.ds(r2, 128), pl.ds(c2, 256)] = vt.astype(BF16)
                to_sibling(r2, c2, 128, 256, base + r2, al256((i + 3) * 256))

        for n in swapped:
            i0, j0 = quad[n]
            k = SWAPPED.index(col * 4 + n)

            @pl.when(b == n)
            def _():
                vt = v.T
                r2 = (j0 - 3) * 256 + h * 128
                swap[k, h] = vt
                rcopy(swap.at[k, h], gram.at[pl.ds(r2, 128), pl.ds((i0 + 3) * 256, 256)], sw_s, sw_r, sib).start()
                af[base + r2:base + r2 + 128, i0 * 256:(i0 + 1) * 256] = vt.astype(BF16)

    ring = [coord[dims(col)[0]] for col in range(3)]
    for col in range(3):
        for h in range(2):
            place(col, ring[col], h)
    for col in range(3):
        fwd_pass(col)
    for col in range(3):
        place(col, (ring[col] + 3) % 4, 0)
        place(col, (ring[col] + 1) % 4, 1)
    for col in range(3):
        fwd_wait(col, 2)
        place(col, (ring[col] + 3) % 4, 1)
        place(col, (ring[col] + 1) % 4, 0)
    for col in range(3):
        fwd_wait(col, 3)
        for h in range(2):
            place(col, (ring[col] + 2) % 4, h)
    for col in range(3):
        fwd_sent(col)
    rcopy(swap, swap, sw_s, sw_r, sib).wait()
    for n in range(3):
        i, j = BLOCKS[SWAPPED[n]]
        rs, cs = slice((j - 3) * 256, (j - 2) * 256), slice((i + 3) * 256, (i + 4) * 256)
        af[rs, cs] = gram[rs, cs].astype(BF16)

    def piece(buf, ssem, rsem, p):
        q = (p + 3) % 6
        base = buf.shape[0] - half
        return rcopy(buf.at[pl.ds(0, half), pl.ds(pl.multiple_of(p * 256, 256), 256)],
                     buf.at[pl.ds(base, half), pl.ds(pl.multiple_of(q * 256, 256), 256)], ssem, rsem, sib)

    def send_two(buf, ssem, rsem, n):
        piece(buf, ssem, rsem, 2 * n).start()
        piece(buf, ssem, rsem, 2 * n + 1).start()

    def wait_recv(buf, ssem, rsem, rows=768):
        rcopy(buf.at[pl.ds(0, rows)], buf.at[pl.ds(0, rows)], ssem, rsem, sib).wait_recv()

    def wait_send(buf, ssem, rsem, rows=768):
        rcopy(buf.at[pl.ds(0, rows)], buf.at[pl.ds(0, rows)], ssem, rsem, sib).wait_send()

    def diag_copy():
        return rcopy(dv.at[:, pl.ds(0, half)], dv.at[:, pl.ds(half, half)], dv_s, dv_r, sib)

    diag = lax.broadcasted_iota(jnp.int32, (128, 128), 0) == lax.broadcasted_iota(jnp.int32, (128, 128), 1)

    def poly_step(rows):
        mid[own, :] = dot(af[own, own], af[own, :])
        wait_recv(af, pa_s, pa_r, rows)

        for n in range(3):
            cs = slice(n * 512, n * 512 + 512)
            acc = mid[own, cs] + dot(af[own, oth], af[oth_rows, cs])
            bff[own, cs] = (COEF_B * af[own, cs].astype(F32) + COEF_C * acc).astype(BF16)
            for i in range(4 * n, min(4 * n + 4, 6)):
                ts = slice(i * 128, i * 128 + 128)
                tile = bff[ts, ts].astype(F32)
                on = jnp.sum(jnp.where(diag, tile, 0.0), axis=0, keepdims=True)
                dv[:, ts] = jnp.broadcast_to(COEF_A + on, (8, 128))
                bff[ts, ts] = jnp.where(diag, 0.0, tile).astype(BF16)
            send_two(bff, pb_s, pb_r, n)

        diag_copy().start()
        wait_send(af, pa_s, pa_r, rows)

    poly_step(640)

    @pl.loop(0, NS_STEPS - 1)
    def _(k):
        mid[both, :] = dot(af[both, own], bff[own, :])
        wait_recv(bff, pb_s, pb_r)
        diag_copy().wait_recv()
        v = mid[both, :] + dot(af[both, oth], bff[oth, :])
        q_diag = dv[0:1, :]
        top = v[own] + gram[...] * q_diag
        mid[own, :] = top
        tb[...] = top.astype(BF16)
        x_new = (v[xrow] + af[xrow, :].astype(F32) * q_diag).astype(BF16)
        af[xrow, :] = x_new

        for n in range(3):
            cs = slice(n * 512, n * 512 + 512)
            v = mid[own, cs] * dv[0:1, cs] + dot(tb[...], bff[:, cs])
            gram[:, cs] = v
            af[own, cs] = v.astype(BF16)
            send_two(af, pa_s, pa_r, n)

        wait_send(bff, pb_s, pb_r)
        diag_copy().wait_send()
        poly_step(768)

    mid[xrow, :] = dot(af[xrow, own], bff[own, :])
    wait_recv(bff, pb_s, pb_r)
    diag_copy().wait_recv()
    mid[xrow, :] = mid[xrow, :] + af[xrow, :].astype(F32) * dv[0:1, :] + dot(af[xrow, oth], bff[oth, :])
    wait_send(bff, pb_s, pb_r)
    diag_copy().wait_send()

    @pl.loop(0, 4)
    def _(i):
        v = mid[xrow, pl.ds(pl.multiple_of(i * 384, 384), 384)].astype(BF16).astype(F32)
        v = jnp.concatenate([v, jnp.zeros((lanes - used, 384), F32)], axis=0).T
        ys[pl.ds(i * 16, 16)] = v.reshape(16, 24, 128).astype(BF16)

    for o in FAR_FIRST:
        d = target(o)
        rcopy(ys.at[(d + 32 * t) % 64], yr.at[me], out_s, out_r, {"data": d}).start()

    yr[me] = ys[slot]

    rcopy(ys.at[pl.ds(0, 63)], yr.at[pl.ds(0, 63)], out_s, out_r, sib).wait()

    @pl.loop(0, 16)
    def _(g):
        last = yr[g * 4 + 3].astype(F32)
        for r in range(3):
            x = jnp.where(lane < used, yr[g * 4 + r].astype(F32), pltpu.roll(last, 96 - 32 * r, 1))
            x_out[:, pl.ds(pl.multiple_of((g * 3 + r) * 128, 128), 128)] = x.astype(BF16)


def solution(mesh):
    data_size = mesh.shape["data"]
    tp_size = mesh.shape["tp"]
    part_spec = P(("stage", "data"), "tp")

    def local_step(weight, momentum, gradient):
        rows_local, cols_local = gradient.shape
        rows = rows_local * data_size
        sem = pltpu.SemaphoreType.DMA
        shapes = [
            pltpu.VMEM((24, 6144), F32), pltpu.VMEM((24, 6144), BF16),
            pltpu.VMEM((64, 24, 128), F32), pltpu.VMEM((64, 24, 128), F32), pltpu.VMEM((2, 8, 128), F32), pltpu.VMEM((1536, 256), BF16),
            pltpu.VMEM((3, 4, 16, 32, 128), F32), pltpu.VMEM((3, 3, 16, 32, 128), F32), pltpu.VMEM((3, 4, 4, 32, 128), F32),
            pltpu.VMEM((3, 3, 4, 32, 128), F32), pltpu.VMEM((3, 4, 32, 128), F32), pltpu.VMEM((3, 3, 32, 128), F32),
            pltpu.VMEM((3, 4, 4, 4, 32, 128), F32), pltpu.VMEM((3, 2, 128, 256), F32),
            pltpu.VMEM((768, 1536), F32), pltpu.VMEM((864, 1536), F32), pltpu.VMEM((1632, 1536), BF16), pltpu.VMEM((1536, 1536), BF16),
            pltpu.VMEM((8, 1536), F32), pltpu.VMEM((768, 1536), BF16),
            pltpu.VMEM((64, 24, 128), BF16), pltpu.VMEM((64, 24, 128), BF16),
            sem((2,)), sem, sem, sem, sem, sem, sem, sem, sem, sem((3,)), sem((9,)), sem((3,)), sem((12,)), sem((9,)), sem((9,)), sem((9,)), sem((9,)),
            sem, sem, sem, sem, sem, sem, sem, sem,
        ]
        anywhere = pl.BlockSpec(memory_space=pl.ANY)
        x_fin = pl.pallas_call(
            kernel,
            out_shape=jax.ShapeDtypeStruct((rows_local, cols_local), BF16),
            in_specs=[anywhere] * 2,
            out_specs=pl.BlockSpec(memory_space=pltpu.VMEM),
            scratch_shapes=shapes,
            compiler_params=pltpu.CompilerParams(collective_id=0, has_side_effects=True, vmem_limit_bytes=VMEM_MIB * 1024 * 1024),
            name="muon_steps",
        )(momentum, gradient)
        new_mom = MOMENTUM * momentum + gradient.astype(F32)
        rms_scale = 0.2 * math.sqrt(max(rows, cols_local * tp_size))
        new_weight = weight - LEARN_RATE * (rms_scale * x_fin.astype(F32) + WEIGHT_DECAY * weight)
        return new_weight, new_mom

    return jax.shard_map(local_step, mesh=mesh, in_specs=(part_spec, part_spec, part_spec), out_specs=(part_spec, part_spec), check_vma=False)
```

```python
import functools
import math
import jax
import jax.numpy as jnp
from jax import lax
from jax.experimental import pallas as pl
from jax.experimental.pallas import tpu as pltpu
from jax.sharding import PartitionSpec as P

NS_STEPS = 5
MOMENTUM = 0.95
LEARN_RATE = 0.5
WEIGHT_DECAY = 0.1
COEF_A = 3.4445
COEF_B = -4.7750
COEF_C = 2.0315
EPSILON = 1e-7

MESH = pl.DeviceIdType.MESH
F32 = jnp.float32
BF16 = jnp.bfloat16
BLOCKS = ((0, 0), (1, 0), (1, 1), (2, 0), (2, 1), (2, 2), (0, 3), (0, 4), (0, 5), (1, 4), (1, 5), (2, 5))
SWAPPED = (7, 8, 10)
STRIDES = (1, 4, 16)
VMEM_MIB = 54


def dot(p, q):
    return jnp.dot(p, q, preferred_element_type=F32)


def kernel(m_hbm, g_hbm, x_out, mv, gv, nb, rx, sq, xg, part, rb1, s1, rb2, s2, rb3, gath, swap, gram, mid, af, bff, dv, tb, ys, yr,
           in_s, dv_s, dv_r, a2a_s, a2a_r, sq_s, sq_r, xg_s, xg_r, near_s, near_r, fwd_s, fwd_r, rs_s, rs_r, sw_s, sw_r, pa_s, pa_r, pb_s, pb_r, out_s, out_r):
    me = lax.axis_index("data")
    t = lax.axis_index("tp")
    sib = {"tp": 1 - t}
    coord = (me % 4, (me // 4) % 4, me // 16)
    rows_src, lanes = nb.shape[1:]
    used = 96
    half = 768
    own = slice(0, half)
    xrow = slice(half, half + used)
    both = slice(0, half + used)
    oth = slice(half, 2 * half)
    oth_rows = slice(half + used, 2 * half + used)

    def rcopy(src, dst, ssem, rsem, dev):
        return pltpu.make_async_remote_copy(src_ref=src, dst_ref=dst, send_sem=ssem, recv_sem=rsem, device_id=dev, device_id_type=MESH)

    barrier = pltpu.get_barrier_semaphore()

    @pl.loop(1, 64)
    def _(o):
        pl.semaphore_signal(barrier, inc=1, device_id={"data": (me + o) % 64}, device_id_type=MESH)

    pl.semaphore_signal(barrier, inc=1, device_id=sib, device_id_type=MESH)

    load_m = pltpu.make_async_copy(m_hbm, mv, in_s.at[0])
    load_g = pltpu.make_async_copy(g_hbm, gv, in_s.at[1])
    load_m.start()
    load_g.start()
    load_m.wait()
    load_g.wait()
    lane = lax.broadcasted_iota(jnp.int32, (rows_src, lanes), 1)

    def group(g, ssq):
        tiles = []
        for r in range(3):
            cs = pl.ds(pl.multiple_of((g * 3 + r) * 128, 128), 128)
            grad = gv[:, cs].astype(F32)
            new_mom = MOMENTUM * mv[:, cs] + grad
            nest = grad + MOMENTUM * new_mom
            nb[g * 4 + r] = nest
            ssq = ssq + nest * nest
            tiles.append(pltpu.roll(nest, 32 * (r + 1), 1))
        nb[g * 4 + 3] = jnp.where(lane < 32, tiles[0], jnp.where(lane < 64, tiles[1], tiles[2]))
        return ssq

    ssq = lax.fori_loop(0, 16, group, jnp.zeros((rows_src, lanes), F32))
    ssq = jnp.sum(jnp.sum(ssq, axis=0, keepdims=True), axis=1, keepdims=True)
    lane8 = lax.broadcasted_iota(jnp.int32, (8, lanes), 1)

    @pl.loop(0, 64)
    def _(d):
        nb[d, 0:8] = jnp.where(lane8 < used, nb[d, 0:8], ssq)

    pl.semaphore_wait(barrier, 64)

    slot = (me + 32 * t) % 64

    @pl.loop(1, 64)
    def _(o):
        d = (me + o) % 64
        rcopy(nb.at[d], rx.at[slot], a2a_s, a2a_r, {"data": d}).start()

    rx[slot] = nb[me]

    rcopy(nb.at[pl.ds(0, 63)], rx.at[pl.ds(0, 63)], a2a_s, a2a_r, sib).wait()

    sq[0] = jnp.sum(rx[:, 0:8, :], axis=0)
    c = rcopy(sq.at[0], sq.at[1], sq_s, sq_r, sib)
    c.start()
    c.wait()
    total = (sq[0] + sq[1])[0:1, lanes - 1:lanes]
    norm = jnp.sqrt(total) + EPSILON
    lane_ok = lax.broadcasted_iota(jnp.int32, (384, lanes), 1) < used

    def xg_copy(h):
        return rcopy(xg.at[pl.ds(h * half, half), pl.ds(0, 128)], xg.at[pl.ds((1 - h) * half, half), pl.ds(128, 128)], xg_s, xg_r, sib)

    for i in range(4):
        v = rx[pl.ds(i * 16, 16)].reshape(384, lanes)
        x = jnp.where(lane_ok, v / norm, 0.0).astype(BF16)
        xg[pl.ds(pl.multiple_of(i * 384, 384), 384), 0:128] = x
        af[xrow, pl.ds(pl.multiple_of(i * 384, 384), 384)] = x.astype(F32).T[0:used].astype(BF16)
        if i % 2 == 1:
            xg_copy(i // 2).start()
    rcopy(xg.at[:, pl.ds(0, 128)], xg.at[:, pl.ds(128, 128)], xg_s, xg_r, sib).wait()

    def peer(dim, o):
        m = coord[dim]
        return {"data": me + ((m + o) % 4 - m) * STRIDES[dim]}

    def dims(col):
        return col, (col + 1) % 3, (col + 2) % 3

    first, second = pl.ds(0, 8), pl.ds(8, 8)

    def near(col, src, dst, k, o):
        return rcopy(src, dst, near_s.at[col], near_r.at[col * 3 + k], peer(dims(col)[0], o))

    def near_start(col):
        m = coord[dims(col)[0]]
        up, down, far = (m + 1) % 4, (m + 3) % 4, (m + 2) % 4
        near(col, part.at[col, far, first], rb1.at[col, 2, first], 0, 1).start()
        near(col, part.at[col, far, second], rb1.at[col, 2, second], 1, 3).start()
        near(col, part.at[col, up, second], rb1.at[col, 0, second], 2, 1).start()
        near(col, part.at[col, down, first], rb1.at[col, 1, first], 2, 3).start()

    def near_merge(col):
        m = coord[dims(col)[0]]
        up, down = (m + 1) % 4, (m + 3) % 4
        near(col, part.at[col, up, first], rb1.at[col, 2, first], 0, 1).wait_recv()
        part[col, up, first] = part[col, up, first] + rb1[col, 2, first]
        near(col, part.at[col, up, first], rb1.at[col, 0, first], 2, 1).start()
        near(col, part.at[col, down, second], rb1.at[col, 2, second], 1, 3).wait_recv()
        part[col, down, second] = part[col, down, second] + rb1[col, 2, second]
        near(col, part.at[col, down, second], rb1.at[col, 1, second], 2, 3).start()

    def near_wait(col):
        two = rb1.at[col, pl.ds(0, 2)]
        near(col, two, two, 2, 1).wait_recv()
        near(col, rb1.at[col], rb1.at[col], 2, 1).wait_send()

    low, high = pl.ds(0, 2), pl.ds(2, 2)

    def fwd(col, block, rows, k, o):
        ref = gath.at[col, block, rows]
        return rcopy(ref, ref, fwd_s.at[col], fwd_r.at[col * 4 + k], peer(dims(col)[0], o))

    def fwd_start(col):
        m = coord[dims(col)[0]]
        fwd(col, m, low, 0, 1).start()
        fwd(col, m, high, 1, 3).start()
        fwd(col, m, high, 2, 1).start()
        fwd(col, m, low, 2, 3).start()

    def fwd_pass(col):
        m = coord[dims(col)[0]]
        up, down = (m + 1) % 4, (m + 3) % 4
        fwd(col, down, low, 0, 1).wait_recv()
        fwd(col, down, low, 3, 1).start()
        fwd(col, up, high, 1, 3).wait_recv()
        fwd(col, up, high, 3, 3).start()

    def fwd_wait(col, k):
        one = gath.at[col, 0]
        rcopy(one, one, fwd_s.at[col], fwd_r.at[col * 4 + k], sib).wait_recv()

    def fwd_sent(col):
        three = gath.at[col, pl.ds(0, 3)]
        rcopy(three, three, fwd_s.at[col], fwd_r.at[col * 4 + 2], sib).wait_send()

    def mid_copy(col, o):
        d = dims(col)[1]
        j = (coord[d] + o) % 4
        return rcopy(s1.at[col, j], rb2.at[col, o - 1], rs_s.at[col], rs_r.at[col], peer(d, o))

    def small_copy(col, o):
        d = dims(col)[2]
        return rcopy(s2.at[col], rb3.at[col, coord[d]], rs_s.at[3 + col], rs_r.at[3 + col], peer(d, o))

    def ag_copy(col, o):
        m1, m2 = (coord[d] for d in dims(col)[:2])
        ref = gath.at[col, m1, m2]
        return rcopy(ref, ref, rs_s.at[6 + col], rs_r.at[6 + col], peer(dims(col)[1], o))

    def wait_three(ref, k):
        rcopy(ref, ref, rs_s.at[k], rs_r.at[k], sib).wait()

    for col in range(3):
        for b in range(4):
            i, j = BLOCKS[col * 4 + b]
            res = lax.dot_general(xg[i * 256:(i + 1) * 256, :], xg[j * 256:(j + 1) * 256, :], (((1,), (1,)), ((), ())), preferred_element_type=F32)
            for h in range(2):
                part[col, b, h * 8:(h + 1) * 8] = res[:, h * 128:(h + 1) * 128].reshape(8, 32, 128)
        near_start(col)
    for col in range(3):
        near_merge(col)
    for col in range(3):
        near_wait(col)
        s1[col] = (part[col, coord[dims(col)[0]]] + rb1[col, 0] + rb1[col, 1]).reshape(4, 4, 32, 128)
        for o in range(1, 4):
            mid_copy(col, o).start()
    for col in range(3):
        wait_three(rb2.at[col], col)
        total = s1[col, coord[dims(col)[1]]] + rb2[col, 0] + rb2[col, 1] + rb2[col, 2]
        s2[col] = total
        for o in range(1, 4):
            small_copy(col, o).start()
        rb3[col, coord[dims(col)[2]]] = total
    for col in range(3):
        wait_three(rb3.at[col, pl.ds(0, 3)], 3 + col)
        m1, m2 = (coord[d] for d in dims(col)[:2])
        gath[col, m1, m2] = (rb3[col, 0] + rb3[col, 1]) + (rb3[col, 2] + rb3[col, 3])
        for o in range(1, 4):
            ag_copy(col, o).start()
    for col in range(3):
        wait_three(gath.at[col, 0, pl.ds(0, 3)], 6 + col)
        fwd_start(col)

    base = half + used

    def lookup(values, at):
        out = values[3]
        for n in range(3):
            out = jnp.where(at == n, values[n], out)
        return out

    def to_sibling(r, c, rows, cols_n, r2, c2):
        rcopy(af.at[pl.ds(r, rows), pl.ds(c, cols_n)], af.at[pl.ds(r2, rows), pl.ds(c2, cols_n)], pa_s, pa_r, sib).start()

    def al256(v):
        return pl.multiple_of(v, 256)

    def al128(v):
        return pl.multiple_of(v, 128)

    def place(col, b, h):
        quad = BLOCKS[col * 4:col * 4 + 4]
        i = lookup([p[0] for p in quad], b)
        j = lookup([p[1] for p in quad], b)
        v = gath[col, b, 2 * h:2 * h + 2].reshape(256, 128)
        r, c = al256(i * 256), al128(j * 256 + h * 128)
        gram[pl.ds(r, 256), pl.ds(c, 128)] = v
        af[pl.ds(r, 256), pl.ds(c, 128)] = v.astype(BF16)
        to_sibling(r, c, 256, 128, base + r, al128((j + 3) % 6 * 256 + h * 128))
        mirrored = [n for n in range(4) if quad[n][1] < quad[n][0]]
        swapped = [n for n in range(4) if col * 4 + n in SWAPPED]
        if mirrored:
            hit = b == mirrored[0]
            for n in mirrored[1:]:
                hit = hit | (b == n)

            @pl.when(hit)
            def _():
                vt = v.T
                r2, c2 = al128(j * 256 + h * 128), al256(i * 256)
                gram[pl.ds(r2, 128), pl.ds(c2, 256)] = vt
                af[pl.ds(r2, 128), pl.ds(c2, 256)] = vt.astype(BF16)
                to_sibling(r2, c2, 128, 256, base + r2, al256((i + 3) * 256))

        for n in swapped:
            i0, j0 = quad[n]
            k = SWAPPED.index(col * 4 + n)

            @pl.when(b == n)
            def _():
                vt = v.T
                r2 = (j0 - 3) * 256 + h * 128
                swap[k, h] = vt
                rcopy(swap.at[k, h], gram.at[pl.ds(r2, 128), pl.ds((i0 + 3) * 256, 256)], sw_s, sw_r, sib).start()
                af[base + r2:base + r2 + 128, i0 * 256:(i0 + 1) * 256] = vt.astype(BF16)

    ring = [coord[dims(col)[0]] for col in range(3)]
    for col in range(3):
        for h in range(2):
            place(col, ring[col], h)
    for col in range(3):
        fwd_pass(col)
    for col in range(3):
        place(col, (ring[col] + 3) % 4, 0)
        place(col, (ring[col] + 1) % 4, 1)
    for col in range(3):
        fwd_wait(col, 2)
        place(col, (ring[col] + 3) % 4, 1)
        place(col, (ring[col] + 1) % 4, 0)
    for col in range(3):
        fwd_wait(col, 3)
        for h in range(2):
            place(col, (ring[col] + 2) % 4, h)
    for col in range(3):
        fwd_sent(col)
    rcopy(swap, swap, sw_s, sw_r, sib).wait()
    for n in range(3):
        i, j = BLOCKS[SWAPPED[n]]
        rs, cs = slice((j - 3) * 256, (j - 2) * 256), slice((i + 3) * 256, (i + 4) * 256)
        af[rs, cs] = gram[rs, cs].astype(BF16)

    def piece(buf, ssem, rsem, p):
        q = (p + 3) % 6
        base = buf.shape[0] - half
        return rcopy(buf.at[pl.ds(0, half), pl.ds(pl.multiple_of(p * 256, 256), 256)],
                     buf.at[pl.ds(base, half), pl.ds(pl.multiple_of(q * 256, 256), 256)], ssem, rsem, sib)

    def send_two(buf, ssem, rsem, n):
        piece(buf, ssem, rsem, 2 * n).start()
        piece(buf, ssem, rsem, 2 * n + 1).start()

    def wait_recv(buf, ssem, rsem, rows=768):
        rcopy(buf.at[pl.ds(0, rows)], buf.at[pl.ds(0, rows)], ssem, rsem, sib).wait_recv()

    def wait_send(buf, ssem, rsem, rows=768):
        rcopy(buf.at[pl.ds(0, rows)], buf.at[pl.ds(0, rows)], ssem, rsem, sib).wait_send()

    def diag_copy():
        return rcopy(dv.at[:, pl.ds(0, half)], dv.at[:, pl.ds(half, half)], dv_s, dv_r, sib)

    diag = lax.broadcasted_iota(jnp.int32, (128, 128), 0) == lax.broadcasted_iota(jnp.int32, (128, 128), 1)

    def poly_step(rows):
        mid[own, :] = dot(af[own, own], af[own, :])
        wait_recv(af, pa_s, pa_r, rows)

        for n in range(3):
            cs = slice(n * 512, n * 512 + 512)
            acc = mid[own, cs] + dot(af[own, oth], af[oth_rows, cs])
            bff[own, cs] = (COEF_B * af[own, cs].astype(F32) + COEF_C * acc).astype(BF16)
            for i in range(4 * n, min(4 * n + 4, 6)):
                ts = slice(i * 128, i * 128 + 128)
                tile = bff[ts, ts].astype(F32)
                on = jnp.sum(jnp.where(diag, tile, 0.0), axis=0, keepdims=True)
                dv[:, ts] = jnp.broadcast_to(COEF_A + on, (8, 128))
                bff[ts, ts] = jnp.where(diag, 0.0, tile).astype(BF16)
            send_two(bff, pb_s, pb_r, n)

        diag_copy().start()
        wait_send(af, pa_s, pa_r, rows)

    poly_step(640)

    @pl.loop(0, NS_STEPS - 1)
    def _(k):
        mid[both, :] = dot(af[both, own], bff[own, :])
        wait_recv(bff, pb_s, pb_r)
        diag_copy().wait_recv()
        v = mid[both, :] + dot(af[both, oth], bff[oth, :])
        q_diag = dv[0:1, :]
        top = v[own] + gram[...] * q_diag
        mid[own, :] = top
        tb[...] = top.astype(BF16)
        x_new = (v[xrow] + af[xrow, :].astype(F32) * q_diag).astype(BF16)
        af[xrow, :] = x_new

        for n in range(3):
            cs = slice(n * 512, n * 512 + 512)
            v = mid[own, cs] * dv[0:1, cs] + dot(tb[...], bff[:, cs])
            gram[:, cs] = v
            af[own, cs] = v.astype(BF16)
            send_two(af, pa_s, pa_r, n)

        wait_send(bff, pb_s, pb_r)
        diag_copy().wait_send()
        poly_step(768)

    mid[xrow, :] = dot(af[xrow, own], bff[own, :])
    wait_recv(bff, pb_s, pb_r)
    diag_copy().wait_recv()
    mid[xrow, :] = mid[xrow, :] + af[xrow, :].astype(F32) * dv[0:1, :] + dot(af[xrow, oth], bff[oth, :])
    wait_send(bff, pb_s, pb_r)
    diag_copy().wait_send()

    @pl.loop(0, 4)
    def _(i):
        v = mid[xrow, pl.ds(pl.multiple_of(i * 384, 384), 384)].astype(BF16).astype(F32)
        v = jnp.concatenate([v, jnp.zeros((lanes - used, 384), F32)], axis=0).T
        ys[pl.ds(i * 16, 16)] = v.reshape(16, 24, 128).astype(BF16)

    @pl.loop(1, 64)
    def _(o):
        d = (me + o) % 64
        rcopy(ys.at[(d + 32 * t) % 64], yr.at[me], out_s, out_r, {"data": d}).start()

    yr[me] = ys[slot]

    rcopy(ys.at[pl.ds(0, 63)], yr.at[pl.ds(0, 63)], out_s, out_r, sib).wait()

    @pl.loop(0, 16)
    def _(g):
        last = yr[g * 4 + 3].astype(F32)
        for r in range(3):
            x = jnp.where(lane < used, yr[g * 4 + r].astype(F32), pltpu.roll(last, 96 - 32 * r, 1))
            x_out[:, pl.ds(pl.multiple_of((g * 3 + r) * 128, 128), 128)] = x.astype(BF16)


def solution(mesh):
    data_size = mesh.shape["data"]
    tp_size = mesh.shape["tp"]
    part_spec = P(("stage", "data"), "tp")

    def local_step(weight, momentum, gradient):
        rows_local, cols_local = gradient.shape
        rows = rows_local * data_size
        sem = pltpu.SemaphoreType.DMA
        shapes = [
            pltpu.VMEM((24, 6144), F32), pltpu.VMEM((24, 6144), BF16),
            pltpu.VMEM((64, 24, 128), F32), pltpu.VMEM((64, 24, 128), F32), pltpu.VMEM((2, 8, 128), F32), pltpu.VMEM((1536, 256), BF16),
            pltpu.VMEM((3, 4, 16, 32, 128), F32), pltpu.VMEM((3, 3, 16, 32, 128), F32), pltpu.VMEM((3, 4, 4, 32, 128), F32),
            pltpu.VMEM((3, 3, 4, 32, 128), F32), pltpu.VMEM((3, 4, 32, 128), F32), pltpu.VMEM((3, 4, 4, 32, 128), F32),
            pltpu.VMEM((3, 4, 4, 4, 32, 128), F32), pltpu.VMEM((3, 2, 128, 256), F32),
            pltpu.VMEM((768, 1536), F32), pltpu.VMEM((864, 1536), F32), pltpu.VMEM((1632, 1536), BF16), pltpu.VMEM((1536, 1536), BF16),
            pltpu.VMEM((8, 1536), F32), pltpu.VMEM((768, 1536), BF16),
            pltpu.VMEM((64, 24, 128), BF16), pltpu.VMEM((64, 24, 128), BF16),
            sem((2,)), sem, sem, sem, sem, sem, sem, sem, sem, sem((3,)), sem((9,)), sem((3,)), sem((12,)), sem((9,)), sem((9,)),
            sem, sem, sem, sem, sem, sem, sem, sem,
        ]
        anywhere = pl.BlockSpec(memory_space=pl.ANY)
        x_fin = pl.pallas_call(
            kernel,
            out_shape=jax.ShapeDtypeStruct((rows_local, cols_local), BF16),
            in_specs=[anywhere] * 2,
            out_specs=pl.BlockSpec(memory_space=pltpu.VMEM),
            scratch_shapes=shapes,
            compiler_params=pltpu.CompilerParams(collective_id=0, has_side_effects=True, vmem_limit_bytes=VMEM_MIB * 1024 * 1024),
            name="muon_steps",
        )(momentum, gradient)
        new_mom = MOMENTUM * momentum + gradient.astype(F32)
        rms_scale = 0.2 * math.sqrt(max(rows, cols_local * tp_size))
        new_weight = weight - LEARN_RATE * (rms_scale * x_fin.astype(F32) + WEIGHT_DECAY * weight)
        return new_weight, new_mom

    return jax.shard_map(local_step, mesh=mesh, in_specs=(part_spec, part_spec, part_spec), out_specs=(part_spec, part_spec), check_vma=False)
```

```python
import functools
import math
import jax
import jax.numpy as jnp
from jax import lax
from jax.experimental import pallas as pl
from jax.experimental.pallas import tpu as pltpu
from jax.sharding import PartitionSpec as P

NS_STEPS = 5
MOMENTUM = 0.95
LEARN_RATE = 0.5
WEIGHT_DECAY = 0.1
COEF_A = 3.4445
COEF_B = -4.7750
COEF_C = 2.0315
EPSILON = 1e-7

MESH = pl.DeviceIdType.MESH
F32 = jnp.float32
BF16 = jnp.bfloat16
BLOCKS = ((0, 0), (1, 0), (1, 1), (2, 0), (2, 1), (2, 2), (0, 3), (0, 4), (0, 5), (1, 4), (1, 5), (2, 5))
SWAPPED = (7, 8, 10)
STRIDES = (1, 4, 16)
VMEM_MIB = 54


def dot(p, q):
    return jnp.dot(p, q, preferred_element_type=F32)


def kernel(m_hbm, g_hbm, x_out, mv, gv, nb, rx, sq, xg, part, rb1, s1, rb2, s2, rb3, gath, swap, gram, mid, af, bff, dv, tb, xs, xsend, xrecv, ys, yr,
           in_s, dv_s, dv_r, xs_s, xs_r, xp_s, xp_r, a2a_s, a2a_r, sq_s, sq_r, xg_s, xg_r, near_s, near_r, fwd_s, fwd_r, rs_s, rs_r, sw_s, sw_r, pa_s, pa_r, pb_s, pb_r, out_s, out_r):
    me = lax.axis_index("data")
    t = lax.axis_index("tp")
    sib = {"tp": 1 - t}
    coord = (me % 4, (me // 4) % 4, me // 16)
    rows_src, lanes = nb.shape[1:]
    used = 96
    half = 768
    own = slice(0, half)
    xrow = slice(half, half + used)
    both = slice(0, half + used)
    oth = slice(half, 2 * half)
    oth_rows = slice(half + used, 2 * half + used)

    def rcopy(src, dst, ssem, rsem, dev):
        return pltpu.make_async_remote_copy(src_ref=src, dst_ref=dst, send_sem=ssem, recv_sem=rsem, device_id=dev, device_id_type=MESH)

    barrier = pltpu.get_barrier_semaphore()

    @pl.loop(1, 64)
    def _(o):
        pl.semaphore_signal(barrier, inc=1, device_id={"data": (me + o) % 64}, device_id_type=MESH)

    pl.semaphore_signal(barrier, inc=1, device_id=sib, device_id_type=MESH)

    load_m = pltpu.make_async_copy(m_hbm, mv, in_s.at[0])
    load_g = pltpu.make_async_copy(g_hbm, gv, in_s.at[1])
    load_m.start()
    load_g.start()
    load_m.wait()
    load_g.wait()
    lane = lax.broadcasted_iota(jnp.int32, (rows_src, lanes), 1)

    def group(g, ssq):
        tiles = []
        for r in range(3):
            cs = pl.ds(pl.multiple_of((g * 3 + r) * 128, 128), 128)
            grad = gv[:, cs].astype(F32)
            new_mom = MOMENTUM * mv[:, cs] + grad
            nest = grad + MOMENTUM * new_mom
            nb[g * 4 + r] = nest
            ssq = ssq + nest * nest
            tiles.append(pltpu.roll(nest, 32 * (r + 1), 1))
        nb[g * 4 + 3] = jnp.where(lane < 32, tiles[0], jnp.where(lane < 64, tiles[1], tiles[2]))
        return ssq

    ssq = lax.fori_loop(0, 16, group, jnp.zeros((rows_src, lanes), F32))
    ssq = jnp.sum(jnp.sum(ssq, axis=0, keepdims=True), axis=1, keepdims=True)
    lane8 = lax.broadcasted_iota(jnp.int32, (8, lanes), 1)

    @pl.loop(0, 64)
    def _(d):
        nb[d, 0:8] = jnp.where(lane8 < used, nb[d, 0:8], ssq)

    pl.semaphore_wait(barrier, 64)

    slot = (me + 32 * t) % 64

    @pl.loop(1, 64)
    def _(o):
        d = (me + o) % 64
        rcopy(nb.at[d], rx.at[slot], a2a_s, a2a_r, {"data": d}).start()

    rx[slot] = nb[me]

    rcopy(nb.at[pl.ds(0, 63)], rx.at[pl.ds(0, 63)], a2a_s, a2a_r, sib).wait()

    sq[0] = jnp.sum(rx[:, 0:8, :], axis=0)
    c = rcopy(sq.at[0], sq.at[1], sq_s, sq_r, sib)
    c.start()
    c.wait()
    total = (sq[0] + sq[1])[0:1, lanes - 1:lanes]
    norm = jnp.sqrt(total) + EPSILON
    lane_ok = lax.broadcasted_iota(jnp.int32, (384, lanes), 1) < used

    def xg_copy(h):
        return rcopy(xg.at[pl.ds(h * half, half), pl.ds(0, 128)], xg.at[pl.ds((1 - h) * half, half), pl.ds(128, 128)], xg_s, xg_r, sib)

    for i in range(4):
        v = rx[pl.ds(i * 16, 16)].reshape(384, lanes)
        x = jnp.where(lane_ok, v / norm, 0.0).astype(BF16)
        xg[pl.ds(pl.multiple_of(i * 384, 384), 384), 0:128] = x
        af[xrow, pl.ds(pl.multiple_of(i * 384, 384), 384)] = x.astype(F32).T[0:used].astype(BF16)
        if i % 2 == 1:
            xg_copy(i // 2).start()
    rcopy(xg.at[:, pl.ds(0, 128)], xg.at[:, pl.ds(128, 128)], xg_s, xg_r, sib).wait()

    def peer(dim, o):
        m = coord[dim]
        return {"data": me + ((m + o) % 4 - m) * STRIDES[dim]}

    def dims(col):
        return col, (col + 1) % 3, (col + 2) % 3

    first, second = pl.ds(0, 8), pl.ds(8, 8)

    def near(col, src, dst, k, o):
        return rcopy(src, dst, near_s.at[col], near_r.at[col * 3 + k], peer(dims(col)[0], o))

    def near_start(col):
        m = coord[dims(col)[0]]
        up, down, far = (m + 1) % 4, (m + 3) % 4, (m + 2) % 4
        near(col, part.at[col, far, first], rb1.at[col, 2, first], 0, 1).start()
        near(col, part.at[col, far, second], rb1.at[col, 2, second], 1, 3).start()
        near(col, part.at[col, up, second], rb1.at[col, 0, second], 2, 1).start()
        near(col, part.at[col, down, first], rb1.at[col, 1, first], 2, 3).start()

    def near_merge(col):
        m = coord[dims(col)[0]]
        up, down = (m + 1) % 4, (m + 3) % 4
        near(col, part.at[col, up, first], rb1.at[col, 2, first], 0, 1).wait_recv()
        part[col, up, first] = part[col, up, first] + rb1[col, 2, first]
        near(col, part.at[col, up, first], rb1.at[col, 0, first], 2, 1).start()
        near(col, part.at[col, down, second], rb1.at[col, 2, second], 1, 3).wait_recv()
        part[col, down, second] = part[col, down, second] + rb1[col, 2, second]
        near(col, part.at[col, down, second], rb1.at[col, 1, second], 2, 3).start()

    def near_wait(col):
        two = rb1.at[col, pl.ds(0, 2)]
        near(col, two, two, 2, 1).wait_recv()
        near(col, rb1.at[col], rb1.at[col], 2, 1).wait_send()

    low, high = pl.ds(0, 2), pl.ds(2, 2)

    def fwd(col, block, rows, k, o):
        ref = gath.at[col, block, rows]
        return rcopy(ref, ref, fwd_s.at[col], fwd_r.at[col * 4 + k], peer(dims(col)[0], o))

    def fwd_start(col):
        m = coord[dims(col)[0]]
        fwd(col, m, low, 0, 1).start()
        fwd(col, m, high, 1, 3).start()
        fwd(col, m, high, 2, 1).start()
        fwd(col, m, low, 2, 3).start()

    def fwd_pass(col):
        m = coord[dims(col)[0]]
        up, down = (m + 1) % 4, (m + 3) % 4
        fwd(col, down, low, 0, 1).wait_recv()
        fwd(col, down, low, 3, 1).start()
        fwd(col, up, high, 1, 3).wait_recv()
        fwd(col, up, high, 3, 3).start()

    def fwd_wait(col, k):
        one = gath.at[col, 0]
        rcopy(one, one, fwd_s.at[col], fwd_r.at[col * 4 + k], sib).wait_recv()

    def fwd_sent(col):
        three = gath.at[col, pl.ds(0, 3)]
        rcopy(three, three, fwd_s.at[col], fwd_r.at[col * 4 + 2], sib).wait_send()

    def mid_copy(col, o):
        d = dims(col)[1]
        j = (coord[d] + o) % 4
        return rcopy(s1.at[col, j], rb2.at[col, o - 1], rs_s.at[col], rs_r.at[col], peer(d, o))

    def small_copy(col, o):
        d = dims(col)[2]
        return rcopy(s2.at[col], rb3.at[col, coord[d]], rs_s.at[3 + col], rs_r.at[3 + col], peer(d, o))

    def ag_copy(col, o):
        m1, m2 = (coord[d] for d in dims(col)[:2])
        ref = gath.at[col, m1, m2]
        return rcopy(ref, ref, rs_s.at[6 + col], rs_r.at[6 + col], peer(dims(col)[1], o))

    def wait_three(ref, k):
        rcopy(ref, ref, rs_s.at[k], rs_r.at[k], sib).wait()

    for col in range(3):
        for b in range(4):
            i, j = BLOCKS[col * 4 + b]
            res = lax.dot_general(xg[i * 256:(i + 1) * 256, :], xg[j * 256:(j + 1) * 256, :], (((1,), (1,)), ((), ())), preferred_element_type=F32)
            for h in range(2):
                part[col, b, h * 8:(h + 1) * 8] = res[:, h * 128:(h + 1) * 128].reshape(8, 32, 128)
        near_start(col)
    for col in range(3):
        near_merge(col)
    for col in range(3):
        near_wait(col)
        s1[col] = (part[col, coord[dims(col)[0]]] + rb1[col, 0] + rb1[col, 1]).reshape(4, 4, 32, 128)
        for o in range(1, 4):
            mid_copy(col, o).start()
    for col in range(3):
        wait_three(rb2.at[col], col)
        total = s1[col, coord[dims(col)[1]]] + rb2[col, 0] + rb2[col, 1] + rb2[col, 2]
        s2[col] = total
        for o in range(1, 4):
            small_copy(col, o).start()
        rb3[col, coord[dims(col)[2]]] = total
    for col in range(3):
        wait_three(rb3.at[col, pl.ds(0, 3)], 3 + col)
        m1, m2 = (coord[d] for d in dims(col)[:2])
        gath[col, m1, m2] = (rb3[col, 0] + rb3[col, 1]) + (rb3[col, 2] + rb3[col, 3])
        for o in range(1, 4):
            ag_copy(col, o).start()
    for col in range(3):
        wait_three(gath.at[col, 0, pl.ds(0, 3)], 6 + col)
        fwd_start(col)

    base = half + used

    def lookup(values, at):
        out = values[3]
        for n in range(3):
            out = jnp.where(at == n, values[n], out)
        return out

    def to_sibling(r, c, rows, cols_n, r2, c2):
        rcopy(af.at[pl.ds(r, rows), pl.ds(c, cols_n)], af.at[pl.ds(r2, rows), pl.ds(c2, cols_n)], pa_s, pa_r, sib).start()

    def al256(v):
        return pl.multiple_of(v, 256)

    def al128(v):
        return pl.multiple_of(v, 128)

    def place(col, b, h):
        quad = BLOCKS[col * 4:col * 4 + 4]
        i = lookup([p[0] for p in quad], b)
        j = lookup([p[1] for p in quad], b)
        v = gath[col, b, 2 * h:2 * h + 2].reshape(256, 128)
        r, c = al256(i * 256), al128(j * 256 + h * 128)
        gram[pl.ds(r, 256), pl.ds(c, 128)] = v
        af[pl.ds(r, 256), pl.ds(c, 128)] = v.astype(BF16)
        to_sibling(r, c, 256, 128, base + r, al128((j + 3) % 6 * 256 + h * 128))
        mirrored = [n for n in range(4) if quad[n][1] < quad[n][0]]
        swapped = [n for n in range(4) if col * 4 + n in SWAPPED]
        if mirrored:
            hit = b == mirrored[0]
            for n in mirrored[1:]:
                hit = hit | (b == n)

            @pl.when(hit)
            def _():
                vt = v.T
                r2, c2 = al128(j * 256 + h * 128), al256(i * 256)
                gram[pl.ds(r2, 128), pl.ds(c2, 256)] = vt
                af[pl.ds(r2, 128), pl.ds(c2, 256)] = vt.astype(BF16)
                to_sibling(r2, c2, 128, 256, base + r2, al256((i + 3) * 256))

        for n in swapped:
            i0, j0 = quad[n]
            k = SWAPPED.index(col * 4 + n)

            @pl.when(b == n)
            def _():
                vt = v.T
                r2 = (j0 - 3) * 256 + h * 128
                swap[k, h] = vt
                rcopy(swap.at[k, h], gram.at[pl.ds(r2, 128), pl.ds((i0 + 3) * 256, 256)], sw_s, sw_r, sib).start()
                af[base + r2:base + r2 + 128, i0 * 256:(i0 + 1) * 256] = vt.astype(BF16)

    ring = [coord[dims(col)[0]] for col in range(3)]
    for col in range(3):
        for h in range(2):
            place(col, ring[col], h)
    for col in range(3):
        fwd_pass(col)
    for col in range(3):
        place(col, (ring[col] + 3) % 4, 0)
        place(col, (ring[col] + 1) % 4, 1)
    for col in range(3):
        fwd_wait(col, 2)
        place(col, (ring[col] + 3) % 4, 1)
        place(col, (ring[col] + 1) % 4, 0)
    for col in range(3):
        fwd_wait(col, 3)
        for h in range(2):
            place(col, (ring[col] + 2) % 4, h)
    for col in range(3):
        fwd_sent(col)
    rcopy(swap, swap, sw_s, sw_r, sib).wait()
    for n in range(3):
        i, j = BLOCKS[SWAPPED[n]]
        rs, cs = slice((j - 3) * 256, (j - 2) * 256), slice((i + 3) * 256, (i + 4) * 256)
        af[rs, cs] = gram[rs, cs].astype(BF16)

    def piece(buf, ssem, rsem, p):
        q = (p + 3) % 6
        base = buf.shape[0] - half
        return rcopy(buf.at[pl.ds(0, half), pl.ds(pl.multiple_of(p * 256, 256), 256)],
                     buf.at[pl.ds(base, half), pl.ds(pl.multiple_of(q * 256, 256), 256)], ssem, rsem, sib)

    def send_two(buf, ssem, rsem, n):
        piece(buf, ssem, rsem, 2 * n).start()
        piece(buf, ssem, rsem, 2 * n + 1).start()

    def wait_recv(buf, ssem, rsem, rows=768):
        rcopy(buf.at[pl.ds(0, rows)], buf.at[pl.ds(0, rows)], ssem, rsem, sib).wait_recv()

    def wait_send(buf, ssem, rsem, rows=768):
        rcopy(buf.at[pl.ds(0, rows)], buf.at[pl.ds(0, rows)], ssem, rsem, sib).wait_send()

    def diag_copy():
        return rcopy(dv.at[:, pl.ds(0, half)], dv.at[:, pl.ds(half, half)], dv_s, dv_r, sib)

    diag = lax.broadcasted_iota(jnp.int32, (128, 128), 0) == lax.broadcasted_iota(jnp.int32, (128, 128), 1)

    def poly_step(rows):
        mid[own, :] = dot(af[own, own], af[own, :])
        wait_recv(af, pa_s, pa_r, rows)

        for n in range(3):
            cs = slice(n * 512, n * 512 + 512)
            acc = mid[own, cs] + dot(af[own, oth], af[oth_rows, cs])
            bff[own, cs] = (COEF_B * af[own, cs].astype(F32) + COEF_C * acc).astype(BF16)
            for i in range(4 * n, min(4 * n + 4, 6)):
                ts = slice(i * 128, i * 128 + 128)
                tile = bff[ts, ts].astype(F32)
                on = jnp.sum(jnp.where(diag, tile, 0.0), axis=0, keepdims=True)
                dv[:, ts] = jnp.broadcast_to(COEF_A + on, (8, 128))
                bff[ts, ts] = jnp.where(diag, 0.0, tile).astype(BF16)
            send_two(bff, pb_s, pb_r, n)

        diag_copy().start()
        wait_send(af, pa_s, pa_r, rows)

    poly_step(640)

    @pl.loop(0, NS_STEPS - 1)
    def _(k):
        mid[both, :] = dot(af[both, own], bff[own, :])
        wait_recv(bff, pb_s, pb_r)
        diag_copy().wait_recv()
        v = mid[both, :] + dot(af[both, oth], bff[oth, :])
        q_diag = dv[0:1, :]
        top = v[own] + gram[...] * q_diag
        mid[own, :] = top
        tb[...] = top.astype(BF16)
        x_new = (v[xrow] + af[xrow, :].astype(F32) * q_diag).astype(BF16)
        af[xrow, :] = x_new

        for n in range(3):
            cs = slice(n * 512, n * 512 + 512)
            v = mid[own, cs] * dv[0:1, cs] + dot(tb[...], bff[:, cs])
            gram[:, cs] = v
            af[own, cs] = v.astype(BF16)
            send_two(af, pa_s, pa_r, n)

        wait_send(bff, pb_s, pb_r)
        diag_copy().wait_send()

        @pl.when(k < NS_STEPS - 2)
        def _():
            poly_step(768)

    share = rcopy(af.at[pl.ds(half, used), pl.ds(half, half)], xs, xs_s, xs_r, sib)
    share.start()
    mid[own, :] = dot(af[own, own], af[own, :])
    wait_recv(af, pa_s, pa_r)
    share.wait()
    pair = jnp.concatenate([af[xrow, own], xs[...]], axis=0)
    for n in range(3):
        cs = slice(n * 512, n * 512 + 512)
        acc = mid[own, cs] + dot(af[own, oth], af[oth_rows, cs])
        bff[own, cs] = (COEF_B * af[own, cs].astype(F32) + COEF_C * acc).astype(BF16)
        v = dot(pair, bff[own, cs])
        mid[xrow, cs] = COEF_A * af[xrow, cs].astype(F32) + v[0:used]
        xsend[:, cs] = v[used:2 * used]
        for p in (2 * n, 2 * n + 1):
            rcopy(xsend.at[:, pl.ds(p * 256, 256)], xrecv.at[:, pl.ds((p + 3) % 6 * 256, 256)], xp_s, xp_r, sib).start()
    wait_send(af, pa_s, pa_r)
    rcopy(xsend, xrecv, xp_s, xp_r, sib).wait()
    mid[xrow, :] = mid[xrow, :] + xrecv[...]

    @pl.loop(0, 4)
    def _(i):
        v = mid[xrow, pl.ds(pl.multiple_of(i * 384, 384), 384)].astype(BF16).astype(F32)
        v = jnp.concatenate([v, jnp.zeros((lanes - used, 384), F32)], axis=0).T
        ys[pl.ds(i * 16, 16)] = v.reshape(16, 24, 128).astype(BF16)

    @pl.loop(1, 64)
    def _(o):
        d = (me + o) % 64
        rcopy(ys.at[(d + 32 * t) % 64], yr.at[me], out_s, out_r, {"data": d}).start()

    yr[me] = ys[slot]

    rcopy(ys.at[pl.ds(0, 63)], yr.at[pl.ds(0, 63)], out_s, out_r, sib).wait()

    @pl.loop(0, 16)
    def _(g):
        last = yr[g * 4 + 3].astype(F32)
        for r in range(3):
            x = jnp.where(lane < used, yr[g * 4 + r].astype(F32), pltpu.roll(last, 96 - 32 * r, 1))
            x_out[:, pl.ds(pl.multiple_of((g * 3 + r) * 128, 128), 128)] = x.astype(BF16)


def solution(mesh):
    data_size = mesh.shape["data"]
    tp_size = mesh.shape["tp"]
    part_spec = P(("stage", "data"), "tp")

    def local_step(weight, momentum, gradient):
        rows_local, cols_local = gradient.shape
        rows = rows_local * data_size
        sem = pltpu.SemaphoreType.DMA
        shapes = [
            pltpu.VMEM((24, 6144), F32), pltpu.VMEM((24, 6144), BF16),
            pltpu.VMEM((64, 24, 128), F32), pltpu.VMEM((64, 24, 128), F32), pltpu.VMEM((2, 8, 128), F32), pltpu.VMEM((1536, 256), BF16),
            pltpu.VMEM((3, 4, 16, 32, 128), F32), pltpu.VMEM((3, 3, 16, 32, 128), F32), pltpu.VMEM((3, 4, 4, 32, 128), F32),
            pltpu.VMEM((3, 3, 4, 32, 128), F32), pltpu.VMEM((3, 4, 32, 128), F32), pltpu.VMEM((3, 4, 4, 32, 128), F32),
            pltpu.VMEM((3, 4, 4, 4, 32, 128), F32), pltpu.VMEM((3, 2, 128, 256), F32),
            pltpu.VMEM((768, 1536), F32), pltpu.VMEM((864, 1536), F32), pltpu.VMEM((1632, 1536), BF16), pltpu.VMEM((1536, 1536), BF16),
            pltpu.VMEM((8, 1536), F32), pltpu.VMEM((768, 1536), BF16),
            pltpu.VMEM((96, 768), BF16), pltpu.VMEM((96, 1536), F32), pltpu.VMEM((96, 1536), F32),
            pltpu.VMEM((64, 24, 128), BF16), pltpu.VMEM((64, 24, 128), BF16),
            sem((2,)), sem, sem, sem, sem, sem, sem, sem, sem, sem, sem, sem, sem, sem((3,)), sem((9,)), sem((3,)), sem((12,)), sem((9,)), sem((9,)),
            sem, sem, sem, sem, sem, sem, sem, sem,
        ]
        anywhere = pl.BlockSpec(memory_space=pl.ANY)
        x_fin = pl.pallas_call(
            kernel,
            out_shape=jax.ShapeDtypeStruct((rows_local, cols_local), BF16),
            in_specs=[anywhere] * 2,
            out_specs=pl.BlockSpec(memory_space=pltpu.VMEM),
            scratch_shapes=shapes,
            compiler_params=pltpu.CompilerParams(collective_id=0, has_side_effects=True, vmem_limit_bytes=VMEM_MIB * 1024 * 1024),
            name="muon_steps",
        )(momentum, gradient)
        new_mom = MOMENTUM * momentum + gradient.astype(F32)
        rms_scale = 0.2 * math.sqrt(max(rows, cols_local * tp_size))
        new_weight = weight - LEARN_RATE * (rms_scale * x_fin.astype(F32) + WEIGHT_DECAY * weight)
        return new_weight, new_mom

    return jax.shard_map(local_step, mesh=mesh, in_specs=(part_spec, part_spec, part_spec), out_specs=(part_spec, part_spec), check_vma=False)
```

```python
import functools
import math
import jax
import jax.numpy as jnp
from jax import lax
from jax.experimental import pallas as pl
from jax.experimental.pallas import tpu as pltpu
from jax.sharding import PartitionSpec as P

NS_STEPS = 5
MOMENTUM = 0.95
LEARN_RATE = 0.5
WEIGHT_DECAY = 0.1
COEF_A = 3.4445
COEF_B = -4.7750
COEF_C = 2.0315
EPSILON = 1e-7

MESH = pl.DeviceIdType.MESH
F32 = jnp.float32
BF16 = jnp.bfloat16
BLOCKS = ((0, 0), (1, 0), (1, 1), (2, 0), (2, 1), (2, 2), (0, 3), (0, 4), (0, 5), (1, 4), (1, 5), (2, 5))
SWAPPED = (7, 8, 10)
STRIDES = (1, 4, 16)
VMEM_MIB = 54


def dot(p, q):
    return jnp.dot(p, q, preferred_element_type=F32)


def kernel(m_hbm, g_hbm, x_out, mv, gv, nb, rx, sq, xg, part, rb1, s1, rb2, s2, rb3, gath, swap, gram, mid, af, bff, dv, tb, xs, xsend, xrecv, ys, yr,
           in_s, dv_s, dv_r, xs_s, xs_r, xp_s, xp_r, a2a_s, a2a_r, sq_s, sq_r, xg_s, xg_r, near_s, near_r, fwd_s, fwd_r, rs_s, rs_r, sw_s, sw_r, pa_s, pa_r, pb_s, pb_r, out_s, out_r):
    me = lax.axis_index("data")
    t = lax.axis_index("tp")
    sib = {"tp": 1 - t}
    coord = (me % 4, (me // 4) % 4, me // 16)
    rows_src, lanes = nb.shape[1:]
    used = 96
    half = 768
    own = slice(0, half)
    xrow = slice(half, half + used)
    both = slice(0, half + used)
    oth = slice(half, 2 * half)
    oth_rows = slice(half + used, 2 * half + used)

    def rcopy(src, dst, ssem, rsem, dev):
        return pltpu.make_async_remote_copy(src_ref=src, dst_ref=dst, send_sem=ssem, recv_sem=rsem, device_id=dev, device_id_type=MESH)

    barrier = pltpu.get_barrier_semaphore()

    @pl.loop(1, 64)
    def _(o):
        pl.semaphore_signal(barrier, inc=1, device_id={"data": (me + o) % 64}, device_id_type=MESH)

    pl.semaphore_signal(barrier, inc=1, device_id=sib, device_id_type=MESH)

    load_m = pltpu.make_async_copy(m_hbm, mv, in_s.at[0])
    load_g = pltpu.make_async_copy(g_hbm, gv, in_s.at[1])
    load_m.start()
    load_g.start()
    load_m.wait()
    load_g.wait()
    lane = lax.broadcasted_iota(jnp.int32, (rows_src, lanes), 1)

    def group(g, ssq):
        tiles = []
        for r in range(3):
            cs = pl.ds(pl.multiple_of((g * 3 + r) * 128, 128), 128)
            grad = gv[:, cs].astype(F32)
            new_mom = MOMENTUM * mv[:, cs] + grad
            nest = grad + MOMENTUM * new_mom
            nb[g * 4 + r] = nest
            ssq = ssq + nest * nest
            tiles.append(pltpu.roll(nest, 32 * (r + 1), 1))
        nb[g * 4 + 3] = jnp.where(lane < 32, tiles[0], jnp.where(lane < 64, tiles[1], tiles[2]))
        return ssq

    ssq = lax.fori_loop(0, 16, group, jnp.zeros((rows_src, lanes), F32))
    ssq = jnp.sum(jnp.sum(ssq, axis=0, keepdims=True), axis=1, keepdims=True)
    lane8 = lax.broadcasted_iota(jnp.int32, (8, lanes), 1)

    @pl.loop(0, 64)
    def _(d):
        nb[d, 0:8] = jnp.where(lane8 < used, nb[d, 0:8], ssq)

    pl.semaphore_wait(barrier, 64)

    slot = (me + 32 * t) % 64

    @pl.loop(1, 64)
    def _(o):
        d = (me + o) % 64
        rcopy(nb.at[d], rx.at[slot], a2a_s, a2a_r, {"data": d}).start()

    rx[slot] = nb[me]

    rcopy(nb.at[pl.ds(0, 63)], rx.at[pl.ds(0, 63)], a2a_s, a2a_r, sib).wait()

    sq[0] = jnp.sum(rx[:, 0:8, :], axis=0)
    c = rcopy(sq.at[0], sq.at[1], sq_s, sq_r, sib)
    c.start()
    c.wait()
    total = (sq[0] + sq[1])[0:1, lanes - 1:lanes]
    norm = jnp.sqrt(total) + EPSILON
    lane_ok = lax.broadcasted_iota(jnp.int32, (384, lanes), 1) < used

    def xg_copy(h):
        return rcopy(xg.at[pl.ds(h * half, half), pl.ds(0, 128)], xg.at[pl.ds((1 - h) * half, half), pl.ds(128, 128)], xg_s, xg_r, sib)

    for i in range(4):
        v = rx[pl.ds(i * 16, 16)].reshape(384, lanes)
        x = jnp.where(lane_ok, v / norm, 0.0).astype(BF16)
        xg[pl.ds(pl.multiple_of(i * 384, 384), 384), 0:128] = x
        af[xrow, pl.ds(pl.multiple_of(i * 384, 384), 384)] = x.astype(F32).T[0:used].astype(BF16)
        if i % 2 == 1:
            xg_copy(i // 2).start()
    rcopy(xg.at[:, pl.ds(0, 128)], xg.at[:, pl.ds(128, 128)], xg_s, xg_r, sib).wait()

    def peer(dim, o):
        m = coord[dim]
        return {"data": me + ((m + o) % 4 - m) * STRIDES[dim]}

    def dims(col):
        return col, (col + 1) % 3, (col + 2) % 3

    first, second = pl.ds(0, 8), pl.ds(8, 8)

    def near(col, src, dst, k, o):
        return rcopy(src, dst, near_s.at[col], near_r.at[col * 3 + k], peer(dims(col)[0], o))

    def near_start(col):
        m = coord[dims(col)[0]]
        up, down, far = (m + 1) % 4, (m + 3) % 4, (m + 2) % 4
        near(col, part.at[col, far, first], rb1.at[col, 2, first], 0, 1).start()
        near(col, part.at[col, far, second], rb1.at[col, 2, second], 1, 3).start()
        near(col, part.at[col, up, second], rb1.at[col, 0, second], 2, 1).start()
        near(col, part.at[col, down, first], rb1.at[col, 1, first], 2, 3).start()

    def near_merge(col):
        m = coord[dims(col)[0]]
        up, down = (m + 1) % 4, (m + 3) % 4
        near(col, part.at[col, up, first], rb1.at[col, 2, first], 0, 1).wait_recv()
        part[col, up, first] = part[col, up, first] + rb1[col, 2, first]
        near(col, part.at[col, up, first], rb1.at[col, 0, first], 2, 1).start()
        near(col, part.at[col, down, second], rb1.at[col, 2, second], 1, 3).wait_recv()
        part[col, down, second] = part[col, down, second] + rb1[col, 2, second]
        near(col, part.at[col, down, second], rb1.at[col, 1, second], 2, 3).start()

    def near_wait(col):
        two = rb1.at[col, pl.ds(0, 2)]
        near(col, two, two, 2, 1).wait_recv()
        near(col, rb1.at[col], rb1.at[col], 2, 1).wait_send()

    low, high = pl.ds(0, 2), pl.ds(2, 2)

    def fwd(col, block, rows, k, o):
        ref = gath.at[col, block, rows]
        return rcopy(ref, ref, fwd_s.at[col], fwd_r.at[col * 4 + k], peer(dims(col)[0], o))

    def fwd_start(col):
        m = coord[dims(col)[0]]
        fwd(col, m, low, 0, 1).start()
        fwd(col, m, high, 1, 3).start()
        fwd(col, m, high, 2, 1).start()
        fwd(col, m, low, 2, 3).start()

    def fwd_pass(col):
        m = coord[dims(col)[0]]
        up, down = (m + 1) % 4, (m + 3) % 4
        fwd(col, down, low, 0, 1).wait_recv()
        fwd(col, down, low, 3, 1).start()
        fwd(col, up, high, 1, 3).wait_recv()
        fwd(col, up, high, 3, 3).start()

    def fwd_wait(col, k):
        one = gath.at[col, 0]
        rcopy(one, one, fwd_s.at[col], fwd_r.at[col * 4 + k], sib).wait_recv()

    def fwd_sent(col):
        three = gath.at[col, pl.ds(0, 3)]
        rcopy(three, three, fwd_s.at[col], fwd_r.at[col * 4 + 2], sib).wait_send()

    def mid_copy(col, o):
        d = dims(col)[1]
        j = (coord[d] + o) % 4
        return rcopy(s1.at[col, j], rb2.at[col, o - 1], rs_s.at[col], rs_r.at[col], peer(d, o))

    def small_copy(col, o):
        d = dims(col)[2]
        return rcopy(s2.at[col], rb3.at[col, coord[d]], rs_s.at[3 + col], rs_r.at[3 + col], peer(d, o))

    def ag_copy(col, o):
        m1, m2 = (coord[d] for d in dims(col)[:2])
        ref = gath.at[col, m1, m2]
        return rcopy(ref, ref, rs_s.at[6 + col], rs_r.at[6 + col], peer(dims(col)[1], o))

    def wait_three(ref, k):
        rcopy(ref, ref, rs_s.at[k], rs_r.at[k], sib).wait()

    for col in range(3):
        for b in range(4):
            i, j = BLOCKS[col * 4 + b]
            res = lax.dot_general(xg[i * 256:(i + 1) * 256, :], xg[j * 256:(j + 1) * 256, :], (((1,), (1,)), ((), ())), preferred_element_type=F32)
            for h in range(2):
                part[col, b, h * 8:(h + 1) * 8] = res[:, h * 128:(h + 1) * 128].reshape(8, 32, 128)
        near_start(col)
    for col in range(3):
        near_merge(col)
    for col in range(3):
        near_wait(col)
        s1[col] = (part[col, coord[dims(col)[0]]] + rb1[col, 0] + rb1[col, 1]).reshape(4, 4, 32, 128)
        for o in range(1, 4):
            mid_copy(col, o).start()
    for col in range(3):
        wait_three(rb2.at[col], col)
        total = s1[col, coord[dims(col)[1]]] + rb2[col, 0] + rb2[col, 1] + rb2[col, 2]
        s2[col] = total
        for o in range(1, 4):
            small_copy(col, o).start()
        rb3[col, coord[dims(col)[2]]] = total
    for col in range(3):
        wait_three(rb3.at[col, pl.ds(0, 3)], 3 + col)
        m1, m2 = (coord[d] for d in dims(col)[:2])
        gath[col, m1, m2] = (rb3[col, 0] + rb3[col, 1]) + (rb3[col, 2] + rb3[col, 3])
        for o in range(1, 4):
            ag_copy(col, o).start()
    for col in range(3):
        wait_three(gath.at[col, 0, pl.ds(0, 3)], 6 + col)
        fwd_start(col)

    base = half + used

    def lookup(values, at):
        out = values[3]
        for n in range(3):
            out = jnp.where(at == n, values[n], out)
        return out

    def to_sibling(r, c, rows, cols_n, r2, c2):
        rcopy(af.at[pl.ds(r, rows), pl.ds(c, cols_n)], af.at[pl.ds(r2, rows), pl.ds(c2, cols_n)], pa_s, pa_r, sib).start()

    def al256(v):
        return pl.multiple_of(v, 256)

    def al128(v):
        return pl.multiple_of(v, 128)

    def place(col, b, h):
        quad = BLOCKS[col * 4:col * 4 + 4]
        i = lookup([p[0] for p in quad], b)
        j = lookup([p[1] for p in quad], b)
        v = gath[col, b, 2 * h:2 * h + 2].reshape(256, 128)
        r, c = al256(i * 256), al128(j * 256 + h * 128)
        gram[pl.ds(r, 256), pl.ds(c, 128)] = v
        af[pl.ds(r, 256), pl.ds(c, 128)] = v.astype(BF16)
        to_sibling(r, c, 256, 128, base + r, al128((j + 3) % 6 * 256 + h * 128))
        mirrored = [n for n in range(4) if quad[n][1] < quad[n][0]]
        swapped = [n for n in range(4) if col * 4 + n in SWAPPED]
        if mirrored:
            hit = b == mirrored[0]
            for n in mirrored[1:]:
                hit = hit | (b == n)

            @pl.when(hit)
            def _():
                vt = v.T
                r2, c2 = al128(j * 256 + h * 128), al256(i * 256)
                gram[pl.ds(r2, 128), pl.ds(c2, 256)] = vt
                af[pl.ds(r2, 128), pl.ds(c2, 256)] = vt.astype(BF16)
                to_sibling(r2, c2, 128, 256, base + r2, al256((i + 3) * 256))

        for n in swapped:
            i0, j0 = quad[n]
            k = SWAPPED.index(col * 4 + n)

            @pl.when(b == n)
            def _():
                vt = v.T
                r2 = (j0 - 3) * 256 + h * 128
                swap[k, h] = vt
                rcopy(swap.at[k, h], gram.at[pl.ds(r2, 128), pl.ds((i0 + 3) * 256, 256)], sw_s, sw_r, sib).start()
                af[base + r2:base + r2 + 128, i0 * 256:(i0 + 1) * 256] = vt.astype(BF16)

    ring = [coord[dims(col)[0]] for col in range(3)]
    for col in range(3):
        for h in range(2):
            place(col, ring[col], h)
    for col in range(3):
        fwd_pass(col)
    for col in range(3):
        place(col, (ring[col] + 3) % 4, 0)
        place(col, (ring[col] + 1) % 4, 1)
    for col in range(3):
        fwd_wait(col, 2)
        place(col, (ring[col] + 3) % 4, 1)
        place(col, (ring[col] + 1) % 4, 0)
    for col in range(3):
        fwd_wait(col, 3)
        for h in range(2):
            place(col, (ring[col] + 2) % 4, h)
    for col in range(3):
        fwd_sent(col)
    rcopy(swap, swap, sw_s, sw_r, sib).wait()
    for n in range(3):
        i, j = BLOCKS[SWAPPED[n]]
        rs, cs = slice((j - 3) * 256, (j - 2) * 256), slice((i + 3) * 256, (i + 4) * 256)
        af[rs, cs] = gram[rs, cs].astype(BF16)

    def piece(buf, ssem, rsem, p):
        q = (p + 3) % 6
        base = buf.shape[0] - half
        return rcopy(buf.at[pl.ds(0, half), pl.ds(pl.multiple_of(p * 256, 256), 256)],
                     buf.at[pl.ds(base, half), pl.ds(pl.multiple_of(q * 256, 256), 256)], ssem, rsem, sib)

    def send_two(buf, ssem, rsem, n):
        piece(buf, ssem, rsem, 2 * n).start()
        piece(buf, ssem, rsem, 2 * n + 1).start()

    def wait_recv(buf, ssem, rsem, rows=768):
        rcopy(buf.at[pl.ds(0, rows)], buf.at[pl.ds(0, rows)], ssem, rsem, sib).wait_recv()

    def wait_send(buf, ssem, rsem, rows=768):
        rcopy(buf.at[pl.ds(0, rows)], buf.at[pl.ds(0, rows)], ssem, rsem, sib).wait_send()

    def diag_copy():
        return rcopy(dv.at[:, pl.ds(0, half)], dv.at[:, pl.ds(half, half)], dv_s, dv_r, sib)

    diag = lax.broadcasted_iota(jnp.int32, (128, 128), 0) == lax.broadcasted_iota(jnp.int32, (128, 128), 1)

    def poly_step(rows):
        mid[own, :] = dot(af[own, own], af[own, :])
        wait_recv(af, pa_s, pa_r, rows)

        for n in range(3):
            cs = slice(n * 512, n * 512 + 512)
            acc = mid[own, cs] + dot(af[own, oth], af[oth_rows, cs])
            bff[own, cs] = (COEF_B * af[own, cs].astype(F32) + COEF_C * acc).astype(BF16)
            for i in range(4 * n, min(4 * n + 4, 6)):
                ts = slice(i * 128, i * 128 + 128)
                tile = bff[ts, ts].astype(F32)
                on = jnp.sum(jnp.where(diag, tile, 0.0), axis=0, keepdims=True)
                dv[:, ts] = jnp.broadcast_to(COEF_A + on, (8, 128))
                bff[ts, ts] = jnp.where(diag, 0.0, tile).astype(BF16)
            send_two(bff, pb_s, pb_r, n)

        diag_copy().start()
        wait_send(af, pa_s, pa_r, rows)

    poly_step(640)

    @pl.loop(0, NS_STEPS - 1)
    def _(k):
        mid[both, :] = dot(af[both, own], bff[own, :])
        wait_recv(bff, pb_s, pb_r)
        diag_copy().wait_recv()
        v = mid[both, :] + dot(af[both, oth], bff[oth, :])
        q_diag = dv[0:1, :]
        top = v[own] + gram[...] * q_diag
        mid[own, :] = top
        tb[...] = top.astype(BF16)
        x_new = (v[xrow] + af[xrow, :].astype(F32) * q_diag).astype(BF16)
        af[xrow, :] = x_new

        for n in range(3):
            cs = slice(n * 512, n * 512 + 512)
            v = mid[own, cs] * dv[0:1, cs] + dot(tb[...], bff[:, cs])
            gram[:, cs] = v
            af[own, cs] = v.astype(BF16)
            send_two(af, pa_s, pa_r, n)

        wait_send(bff, pb_s, pb_r)
        diag_copy().wait_send()

        @pl.when(k < NS_STEPS - 2)
        def _():
            poly_step(768)

    share = rcopy(af.at[pl.ds(half, used), pl.ds(half, half)], xs, xs_s, xs_r, sib)
    share.start()
    mid[own, :] = dot(af[own, own], af[own, :])
    wait_recv(af, pa_s, pa_r)
    share.wait()
    pair = jnp.concatenate([af[xrow, own], xs[...]], axis=0)
    for n in range(3):
        cs = slice(n * 512, n * 512 + 512)
        acc = mid[own, cs] + dot(af[own, oth], af[oth_rows, cs])
        bff[own, cs] = (COEF_B * af[own, cs].astype(F32) + COEF_C * acc).astype(BF16)
        v = dot(pair, bff[own, cs])
        mid[xrow, cs] = COEF_A * af[xrow, cs].astype(F32) + v[0:used]
        xsend[:, cs] = v[used:2 * used]
        for p in (2 * n, 2 * n + 1):
            rcopy(xsend.at[:, pl.ds(p * 256, 256)], xrecv.at[:, pl.ds((p + 3) % 6 * 256, 256)], xp_s, xp_r, sib).start()
    wait_send(af, pa_s, pa_r)
    rcopy(xsend, xrecv, xp_s, xp_r, sib).wait()
    mid[xrow, :] = mid[xrow, :] + xrecv[...]

    for i in range(4):
        v = mid[xrow, pl.ds(i * 384, 384)].astype(BF16).astype(F32)
        v = jnp.concatenate([v, jnp.zeros((lanes - used, 384), F32)], axis=0).T
        ys[pl.ds(i * 16, 16)] = v.reshape(16, 24, 128).astype(BF16)

    @pl.loop(1, 64)
    def _(o):
        d = (me + o) % 64
        rcopy(ys.at[(d + 32 * t) % 64], yr.at[me], out_s, out_r, {"data": d}).start()

    yr[me] = ys[slot]

    rcopy(ys.at[pl.ds(0, 63)], yr.at[pl.ds(0, 63)], out_s, out_r, sib).wait()

    for g in range(16):
        last = yr[g * 4 + 3].astype(F32)
        for r in range(3):
            x = jnp.where(lane < used, yr[g * 4 + r].astype(F32), pltpu.roll(last, 96 - 32 * r, 1))
            x_out[:, pl.ds((g * 3 + r) * 128, 128)] = x.astype(BF16)


def solution(mesh):
    data_size = mesh.shape["data"]
    tp_size = mesh.shape["tp"]
    part_spec = P(("stage", "data"), "tp")

    def local_step(weight, momentum, gradient):
        rows_local, cols_local = gradient.shape
        rows = rows_local * data_size
        sem = pltpu.SemaphoreType.DMA
        shapes = [
            pltpu.VMEM((24, 6144), F32), pltpu.VMEM((24, 6144), BF16),
            pltpu.VMEM((64, 24, 128), F32), pltpu.VMEM((64, 24, 128), F32), pltpu.VMEM((2, 8, 128), F32), pltpu.VMEM((1536, 256), BF16),
            pltpu.VMEM((3, 4, 16, 32, 128), F32), pltpu.VMEM((3, 3, 16, 32, 128), F32), pltpu.VMEM((3, 4, 4, 32, 128), F32),
            pltpu.VMEM((3, 3, 4, 32, 128), F32), pltpu.VMEM((3, 4, 32, 128), F32), pltpu.VMEM((3, 4, 4, 32, 128), F32),
            pltpu.VMEM((3, 4, 4, 4, 32, 128), F32), pltpu.VMEM((3, 2, 128, 256), F32),
            pltpu.VMEM((768, 1536), F32), pltpu.VMEM((864, 1536), F32), pltpu.VMEM((1632, 1536), BF16), pltpu.VMEM((1536, 1536), BF16),
            pltpu.VMEM((8, 1536), F32), pltpu.VMEM((768, 1536), BF16),
            pltpu.VMEM((96, 768), BF16), pltpu.VMEM((96, 1536), F32), pltpu.VMEM((96, 1536), F32),
            pltpu.VMEM((64, 24, 128), BF16), pltpu.VMEM((64, 24, 128), BF16),
            sem((2,)), sem, sem, sem, sem, sem, sem, sem, sem, sem, sem, sem, sem, sem((3,)), sem((9,)), sem((3,)), sem((12,)), sem((9,)), sem((9,)),
            sem, sem, sem, sem, sem, sem, sem, sem,
        ]
        anywhere = pl.BlockSpec(memory_space=pl.ANY)
        x_fin = pl.pallas_call(
            kernel,
            out_shape=jax.ShapeDtypeStruct((rows_local, cols_local), BF16),
            in_specs=[anywhere] * 2,
            out_specs=pl.BlockSpec(memory_space=pltpu.VMEM),
            scratch_shapes=shapes,
            compiler_params=pltpu.CompilerParams(collective_id=0, has_side_effects=True, vmem_limit_bytes=VMEM_MIB * 1024 * 1024),
            name="muon_steps",
        )(momentum, gradient)
        new_mom = MOMENTUM * momentum + gradient.astype(F32)
        rms_scale = 0.2 * math.sqrt(max(rows, cols_local * tp_size))
        new_weight = weight - LEARN_RATE * (rms_scale * x_fin.astype(F32) + WEIGHT_DECAY * weight)
        return new_weight, new_mom

    return jax.shard_map(local_step, mesh=mesh, in_specs=(part_spec, part_spec, part_spec), out_specs=(part_spec, part_spec), check_vma=False)
```
